512 devices in a mesh: win: 128 (over z, y, core), tile: 4 (over x).
Axes of the slice: x: 4, y: 8, z: 8, core: 2. Of those that a mesh axis runs over, the one named last changes fastest.
Arguments:
- right_side: float32 [128, 2, 128, 1024], P('win', None, 'tile'), may hold values from -64 to 64
- error_weight: float32 [128, 2, 128, 1024], P('win', None, 'tile'), may hold values from 0.5 to 4
- coeffs: float32 [4, 128, 2, 128, 1024], P(None, 'win', None, 'tile'), may hold values from 0.1 to 0.4
- obs_block: int32 [128, 128], P('win', 'tile'), may hold values from 0 to 511
- obs_pos: int32 [128, 128, 128], P('win', 'tile'), may hold values from 0 to 127
- obs_weight: float32 [128, 128, 128], P('win', 'tile'), may hold values from 0.5 to 4
Outputs:
- solution_field: float32 [128, 2, 128, 1024], P('win', None, 'tile')
- residual: float32 [128, 2, 128, 1024], P('win', None, 'tile')
The draws below stay inside these ranges and needn't reach their ends.
All inputs are finite; a program needn't handle non-finite values.
Results may differ from the reference program's by a relative error of at most 0.0001.
Values sent between devices are 32-bit elements; how exact they have to be, the bound alone decides.
A program may use at most 64 MiB of HBM per device.

```python
import math
import jax
import jax.numpy as jnp

LEV = 2
TY = 32
NX = 1024
NBLK = 32
OBSW = 128
ITERS = 3
NWIN = 128
NY = 128
BROWS = 512
N_TILE = 4


def draw_right_side(key, part):
    gaussian = jax.random.normal(jax.random.fold_in(key, 11), (NWIN, LEV, NY, NX), jnp.float32)
    gaussian = jnp.clip(gaussian, -6.0, 6.0)
    growth = 1.0 + 2.0 * jnp.arange(NWIN, dtype=jnp.float32) / max(NWIN - 1, 1)
    growth = growth.reshape(NWIN, 1, 1, 1)
    return growth * gaussian


def place_ends(entries, own_key, low, top_value):
    longest = entries.shape.index(max(entries.shape))
    spots = []
    for shift in (0, 1):
        where = [jax.random.randint(jax.random.fold_in(own_key, axis), (), 0, length) for axis, length in enumerate(entries.shape)]
        where[longest] = (where[longest] + shift) % entries.shape[longest]
        spots.append(tuple(where))
    return entries.at[spots[0]].set(low).at[spots[1]].set(top_value)


def block_levels(key, extent, pieces, smallest, largest):
    def one(axis_at, shards_of):
        heights = jax.random.uniform(jax.random.fold_in(jax.random.fold_in(key, 6), axis_at), (shards_of,), jnp.float32, smallest / len(pieces), largest / len(pieces))
        return jnp.repeat(jnp.exp(heights), extent[axis_at] // shards_of).reshape((-1,) + (1,) * (len(extent) - axis_at - 1))

    level = one(*pieces[0])
    for cut in pieces[1:]:
        level = level * one(*cut)
    return level


def setup_inputs(seed: int = 0) -> dict:
    seeds = jax.random.split(jax.random.key(seed), 7)
    right_side = draw_right_side(jax.random.fold_in(seeds[6], 71), 0)
    error_weight = jnp.clip(jnp.exp(math.log(4.0) - 2.0794415 * jax.random.uniform(seeds[1], (NWIN, LEV, NY, NX), jnp.float32) ** block_levels(seeds[1], (NWIN, LEV, NY, NX), ((0, 128), (2, 4)), -0.2, 0.2)), 0.5, 4.0)
    coeffs = jnp.clip(0.1 + 0.3 * jax.random.uniform(seeds[2], (4, NWIN, LEV, NY, NX), jnp.float32) ** block_levels(seeds[2], (4, NWIN, LEV, NY, NX), ((1, 128), (3, 4)), -0.2, 0.2), 0.1, 0.4)
    obs_block = place_ends(jax.random.randint(seeds[3], (NWIN, N_TILE * NBLK), 0, BROWS), jax.random.fold_in(seeds[3], 1), 0, BROWS - 1).astype(jnp.int32)
    obs_pos = place_ends(jax.random.randint(seeds[4], (NWIN, N_TILE * NBLK, OBSW), 0, OBSW), jax.random.fold_in(seeds[4], 1), 0, OBSW - 1).astype(jnp.int32)
    obs_weight = jnp.clip(jnp.exp(math.log(4.0) - 2.0794415 * jax.random.uniform(seeds[5], (NWIN, N_TILE * NBLK, OBSW), jnp.float32) ** block_levels(seeds[5], (NWIN, N_TILE * NBLK, OBSW), ((0, 128), (1, 4)), -0.2, 0.2)), 0.5, 4.0)
    return {"right_side": right_side, "error_weight": error_weight, "coeffs": coeffs, "obs_block": obs_block, "obs_pos": obs_pos, "obs_weight": obs_weight}


def model_step(state, coeffs):
    padded = jnp.pad(state, ((0, 0), (0, 0), (1, 1), (0, 0)))
    north_south = padded[:, :, 2:, :] + padded[:, :, :-2, :]
    return (coeffs[0] * state + coeffs[1] * north_south
            + coeffs[2] * jnp.roll(state, -1, axis=3) + coeffs[3] * jnp.roll(state, 1, axis=3))


def model_adjoint(state, coeffs):
    spread = jnp.pad(coeffs[1] * state, ((0, 0), (0, 0), (1, 1), (0, 0)))
    north_south = spread[:, :, 2:, :] + spread[:, :, :-2, :]
    return (coeffs[0] * state + north_south
            + jnp.roll(coeffs[2] * state, 1, axis=3) + jnp.roll(coeffs[3] * state, -1, axis=3))


def observe(state, obs_block, obs_pos, obs_weight):
    windows = state.shape[0]
    cell_count = LEV * TY * NX
    blocks = state.reshape(windows, LEV, N_TILE, TY, NX).transpose(0, 2, 1, 3, 4).reshape(windows, N_TILE, cell_count)
    flat_index = (obs_block.reshape(windows, N_TILE, NBLK, 1).astype(jnp.int32) * OBSW
                  + obs_pos.reshape(windows, N_TILE, NBLK, OBSW).astype(jnp.int32))
    flat_index = flat_index.reshape(windows, N_TILE, NBLK * OBSW).astype(jnp.int32)
    observed = jnp.take_along_axis(blocks, flat_index, axis=2)
    weighted = observed * obs_weight.reshape(windows, N_TILE, NBLK * OBSW)

    def place(index_row, value_row):
        return jnp.zeros((cell_count,), jnp.float32).at[index_row].add(value_row)

    spread = jax.vmap(jax.vmap(place))(flat_index, weighted)
    return spread.reshape(windows, N_TILE, LEV, TY, NX).transpose(0, 2, 1, 3, 4).reshape(windows, LEV, NY, NX)


def reference(right_side, error_weight, coeffs, obs_block, obs_pos, obs_weight):
    def hessian(state):
        propagated = model_step(state, coeffs)
        before = jnp.concatenate([jnp.zeros_like(propagated[:1]), propagated[:-1]], axis=0)
        weighted = error_weight * (state - before)
        following = jnp.concatenate([weighted[1:], jnp.zeros_like(weighted[:1])], axis=0)
        return weighted - model_adjoint(following, coeffs) + observe(state, obs_block, obs_pos, obs_weight)

    solution_field = jnp.zeros_like(right_side)
    residual = right_side
    direction = right_side
    norm_now = jnp.sum(residual * residual)
    for iteration in range(ITERS):
        product_vec = hessian(direction)
        step_length = norm_now / jnp.sum(direction * product_vec)
        solution_field = solution_field + step_length * direction
        residual = residual - step_length * product_vec
        norm_next = jnp.sum(residual * residual)
        direction = residual + (norm_next / norm_now) * direction
        norm_now = norm_next
    return solution_field, residual
```

```python
import jax
import jax.numpy as jnp
from jax import lax
from jax.experimental import pallas as pl
from jax.experimental.pallas import tpu as pltpu
from jax.sharding import PartitionSpec as P

MESH = pl.DeviceIdType.MESH
F32 = jnp.float32
LEV, TY, NX = 2, 32, 1024
BLOCKS = TY // 8
STEPS = 3
SCALE = 1.0 / 16.0
NZ, NYC, NCORE, NT = 8, 8, 2, 4
NWIN = NZ * NYC * NCORE
PAIRS = ((0, 0), (0, 1), (1, 1), (0, 2), (1, 2), (2, 2), (0, 3), (1, 3), (2, 3))
HALO_N, HALO_S, EDGE, STATE, IMAGE, IMAGE_EDGE, ADJ_N, ADJ_S = 0, 1, 2, 3, 5, 7, 8, 9
MESSAGES = 10


def two_sum(a, b):
    s = a + b
    t = s - a
    return s, (a - (s - t)) + (b - t)


def quick_sum(a, b):
    s = a + b
    return s, b - (s - a)


def split(a):
    c = a * 4097.0
    high = c - (c - a)
    return high, a - high


def two_prod_split(a, b, sa, sb):
    p = a * b
    return p, ((sa[0] * sb[0] - p) + sa[0] * sb[1] + sa[1] * sb[0]) + sa[1] * sb[1]


def two_prod(a, b):
    return two_prod_split(a, b, split(a), split(b))


def add2(a, b):
    s, e = two_sum(a[0], b[0])
    return quick_sum(s, e + (a[1] + b[1]))


def neg2(a):
    return -a[0], -a[1]


def sub2(a, b):
    return add2(a, neg2(b))


def mul2(a, b):
    p, e = two_prod(a[0], b[0])
    return quick_sum(p, e + (a[0] * b[1] + a[1] * b[0]))


def div2(a, b):
    zero = jnp.zeros_like(a[0])
    first = a[0] / b[0]
    rest = sub2(a, mul2((first, zero), b))
    second = rest[0] / b[0]
    rest = sub2(rest, mul2((second, zero), b))
    third = rest[0] / b[0]
    return add2(quick_sum(first, second), (third, zero))


def tree2(items):
    while len(items) > 1:
        items = [
            add2(items[i], items[i + 1]) if i + 1 < len(items) else items[i]
            for i in range(0, len(items), 2)
        ]
    return items[0]


def kernel(
    right_hbm,
    weight_hbm,
    coeff_hbm,
    block_hbm,
    pos_hbm,
    obsw_hbm,
    v1,
    v2,
    v3,
    combo,
    v0,
    weight,
    coeff,
    block,
    pos,
    obsw,
    diag,
    edge,
    weight_edge,
    halo_n,
    halo_s,
    next_edge,
    next_weight_edge,
    next_state,
    next_weight,
    image,
    before,
    image_edge,
    before_edge,
    adj_edge,
    adj_n,
    adj_s,
    follow,
    spread,
    gram_high,
    gram_low,
    row_send,
    row_recv,
    local_sem,
    send_sem,
    recv_sem,
    wsend_sem,
    wrecv_sem,
    rsend_sem,
    rrecv_sem,
):
    win = lax.axis_index("win")
    tile = lax.axis_index("tile")
    core = win % 2
    chip_y = (win // 2) % 8
    chip_z = win // 16
    has_prev, has_next = win > 0, win < NWIN - 1
    has_north, has_south = tile > 0, tile < NT - 1
    prev_id, next_id = (win - 1, tile), (win + 1, tile)
    north_id, south_id = (win, tile - 1), (win, tile + 1)
    states = (v0, v1, v2, v3)

    loads = [
        pltpu.make_async_copy(src, dst, local_sem.at[i])
        for i, (src, dst) in enumerate(
            (
                (right_hbm, v0),
                (weight_hbm, weight),
                (coeff_hbm, coeff),
                (block_hbm, block),
                (pos_hbm, pos),
                (obsw_hbm, obsw),
            )
        )
    ]
    for load in loads:
        load.start()

    slot_a = core * NT + tile
    peers_a, peers_b, peers_c = [], [], []
    for i in range(1, NCORE * NT):
        other = (slot_a + i) % (NCORE * NT)
        peers_a.append((win - core + other // NT, other % NT))
    for i in range(1, NYC):
        other = (chip_y + i) % NYC
        peers_b.append((win + 2 * (other - chip_y), tile))
    for i in range(1, NZ):
        other = (chip_z + i) % NZ
        peers_c.append((win + 16 * (other - chip_z), tile))

    barrier = pltpu.get_barrier_semaphore()
    for peer in (*peers_a, *peers_b, *peers_c):
        pl.semaphore_signal(barrier, inc=1, device_id=peer, device_id_type=MESH)

    @pl.when(has_prev)
    def _():
        pl.semaphore_signal(barrier, inc=1, device_id=prev_id, device_id_type=MESH)

    @pl.when(has_next)
    def _():
        pl.semaphore_signal(barrier, inc=1, device_id=next_id, device_id_type=MESH)

    @pl.when(jnp.logical_not(has_north))
    def _():
        halo_n[...] = jnp.zeros_like(halo_n)
        adj_n[...] = jnp.zeros_like(adj_n)

    @pl.when(jnp.logical_not(has_south))
    def _():
        halo_s[...] = jnp.zeros_like(halo_s)
        adj_s[...] = jnp.zeros_like(adj_s)

    @pl.when(jnp.logical_not(has_prev))
    def _():
        before[...] = jnp.zeros_like(before)
        before_edge[...] = jnp.zeros_like(before_edge)

    @pl.when(jnp.logical_not(has_next))
    def _():
        next_edge[...] = jnp.zeros_like(next_edge)
        next_weight_edge[...] = jnp.zeros_like(next_weight_edge)
        next_state[...] = jnp.zeros_like(next_state)
        next_weight[...] = jnp.zeros_like(next_weight)

    for i in range(2):
        loads[i].wait()
    for side, row in ((0, 0), (1, TY - 1)):
        for l in range(LEV):
            edge[0, side, l : l + 1, :] = v0[l, row : row + 1, :]
            weight_edge[side, l : l + 1, :] = weight[l, row : row + 1, :]

    near = jnp.where(has_prev, 1, 0) + jnp.where(has_next, 1, 0)
    pl.semaphore_wait(barrier, len(peers_a) + len(peers_b) + len(peers_c) + near)

    started = []

    def remote(src, dst, send, recv, peer):
        return pltpu.make_async_remote_copy(
            src_ref=src, dst_ref=dst, send_sem=send, recv_sem=recv, device_id=peer, device_id_type=MESH
        )

    def start_if(condition, copies):
        @pl.when(condition)
        def _():
            for copy in copies:
                copy.start()

        started.append((condition, copies))

    def wait_if(condition, copies):
        @pl.when(condition)
        def _():
            for copy in copies:
                copy.wait_recv()

    row_id = lax.broadcasted_iota(jnp.int32, (8, NX), 0)
    first_row, last_row = row_id == 0, row_id == 7

    def for_blocks(body):
        def step(b, _):
            body(b)
            return 0

        lax.fori_loop(0, BLOCKS, step, 0)

    def rows(b):
        return pl.ds(pl.multiple_of(b * 8, 8), 8)

    def vertical(ref, l, b):
        here = ref[l, rows(b), :]
        above = ref[l, rows(jnp.maximum(b - 1, 0)), :]
        below = ref[l, rows(jnp.minimum(b + 1, BLOCKS - 1)), :]
        above = above * jnp.where(b > 0, 1.0, 0.0)
        below = below * jnp.where(b < BLOCKS - 1, 1.0, 0.0)
        north = jnp.where(first_row, pltpu.roll(above, 1, 0), pltpu.roll(here, 1, 0))
        south = jnp.where(last_row, pltpu.roll(below, 7, 0), pltpu.roll(here, 7, 0))
        return north + south

    def gram(index):
        i, j = PAIRS[index]
        zero = jnp.zeros((8, NX), F32)

        def step(n, acc):
            l, b = n // BLOCKS, n % BLOCKS
            x = states[i][l, rows(b), :]
            y = states[j][l, rows(b), :]
            p, e = two_prod(x, y)
            s, f = two_sum(acc[0], p)
            return s, acc[1] + (e + f)

        high, low = lax.fori_loop(0, LEV * BLOCKS, step, (zero, zero))
        parts = [(high[:, c * 128 : (c + 1) * 128], low[:, c * 128 : (c + 1) * 128]) for c in range(8)]
        total = tree2([quick_sum(*part) for part in parts])
        for shift in (4, 2, 1):
            total = add2(total, (pltpu.roll(total[0], shift, 0), pltpu.roll(total[1], shift, 0)))
        gram_high[index : index + 1, :] = total[0][0:1, :]
        gram_low[index : index + 1, :] = total[1][0:1, :]

    def observed_weights():
        pos_t = jnp.swapaxes(pos[...], 0, 1)
        obsw_t = jnp.swapaxes(obsw[...], 0, 1)
        lane = lax.broadcasted_iota(jnp.int32, (128, 128), 1)
        lines = []
        for b in range(32):
            hit = pos_t[:, b : b + 1] == lane
            lines.append(jnp.sum(jnp.where(hit, obsw_t[:, b : b + 1], 0.0), axis=0, keepdims=True))
        per_block = jnp.concatenate(lines, axis=0)
        row = lax.broadcasted_iota(jnp.int32, (LEV * TY, 32), 0)
        for c in range(NX // 128):
            hot = (block[...] == row * (NX // 128) + c).astype(F32)
            out = jnp.dot(hot, per_block, precision=lax.Precision.HIGHEST, preferred_element_type=F32)
            for l in range(LEV):
                diag[l, :, c * 128 : (c + 1) * 128] = out[l * TY : (l + 1) * TY, :]

    for j in range(STEPS):
        v, out = states[j], states[j + 1]
        ssem, rsem = send_sem.at[j], recv_sem.at[j]
        to_south = [remote(edge.at[j, 1], halo_n.at[j], ssem.at[HALO_N], rsem.at[HALO_N], south_id)]
        to_north = [remote(edge.at[j, 0], halo_s.at[j], ssem.at[HALO_S], rsem.at[HALO_S], north_id)]
        back_edge = [remote(edge.at[j], next_edge.at[j], ssem.at[EDGE], rsem.at[EDGE], prev_id)]
        back = [
            remote(v.at[l], next_state.at[j, l], ssem.at[STATE + l], rsem.at[STATE + l], prev_id)
            for l in range(LEV)
        ]
        back_weight, back_weight_edge = [], []
        if j == 0:
            back_weight_edge = [
                remote(weight_edge, next_weight_edge, wsend_sem.at[2], wrecv_sem.at[2], prev_id)
            ]
            back_weight = [
                remote(weight.at[l], next_weight.at[l], wsend_sem.at[l], wrecv_sem.at[l], prev_id)
                for l in range(LEV)
            ]
        ahead = [
            remote(image.at[j, l], before.at[j, l], ssem.at[IMAGE + l], rsem.at[IMAGE + l], next_id)
            for l in range(LEV)
        ]
        ahead_edge = [
            remote(image_edge.at[j], before_edge.at[j], ssem.at[IMAGE_EDGE], rsem.at[IMAGE_EDGE], next_id)
        ]
        adj_to_south = [remote(adj_edge.at[j, 1], adj_n.at[j], ssem.at[ADJ_N], rsem.at[ADJ_N], south_id)]
        adj_to_north = [remote(adj_edge.at[j, 0], adj_s.at[j], ssem.at[ADJ_S], rsem.at[ADJ_S], north_id)]

        start_if(has_south, to_south)
        start_if(has_north, to_north)
        interleaved = [*back_edge, *back_weight_edge]
        for l in range(LEV):
            interleaved.append(back[l])
            interleaved.extend(back_weight[l : l + 1])
        start_if(has_prev, interleaved)

        if j == 0:
            loads[2].wait()
        for l in range(LEV):

            def propagate(b, l=l):
                here = v[l, rows(b), :]
                image[j, l, rows(b), :] = (
                    coeff[0, l, rows(b), :] * here
                    + coeff[1, l, rows(b), :] * vertical(v, l, b)
                    + coeff[2, l, rows(b), :] * pltpu.roll(here, NX - 1, 1)
                    + coeff[3, l, rows(b), :] * pltpu.roll(here, 1, 1)
                )

            for_blocks(propagate)
            start_if(has_next, [ahead[l]])

        wait_if(has_north, to_south)
        wait_if(has_south, to_north)
        for side, row, halo in ((0, 0, halo_n), (1, TY - 1, halo_s)):
            for l in range(LEV):
                image_edge[j, side, l : l + 1, :] = (
                    coeff[1, l, row : row + 1, :] * halo[j, l : l + 1, :]
                )
        start_if(has_next, ahead_edge)
        wait_if(has_next, [*back_edge, *back_weight_edge])
        edge_follow = {}
        for side, row in ((0, 0), (1, TY - 1)):
            for l in range(LEV):
                f = next_weight_edge[side, l : l + 1, :] * (
                    next_edge[j, side, l : l + 1, :]
                    - (image[j, l, row : row + 1, :] + image_edge[j, side, l : l + 1, :])
                )
                edge_follow[side, l] = f
                adj_edge[j, side, l : l + 1, :] = coeff[1, l, row : row + 1, :] * f
        start_if(has_south, adj_to_south)
        start_if(has_north, adj_to_north)

        if j == 0:
            for load in loads[3:]:
                load.wait()
            observed_weights()
        if j == 1:
            for index in (0, 1, 2):
                gram(index)
        if j == 2:
            for index in (3, 4, 5):
                gram(index)

        for l in range(LEV):
            wait_if(has_next, [back[l], *back_weight[l : l + 1]])

            def following(b, l=l):
                f = next_weight[l, rows(b), :] * (next_state[j, l, rows(b), :] - image[j, l, rows(b), :])
                follow[l, rows(b), :] = f
                spread[l, rows(b), :] = coeff[1, l, rows(b), :] * f

            for_blocks(following)
            for side, row in ((0, 0), (1, TY - 1)):
                follow[l, row : row + 1, :] = edge_follow[side, l]
                spread[l, row : row + 1, :] = adj_edge[j, side, l : l + 1, :]

            def adjoint(b, l=l):
                f = follow[l, rows(b), :]
                back_image = (
                    coeff[0, l, rows(b), :] * f
                    + vertical(spread, l, b)
                    + pltpu.roll(coeff[2, l, rows(b), :] * f, 1, 1)
                    + pltpu.roll(coeff[3, l, rows(b), :] * f, NX - 1, 1)
                )
                here = v[l, rows(b), :]
                out[l, rows(b), :] = (
                    weight[l, rows(b), :] * here - back_image + diag[l, rows(b), :] * here
                )

            for_blocks(adjoint)

        wait_if(has_north, adj_to_south)
        wait_if(has_south, adj_to_north)
        wait_if(has_prev, ahead_edge)
        for l in range(LEV):
            wait_if(has_prev, [ahead[l]])

            def finish(b, l=l):
                out[l, rows(b), :] = SCALE * (
                    out[l, rows(b), :] - weight[l, rows(b), :] * before[j, l, rows(b), :]
                )

            for_blocks(finish)
            for side, row, adj in ((0, 0, adj_n), (1, TY - 1, adj_s)):
                e = out[l, row : row + 1, :] - SCALE * (
                    adj[j, l : l + 1, :]
                    + weight[l, row : row + 1, :] * before_edge[j, side, l : l + 1, :]
                )
                out[l, row : row + 1, :] = e
                if j + 1 < STEPS:
                    edge[j + 1, side, l : l + 1, :] = e

    for index in (6, 7, 8):
        gram(index)

    sub = lax.broadcasted_iota(jnp.int32, (16, 128), 0)
    valid = sub < len(PAIRS)
    total = (jnp.where(valid, gram_high[...], 0.0), jnp.where(valid, gram_low[...], 0.0))
    for shift in (64, 32, 16, 8, 4, 2, 1):
        total = add2(total, (pltpu.roll(total[0], shift, 1), pltpu.roll(total[1], shift, 1)))
    lane = lax.broadcasted_iota(jnp.int32, (16, 128), 1)
    packed = jnp.where(lane == sub, total[0], jnp.where(lane == sub + 16, total[1], 0.0))
    line = jnp.sum(packed, axis=0, keepdims=True)
    line_lane = lax.broadcasted_iota(jnp.int32, (1, 128), 1)
    for stage, (mine, peers) in enumerate(((slot_a, peers_a), (chip_y, peers_b), (chip_z, peers_c))):
        row_send[stage] = line
        row_recv[stage, mine] = line
        copies = [
            remote(row_send.at[stage], row_recv.at[stage, mine], rsend_sem.at[stage, i], rrecv_sem.at[stage, i], peer)
            for i, peer in enumerate(peers)
        ]
        for copy in copies:
            copy.start()
        started.append((None, copies))
        for copy in copies:
            copy.wait_recv()
        parts = [row_recv[stage, i] for i in range(8)]
        total = tree2([(part, pltpu.roll(part, 128 - 16, 1)) for part in parts])
        line = jnp.where(
            line_lane < 16, total[0], jnp.where(line_lane < 32, pltpu.roll(total[1], 16, 1), 0.0)
        )

    def value(i, j):
        at = PAIRS.index((min(i, j), max(i, j)))
        return tuple(
            jnp.broadcast_to(line[:, at + off : at + off + 1], (8, 128)) for off in (0, 16)
        )

    a = [[value(i, n + 1) for n in range(3)] + [value(i, 0)] for i in range(3)]
    for pivot in range(2):
        for i in range(pivot + 1, 3):
            factor = div2(a[i][pivot], a[pivot][pivot])
            for n in range(pivot + 1, 4):
                a[i][n] = sub2(a[i][n], mul2(factor, a[pivot][n]))
    c2 = div2(a[2][3], a[2][2])
    c1 = div2(sub2(a[1][3], mul2(a[1][2], c2)), a[1][1])
    c0 = div2(sub2(sub2(a[0][3], mul2(a[0][1], c1)), mul2(a[0][2], c2)), a[0][0])
    for i, c in enumerate((c0, c1, c2)):
        combo[i] = c[0]

    for condition, copies in started:

        def drain(copies=copies):
            for copy in copies:
                copy.wait_send()

        if condition is None:
            drain()
        else:
            pl.when(condition)(drain)


def on_device(right_side, error_weight, coeffs, obs_block, obs_pos, obs_weight):
    shape = (LEV, TY, NX)
    right = right_side.reshape(shape)
    vmem, hbm = pltpu.VMEM, pltpu.HBM
    state = jax.ShapeDtypeStruct(shape, F32)
    line = (STEPS, 2, LEV, NX)
    scratch = [
        vmem(shape, F32),
        vmem(shape, F32),
        vmem((4, *shape), F32),
        vmem((1, 32), jnp.int32),
        vmem((32, 128), jnp.int32),
        vmem((32, 128), F32),
        vmem(shape, F32),
        vmem(line, F32),
        vmem(line[1:], F32),
        vmem((STEPS, LEV, NX), F32),
        vmem((STEPS, LEV, NX), F32),
        vmem(line, F32),
        vmem(line[1:], F32),
        vmem((STEPS, *shape), F32),
        vmem(shape, F32),
        vmem((STEPS, *shape), F32),
        vmem((STEPS, *shape), F32),
        vmem(line, F32),
        vmem(line, F32),
        vmem(line, F32),
        vmem((STEPS, LEV, NX), F32),
        vmem((STEPS, LEV, NX), F32),
        vmem(shape, F32),
        vmem(shape, F32),
        vmem((16, 128), F32),
        vmem((16, 128), F32),
        vmem((3, 1, 128), F32),
        vmem((3, 8, 1, 128), F32),
        pltpu.SemaphoreType.DMA((6,)),
        pltpu.SemaphoreType.DMA((STEPS, MESSAGES)),
        pltpu.SemaphoreType.DMA((STEPS, MESSAGES)),
        pltpu.SemaphoreType.DMA((3,)),
        pltpu.SemaphoreType.DMA((3,)),
        pltpu.SemaphoreType.DMA((3, 7)),
        pltpu.SemaphoreType.DMA((3, 7)),
    ]
    v1, v2, v3, combo = pl.pallas_call(
        kernel,
        out_shape=(state, state, state, jax.ShapeDtypeStruct((3, 8, 128), F32)),
        in_specs=[pl.BlockSpec(memory_space=hbm)] * 6,
        out_specs=(pl.BlockSpec(memory_space=vmem),) * 4,
        scratch_shapes=scratch,
        compiler_params=pltpu.CompilerParams(collective_id=0, has_side_effects=True),
        name="krylov",
    )(
        right,
        error_weight.reshape(shape),
        coeffs.reshape(4, *shape),
        obs_block,
        obs_pos.reshape(32, 128),
        obs_weight.reshape(32, 128),
    )
    c0, c1, c2 = (combo[i, 0, 0] for i in range(3))
    solution_field = SCALE * (c0 * right + c1 * v1 + c2 * v2)
    residual = right - c0 * v1 - c1 * v2 - c2 * v3
    return solution_field[None], residual[None]


def solution(mesh):
    in_specs = (
        P("win", None, "tile", None),
        P("win", None, "tile", None),
        P(None, "win", None, "tile", None),
        P("win", "tile"),
        P("win", "tile", None),
        P("win", "tile", None),
    )
    out_specs = (P("win", None, "tile", None), P("win", None, "tile", None))
    return jax.shard_map(on_device, mesh=mesh, in_specs=in_specs, out_specs=out_specs, check_vma=False)
```

```python
import jax
import jax.numpy as jnp
from jax import lax
from jax.experimental import pallas as pl
from jax.experimental.pallas import tpu as pltpu
from jax.sharding import PartitionSpec as P

MESH = pl.DeviceIdType.MESH
F32 = jnp.float32
LEV, TY, NX = 2, 32, 1024
BLOCKS = TY // 8
STEPS = 3
SCALE = 1.0 / 16.0
NZ, NYC, NCORE, NT = 8, 8, 2, 4
NWIN = NZ * NYC * NCORE
PAIRS = ((0, 0), (0, 1), (1, 1), (0, 2), (1, 2), (2, 2), (0, 3), (1, 3), (2, 3))
HALO_N, HALO_S, EDGE, STATE, IMAGE, IMAGE_EDGE, ADJ_N, ADJ_S = range(8)
MESSAGES = 8
ROWS = ((0, 0), (1, TY - 1))


def two_sum(a, b):
    s = a + b
    t = s - a
    return s, (a - (s - t)) + (b - t)


def quick_sum(a, b):
    s = a + b
    return s, b - (s - a)


def split(a):
    c = a * 4097.0
    high = c - (c - a)
    return high, a - high


def two_prod_split(a, b, sa, sb):
    p = a * b
    return p, ((sa[0] * sb[0] - p) + sa[0] * sb[1] + sa[1] * sb[0]) + sa[1] * sb[1]


def two_prod(a, b):
    return two_prod_split(a, b, split(a), split(b))


def add2(a, b):
    s, e = two_sum(a[0], b[0])
    return quick_sum(s, e + (a[1] + b[1]))


def neg2(a):
    return -a[0], -a[1]


def sub2(a, b):
    return add2(a, neg2(b))


def mul2(a, b):
    p, e = two_prod(a[0], b[0])
    return quick_sum(p, e + (a[0] * b[1] + a[1] * b[0]))


def div2(a, b):
    zero = jnp.zeros_like(a[0])
    first = a[0] / b[0]
    rest = sub2(a, mul2((first, zero), b))
    return quick_sum(first, rest[0] / b[0])


def tree2(items):
    while len(items) > 1:
        items = [
            add2(items[i], items[i + 1]) if i + 1 < len(items) else items[i]
            for i in range(0, len(items), 2)
        ]
    return items[0]


def rolled(pair, shift, axis):
    return pltpu.roll(pair[0], shift, axis), pltpu.roll(pair[1], shift, axis)


def kernel(
    right_hbm,
    weight_hbm,
    coeff_hbm,
    block_hbm,
    pos_hbm,
    obsw_hbm,
    solution_out,
    residual_out,
    v0,
    v1,
    v2,
    v3,
    weight,
    coeff,
    block,
    pos,
    obsw,
    diag,
    edge,
    weight_edge,
    halo_n,
    halo_s,
    next_edge,
    next_weight_edge,
    next_state,
    next_weight,
    image,
    before,
    image_edge,
    before_edge,
    adj_edge,
    adj_n,
    adj_s,
    follow,
    spread,
    gram_high,
    gram_low,
    row_send,
    row_recv,
    local_sem,
    send_sem,
    recv_sem,
    wsend_sem,
    wrecv_sem,
    rsend_sem,
    rrecv_sem,
    known_sem,
):
    win = lax.axis_index("win")
    tile = lax.axis_index("tile")
    core = win % 2
    chip_y = (win // 2) % 8
    chip_z = win // 16
    has_prev, has_next = win > 0, win < NWIN - 1
    has_north, has_south = tile > 0, tile < NT - 1
    prev_id, next_id = (win - 1, tile), (win + 1, tile)
    north_id, south_id = (win, tile - 1), (win, tile + 1)
    states = (v0, v1, v2, v3)

    loads = [
        pltpu.make_async_copy(src, dst, local_sem.at[i])
        for i, (src, dst) in enumerate(
            (
                (right_hbm, v0),
                (weight_hbm, weight),
                (coeff_hbm, coeff),
                (block_hbm, block),
                (pos_hbm, pos),
                (obsw_hbm, obsw),
            )
        )
    ]
    for load in loads:
        load.start()

    def along_y(by):
        return (win + 2 * ((chip_y + by) % NYC - chip_y), tile)

    def along_z(by, other_core=False):
        start = win + 1 - 2 * core if other_core else win
        return (start + 16 * ((chip_z + by) % NZ - chip_z), tile)

    slot_a = core * NT + tile
    near = [
        (win - core + ((slot_a + i) % 8) // NT, ((slot_a + i) % 8) % NT) for i in range(1, NCORE * NT)
    ]
    near += [along_y(1), along_y(-1)]
    near += [along_z(by, other) for by in (1, -1) for other in (False, True)]

    def signal(semaphore, peer):
        pl.semaphore_signal(semaphore, inc=1, device_id=peer, device_id_type=MESH)

    barrier = pltpu.get_barrier_semaphore()

    @pl.when(has_prev)
    def _():
        signal(barrier, prev_id)

    @pl.when(has_next)
    def _():
        signal(barrier, next_id)

    for peer in near:
        signal(barrier, peer)

    for i in range(2):
        loads[i].wait()
    for side, row in ROWS:
        for l in range(LEV):
            edge[0, l, side] = v0[l, row : row + 1, :]
            weight_edge[l, side] = weight[l, row : row + 1, :]

    pl.semaphore_wait(barrier, len(near) + jnp.where(has_prev, 1, 0) + jnp.where(has_next, 1, 0))

    started = []

    def remote(src, dst, send, recv, peer):
        return pltpu.make_async_remote_copy(
            src_ref=src, dst_ref=dst, send_sem=send, recv_sem=recv, device_id=peer, device_id_type=MESH
        )

    def start_if(condition, copies):
        @pl.when(condition)
        def _():
            for copy in copies:
                copy.start()

        started.append((condition, copies))

    def wait_if(condition, copies):
        @pl.when(condition)
        def _():
            for copy in copies:
                copy.wait_recv()

    def message(kind, j, l):
        src, dst, peer = {
            HALO_N: (edge.at[j, l, 1], halo_n.at[j, l], south_id),
            HALO_S: (edge.at[j, l, 0], halo_s.at[j, l], north_id),
            EDGE: (edge.at[j, l], next_edge.at[j, l], prev_id),
            STATE: (states[j].at[l], next_state.at[j, l], prev_id),
            IMAGE: (image.at[j, l], before.at[j, l], next_id),
            IMAGE_EDGE: (image_edge.at[j, l], before_edge.at[j, l], next_id),
            ADJ_N: (adj_edge.at[j, l, 1], adj_n.at[j, l], south_id),
            ADJ_S: (adj_edge.at[j, l, 0], adj_s.at[j, l], north_id),
        }[kind]
        return remote(src, dst, send_sem.at[j, l, kind], recv_sem.at[j, l, kind], peer)

    def weight_messages(l):
        return [
            remote(weight_edge.at[l], next_weight_edge.at[l], wsend_sem.at[l, 0], wrecv_sem.at[l, 0], prev_id),
            remote(weight.at[l], next_weight.at[l], wsend_sem.at[l, 1], wrecv_sem.at[l, 1], prev_id),
        ]

    row_id = lax.broadcasted_iota(jnp.int32, (8, NX), 0)
    first_row, last_row = row_id == 0, row_id == 7

    def rows(b):
        return slice(8 * b, 8 * b + 8)

    def vertical(ref, l, b):
        here = ref[l, rows(b), :]
        above = pltpu.roll(ref[l, rows(b - 1), :], 1, 0) if b > 0 else 0.0
        below = pltpu.roll(ref[l, rows(b + 1), :], 7, 0) if b < BLOCKS - 1 else 0.0
        north = jnp.where(first_row, above, pltpu.roll(here, 1, 0))
        south = jnp.where(last_row, below, pltpu.roll(here, 7, 0))
        return north + south

    def send_and_propagate(j, l):
        v = states[j]
        start_if(has_south, [message(HALO_N, j, l)])
        start_if(has_north, [message(HALO_S, j, l)])
        back = [message(EDGE, j, l), message(STATE, j, l)]
        if j == 0:
            small, large = weight_messages(l)
            back = [back[0], small, back[1], large]
        start_if(has_prev, back)
        if j == 0 and l == 0:
            loads[2].wait()
        for b in range(BLOCKS):
            here = v[l, rows(b), :]
            image[j, l, rows(b), :] = (
                coeff[0, l, rows(b), :] * here
                + coeff[1, l, rows(b), :] * vertical(v, l, b)
                + coeff[2, l, rows(b), :] * pltpu.roll(here, NX - 1, 1)
                + coeff[3, l, rows(b), :] * pltpu.roll(here, 1, 1)
            )
        start_if(has_next, [message(IMAGE, j, l)])

    edge_follow = {}

    def exchange_edges(j, l):
        wait_if(has_north, [message(HALO_N, j, l)])
        wait_if(has_south, [message(HALO_S, j, l)])
        for side, row in ROWS:
            halo = (halo_n, halo_s)[side]
            image_edge[j, l, side] = coeff[1, l, row : row + 1, :] * halo[j, l]
        start_if(has_next, [message(IMAGE_EDGE, j, l)])
        wait_if(has_next, [message(EDGE, j, l), *(weight_messages(l)[:1] if j == 0 else [])])
        for side, row in ROWS:
            f = next_weight_edge[l, side] * (
                next_edge[j, l, side] - (image[j, l, row : row + 1, :] + image_edge[j, l, side])
            )
            edge_follow[j, l, side] = f
            adj_edge[j, l, side] = coeff[1, l, row : row + 1, :] * f
        start_if(has_south, [message(ADJ_N, j, l)])
        start_if(has_north, [message(ADJ_S, j, l)])

    def complete(j, l):
        v, out = states[j], states[j + 1]
        wait_if(has_next, [message(STATE, j, l), *(weight_messages(l)[1:] if j == 0 else [])])
        for b in range(BLOCKS):
            f = next_weight[l, rows(b), :] * (next_state[j, l, rows(b), :] - image[j, l, rows(b), :])
            follow[l, rows(b), :] = f
            spread[l, rows(b), :] = coeff[1, l, rows(b), :] * f
        for side, row in ROWS:
            follow[l, row : row + 1, :] = edge_follow[j, l, side]
            spread[l, row : row + 1, :] = adj_edge[j, l, side]
        for b in range(BLOCKS):
            f = follow[l, rows(b), :]
            back_image = (
                coeff[0, l, rows(b), :] * f
                + vertical(spread, l, b)
                + pltpu.roll(coeff[2, l, rows(b), :] * f, 1, 1)
                + pltpu.roll(coeff[3, l, rows(b), :] * f, NX - 1, 1)
            )
            here = v[l, rows(b), :]
            out[l, rows(b), :] = weight[l, rows(b), :] * here - back_image + diag[l, rows(b), :] * here
        wait_if(has_north, [message(ADJ_N, j, l)])
        wait_if(has_south, [message(ADJ_S, j, l)])
        wait_if(has_prev, [message(IMAGE_EDGE, j, l), message(IMAGE, j, l)])
        for b in range(BLOCKS):
            out[l, rows(b), :] = SCALE * (
                out[l, rows(b), :] - weight[l, rows(b), :] * before[j, l, rows(b), :]
            )
        for side, row in ROWS:
            adj = (adj_n, adj_s)[side]
            e = out[l, row : row + 1, :] - SCALE * (
                adj[j, l] + weight[l, row : row + 1, :] * before_edge[j, l, side]
            )
            out[l, row : row + 1, :] = e
            if j + 1 < STEPS:
                edge[j + 1, l, side] = e

    def gram(group, l):
        indices = range(3 * group, 3 * group + 3)
        zero = jnp.zeros((8, 128), F32)

        def step(b, acc):
            acc = list(acc)
            at = pl.ds(pl.multiple_of(b * 8, 8), 8)
            for c in range(NX // 128):
                parts = {}
                for index in indices:
                    for s in PAIRS[index]:
                        if s not in parts:
                            x = states[s][l, at, c * 128 : (c + 1) * 128]
                            parts[s] = (x, split(x))
                for n, index in enumerate(indices):
                    i, k = PAIRS[index]
                    p, e = two_prod_split(parts[i][0], parts[k][0], parts[i][1], parts[k][1])
                    s, f = two_sum(acc[2 * n], p)
                    acc[2 * n], acc[2 * n + 1] = s, acc[2 * n + 1] + (e + f)
            return tuple(acc)

        acc = lax.fori_loop(0, BLOCKS, step, (zero,) * 6)
        for n, index in enumerate(indices):
            part = quick_sum(acc[2 * n], acc[2 * n + 1])
            if l > 0:
                part = add2(part, (gram_high[index], gram_low[index]))
            gram_high[index], gram_low[index] = part

    def over_rows(index):
        total = (gram_high[index], gram_low[index])
        for shift in (4, 2, 1):
            total = add2(total, rolled(total, shift, 0))
        return total[0][0:1, :], total[1][0:1, :]

    def observed_weights():
        pos_t = jnp.swapaxes(pos[...], 0, 1)
        obsw_t = jnp.swapaxes(obsw[...], 0, 1)
        lane = lax.broadcasted_iota(jnp.int32, (128, 128), 1)
        lines = []
        for b in range(32):
            hit = pos_t[:, b : b + 1] == lane
            lines.append(jnp.sum(jnp.where(hit, obsw_t[:, b : b + 1], 0.0), axis=0, keepdims=True))
        per_block = jnp.concatenate(lines, axis=0)
        row = lax.broadcasted_iota(jnp.int32, (LEV * TY, 32), 0)
        for c in range(NX // 128):
            hot = (block[...] == row * (NX // 128) + c).astype(F32)
            out = jnp.dot(hot, per_block, precision=lax.Precision.HIGHEST, preferred_element_type=F32)
            for l in range(LEV):
                diag[l, :, c * 128 : (c + 1) * 128] = out[l * TY : (l + 1) * TY, :]

    def zeros(*refs):
        for ref in refs:
            ref[...] = jnp.zeros_like(ref)

    for l in range(LEV):
        send_and_propagate(0, l)
    for at, move in enumerate((along_y, along_z)):
        for by in (1, -1):
            signal(known_sem.at[at, 0], move(by))
    pl.when(jnp.logical_not(has_north))(lambda: zeros(halo_n, adj_n))
    pl.when(jnp.logical_not(has_south))(lambda: zeros(halo_s, adj_s))
    pl.when(jnp.logical_not(has_prev))(lambda: zeros(before, before_edge))
    pl.when(jnp.logical_not(has_next))(lambda: zeros(next_edge, next_weight_edge, next_state, next_weight))
    for load in loads[3:]:
        load.wait()
    observed_weights()
    for at, move in enumerate((along_y, along_z)):
        pl.semaphore_wait(known_sem.at[at, 0], 2)
        for by in (2, -2):
            signal(known_sem.at[at, 1], move(by))
    for l in range(LEV):
        exchange_edges(0, l)
    for j in range(STEPS):
        for l in range(LEV):
            complete(j, l)
            if j + 1 < STEPS:
                send_and_propagate(j + 1, l)
            else:
                gram(2, l)
        if j + 1 < STEPS:
            if j == 0:
                for at in range(2):
                    pl.semaphore_wait(known_sem.at[at, 1], 2)
            for l in range(LEV):
                gram(j, l)
            for l in range(LEV):
                exchange_edges(j + 1, l)

    lines = [over_rows(index) for index in range(len(PAIRS))]
    blank = jnp.zeros((16 - len(PAIRS), 128), F32)
    stacked = jnp.concatenate([*(x for x, _ in lines), blank, *(x for _, x in lines), blank], axis=0)
    turned = jnp.swapaxes(jnp.concatenate([stacked, jnp.zeros((96, 128), F32)], axis=0), 0, 1)
    pieces = [turned[8 * i : 8 * i + 8, :] for i in range(16)]
    total = tree2([(x, pltpu.roll(x, 128 - 16, 1)) for x in pieces])
    for shift in (4, 2, 1):
        total = add2(total, rolled(total, shift, 0))
    lane = lax.broadcasted_iota(jnp.int32, (1, 128), 1)

    def packed(pair):
        return jnp.where(lane < 16, pair[0], jnp.where(lane < 32, pltpu.roll(pair[1], 16, 1), 0.0))

    line = packed((total[0][0:1, :], total[1][0:1, :]))

    def received(stage):
        parts = [row_recv[stage, i] for i in range(8)]
        return tree2([(x, pltpu.roll(x, 128 - 16, 1)) for x in parts])

    def to_x(i, other):
        return remote(
            row_send.at[0], row_recv.at[0, i], rsend_sem.at[0, other], rrecv_sem.at[0, i], (win - core + 1, other)
        )

    def to_y(by):
        return remote(
            row_send.at[1], row_recv.at[1, chip_y], rsend_sem.at[1, by], rrecv_sem.at[1, by], along_y(by)
        )

    def to_z(by, other_core):
        at = by + 8 * other_core
        return remote(
            row_send.at[2], row_recv.at[2, chip_z], rsend_sem.at[2, at], rrecv_sem.at[2, at], along_z(by, other_core)
        )

    is_second = core == 1
    row_send[0] = line
    for other in range(NT):
        condition = jnp.logical_or(core == 0, tile != other)
        start_if(condition, [to_x(slot_a, other)])

    @pl.when(is_second)
    def _():
        row_recv[0, slot_a] = line
        for i in range(NCORE * NT):

            @pl.when(slot_a != i)
            def _(i=i):
                to_x(i, 0).wait_recv()

        mine = packed(received(0))
        row_send[1] = mine
        row_recv[1, chip_y] = mine
        for by in range(1, NYC):
            to_y(by).start()
        for by in range(1, NYC):
            to_y(by).wait_recv()
        mine = packed(received(1))
        row_send[2] = mine
        row_recv[2, chip_z] = mine
        for by in range(1, NZ):
            to_z(by, True).start()
            to_z(by, False).start()
        to_z(0, True).start()
        for by in range(1, NZ):
            to_z(by, False).wait_recv()

    @pl.when(jnp.logical_not(is_second))
    def _():
        for by in range(NZ):
            to_z(by, True).wait_recv()

    total = received(2)
    line = packed(total)

    def value(i, j):
        at = PAIRS.index((min(i, j), max(i, j)))
        return tuple(jnp.broadcast_to(line[:, at + off : at + off + 1], (8, 128)) for off in (0, 16))

    a = [[value(i, n + 1) for n in range(3)] + [value(i, 0)] for i in range(3)]
    for pivot in range(2):
        for i in range(pivot + 1, 3):
            factor = div2(a[i][pivot], a[pivot][pivot])
            for n in range(pivot + 1, 4):
                a[i][n] = sub2(a[i][n], mul2(factor, a[pivot][n]))
    c2 = div2(a[2][3], a[2][2])
    c1 = div2(sub2(a[1][3], mul2(a[1][2], c2)), a[1][1])
    c0 = div2(sub2(sub2(a[0][3], mul2(a[0][1], c1)), mul2(a[0][2], c2)), a[0][0])
    combo = [jnp.concatenate([c[0]] * (NX // 128), axis=1) for c in (c0, c1, c2)]
    for l in range(LEV):
        for b in range(BLOCKS):
            at = (l, rows(b), slice(None))
            u0, u1, u2, u3 = (s[at] for s in states)
            solution_out[0, l, rows(b), :] = SCALE * (combo[0] * u0 + combo[1] * u1 + combo[2] * u2)
            residual_out[0, l, rows(b), :] = u0 - combo[0] * u1 - combo[1] * u2 - combo[2] * u3

    for condition, copies in started:

        @pl.when(condition)
        def _(copies=copies):
            for copy in copies:
                copy.wait_send()

    @pl.when(is_second)
    def _():
        for by in range(1, NYC):
            to_y(by).wait_send()
        for by in range(1, NZ):
            to_z(by, True).wait_send()
            to_z(by, False).wait_send()
        to_z(0, True).wait_send()


def on_device(right_side, error_weight, coeffs, obs_block, obs_pos, obs_weight):
    shape = (LEV, TY, NX)
    vmem, hbm = pltpu.VMEM, pltpu.HBM
    line = (STEPS, LEV, 2, 1, NX)
    half = (STEPS, LEV, 1, NX)
    scratch = [
        vmem(shape, F32),
        vmem(shape, F32),
        vmem(shape, F32),
        vmem(shape, F32),
        vmem(shape, F32),
        vmem((4, *shape), F32),
        vmem((1, 32), jnp.int32),
        vmem((32, 128), jnp.int32),
        vmem((32, 128), F32),
        vmem(shape, F32),
        vmem(line, F32),
        vmem(line[1:], F32),
        vmem(half, F32),
        vmem(half, F32),
        vmem(line, F32),
        vmem(line[1:], F32),
        vmem((STEPS, *shape), F32),
        vmem(shape, F32),
        vmem((STEPS, *shape), F32),
        vmem((STEPS, *shape), F32),
        vmem(line, F32),
        vmem(line, F32),
        vmem(line, F32),
        vmem(half, F32),
        vmem(half, F32),
        vmem(shape, F32),
        vmem(shape, F32),
        vmem((len(PAIRS), 8, 128), F32),
        vmem((len(PAIRS), 8, 128), F32),
        vmem((3, 1, 128), F32),
        vmem((3, 8, 1, 128), F32),
        pltpu.SemaphoreType.DMA((6,)),
        pltpu.SemaphoreType.DMA((STEPS, LEV, MESSAGES)),
        pltpu.SemaphoreType.DMA((STEPS, LEV, MESSAGES)),
        pltpu.SemaphoreType.DMA((LEV, 2)),
        pltpu.SemaphoreType.DMA((LEV, 2)),
        pltpu.SemaphoreType.DMA((3, 16)),
        pltpu.SemaphoreType.DMA((3, 16)),
        pltpu.SemaphoreType.REGULAR((2, 2)),
    ]
    return pl.pallas_call(
        kernel,
        out_shape=(pltpu.VMEM((1, *shape), F32), pltpu.VMEM((1, *shape), F32)),
        in_specs=[pl.BlockSpec(memory_space=hbm)] * 6,
        out_specs=(pl.BlockSpec(memory_space=vmem),) * 2,
        scratch_shapes=scratch,
        compiler_params=pltpu.CompilerParams(collective_id=0, has_side_effects=True),
        name="krylov",
    )(
        right_side.reshape(shape),
        error_weight.reshape(shape),
        coeffs.reshape(4, *shape),
        obs_block,
        obs_pos.reshape(32, 128),
        obs_weight.reshape(32, 128),
    )


def solution(mesh):
    in_specs = (
        P("win", None, "tile", None),
        P("win", None, "tile", None),
        P(None, "win", None, "tile", None),
        P("win", "tile"),
        P("win", "tile", None),
        P("win", "tile", None),
    )
    out_specs = (P("win", None, "tile", None), P("win", None, "tile", None))
    return jax.shard_map(on_device, mesh=mesh, in_specs=in_specs, out_specs=out_specs, check_vma=False)
```

```python
import jax
import jax.numpy as jnp
from jax import lax
from jax.experimental import pallas as pl
from jax.experimental.pallas import tpu as pltpu
from jax.sharding import PartitionSpec as P

MESH = pl.DeviceIdType.MESH
F32 = jnp.float32
LEV, TY, NX = 2, 32, 1024
BLOCKS = TY // 8
STEPS = 3
SCALE = 1.0 / 16.0
NZ, NYC, NCORE, NT = 8, 8, 2, 4
NWIN = NZ * NYC * NCORE
PLANE = NYC * NCORE * NT
PAIRS = ((0, 0), (0, 1), (1, 1), (0, 2), (1, 2), (2, 2), (0, 3), (1, 3), (2, 3))
HALO_N, HALO_S, EDGE, STATE, IMAGE, IMAGE_EDGE, ADJ_N, ADJ_S = range(8)
MESSAGES = 8
TOWARDS = (0, 1, 2, 2, 3, 3, 0, 1)
BACK_ROWS = (STEPS + 1) * (LEV * TY + 2 * LEV) * NX // 128
AHEAD_ROWS = STEPS * (LEV * TY + 2 * LEV) * NX // 128
SIDE_ROWS = STEPS * 2 * LEV * NX // 128
ROWS = ((0, 0), (1, TY - 1))


def two_sum(a, b):
    s = a + b
    t = s - a
    return s, (a - (s - t)) + (b - t)


def quick_sum(a, b):
    s = a + b
    return s, b - (s - a)


def split(a):
    c = a * 4097.0
    high = c - (c - a)
    return high, a - high


def two_prod_split(a, b, sa, sb):
    p = a * b
    return p, ((sa[0] * sb[0] - p) + sa[0] * sb[1] + sa[1] * sb[0]) + sa[1] * sb[1]


def two_prod(a, b):
    return two_prod_split(a, b, split(a), split(b))


def add2(a, b):
    s, e = two_sum(a[0], b[0])
    return quick_sum(s, e + (a[1] + b[1]))


def neg2(a):
    return -a[0], -a[1]


def sub2(a, b):
    return add2(a, neg2(b))


def mul2(a, b):
    p, e = two_prod(a[0], b[0])
    return quick_sum(p, e + (a[0] * b[1] + a[1] * b[0]))


def div2(a, b):
    zero = jnp.zeros_like(a[0])
    first = a[0] / b[0]
    rest = sub2(a, mul2((first, zero), b))
    return quick_sum(first, rest[0] / b[0])


def tree2(items):
    while len(items) > 1:
        items = [
            add2(items[i], items[i + 1]) if i + 1 < len(items) else items[i]
            for i in range(0, len(items), 2)
        ]
    return items[0]


def rolled(pair, shift, axis):
    return pltpu.roll(pair[0], shift, axis), pltpu.roll(pair[1], shift, axis)


def kernel(
    right_hbm,
    weight_hbm,
    coeff_hbm,
    block_hbm,
    pos_hbm,
    obsw_hbm,
    solution_out,
    residual_out,
    v0,
    v1,
    v2,
    v3,
    weight,
    coeff,
    block,
    pos,
    obsw,
    diag,
    edge,
    weight_edge,
    halo_n,
    halo_s,
    next_edge,
    next_weight_edge,
    next_state,
    next_weight,
    image,
    before,
    image_edge,
    before_edge,
    adj_edge,
    adj_n,
    adj_s,
    follow,
    spread,
    gram_high,
    gram_low,
    row_send,
    row_recv,
    plane_recv,
    local_sem,
    send_sem,
    recv_sem,
    wrecv_sem,
    rrecv_sem,
    known_sem,
    ballast,
):
    win = lax.axis_index("win")
    tile = lax.axis_index("tile")
    core = win % 2
    chip_y = (win // 2) % 8
    chip_z = win // 16
    has_prev, has_next = win > 0, win < NWIN - 1
    has_north, has_south = tile > 0, tile < NT - 1
    prev_id, next_id = (win - 1, tile), (win + 1, tile)
    north_id, south_id = (win, tile - 1), (win, tile + 1)
    states = (v0, v1, v2, v3)

    loads = [
        pltpu.make_async_copy(src, dst, local_sem.at[i])
        for i, (src, dst) in enumerate(
            (
                (right_hbm, v0),
                (weight_hbm, weight),
                (coeff_hbm, coeff),
                (block_hbm, block),
                (pos_hbm, pos),
                (obsw_hbm, obsw),
            )
        )
    ]
    for load in loads:
        load.start()

    def along_y(by):
        return (win + 2 * ((chip_y + by) % NYC - chip_y), tile)

    def along_z(by, other_core=False):
        start = win + 1 - 2 * core if other_core else win
        return (start + 16 * ((chip_z + by) % NZ - chip_z), tile)

    group = core * NT + tile
    slot_a = chip_y * 8 + group
    near = [
        (win - core + ((group + i) % 8) // NT, (group + i) % NT) for i in range(1, NCORE * NT)
    ]
    near += [along_y(1), along_y(-1)]
    near += [along_z(by, other) for by in (1, -1) for other in (False, True)]

    def signal(semaphore, peer):
        pl.semaphore_signal(semaphore, inc=1, device_id=peer, device_id_type=MESH)

    barrier = pltpu.get_barrier_semaphore()

    @pl.when(has_prev)
    def _():
        signal(barrier, prev_id)

    @pl.when(has_next)
    def _():
        signal(barrier, next_id)

    for peer in near:
        signal(barrier, peer)

    for i in range(2):
        loads[i].wait()
    for side, row in ROWS:
        for l in range(LEV):
            edge[0, l, side] = v0[l, row : row + 1, :]
            weight_edge[l, side] = weight[l, row : row + 1, :]

    pl.semaphore_wait(barrier, len(near) + jnp.where(has_prev, 1, 0) + jnp.where(has_next, 1, 0))

    def remote(src, dst, send, recv, peer):
        return pltpu.make_async_remote_copy(
            src_ref=src, dst_ref=dst, send_sem=send, recv_sem=recv, device_id=peer, device_id_type=MESH
        )

    def start_if(condition, copies):
        @pl.when(condition)
        def _():
            for copy in copies:
                copy.start()

    def wait_if(condition, copies):
        @pl.when(condition)
        def _():
            for copy in copies:
                copy.wait_recv()

    def message(kind, j, l):
        src, dst, peer = {
            HALO_N: (edge.at[j, l, 1], halo_n.at[j, l], south_id),
            HALO_S: (edge.at[j, l, 0], halo_s.at[j, l], north_id),
            EDGE: (edge.at[j, l], next_edge.at[j, l], prev_id),
            STATE: (states[j].at[l], next_state.at[j, l], prev_id),
            IMAGE: (image.at[j, l], before.at[j, l], next_id),
            IMAGE_EDGE: (image_edge.at[j, l], before_edge.at[j, l], next_id),
            ADJ_N: (adj_edge.at[j, l, 1], adj_n.at[j, l], south_id),
            ADJ_S: (adj_edge.at[j, l, 0], adj_s.at[j, l], north_id),
        }[kind]
        return remote(src, dst, send_sem.at[TOWARDS[kind]], recv_sem.at[j % 2, l, kind], peer)

    def weight_messages(l):
        return [
            remote(weight_edge.at[l], next_weight_edge.at[l], send_sem.at[2], wrecv_sem.at[l, 0], prev_id),
            remote(weight.at[l], next_weight.at[l], send_sem.at[2], wrecv_sem.at[l, 1], prev_id),
        ]

    row_id = lax.broadcasted_iota(jnp.int32, (8, NX), 0)
    first_row, last_row = row_id == 0, row_id == 7

    def rows(b):
        return slice(8 * b, 8 * b + 8)

    def vertical(ref, l, b):
        here = ref[l, rows(b), :]
        above = pltpu.roll(ref[l, rows(b - 1), :], 1, 0) if b > 0 else 0.0
        below = pltpu.roll(ref[l, rows(b + 1), :], 7, 0) if b < BLOCKS - 1 else 0.0
        north = jnp.where(first_row, above, pltpu.roll(here, 1, 0))
        south = jnp.where(last_row, below, pltpu.roll(here, 7, 0))
        return north + south

    def send_and_propagate(j, l):
        v = states[j]
        start_if(has_south, [message(HALO_N, j, l)])
        start_if(has_north, [message(HALO_S, j, l)])
        back = [message(EDGE, j, l), message(STATE, j, l)]
        if j == 0:
            edges = [x for n in range(LEV) for x in (message(EDGE, 0, n), weight_messages(n)[0])]
            back = [*(edges if l == 0 else []), back[1], weight_messages(l)[1]]
        start_if(has_prev, back)
        if j == 0 and l == 0:
            loads[2].wait()
        for b in range(BLOCKS):
            here = v[l, rows(b), :]
            image[j, l, rows(b), :] = (
                coeff[0, l, rows(b), :] * here
                + coeff[1, l, rows(b), :] * vertical(v, l, b)
                + coeff[2, l, rows(b), :] * pltpu.roll(here, NX - 1, 1)
                + coeff[3, l, rows(b), :] * pltpu.roll(here, 1, 1)
            )
        start_if(has_next, [message(IMAGE, j, l)])

    edge_follow = {}

    def exchange_edges(j, l):
        wait_if(has_north, [message(HALO_N, j, l)])
        wait_if(has_south, [message(HALO_S, j, l)])
        for side, row in ROWS:
            halo = (halo_n, halo_s)[side]
            image_edge[j, l, side] = coeff[1, l, row : row + 1, :] * halo[j, l]
        start_if(has_next, [message(IMAGE_EDGE, j, l)])
        wait_if(has_next, [message(EDGE, j, l), *(weight_messages(l)[:1] if j == 0 else [])])
        for side, row in ROWS:
            f = next_weight_edge[l, side] * (
                next_edge[j, l, side] - (image[j, l, row : row + 1, :] + image_edge[j, l, side])
            )
            edge_follow[j, l, side] = f
            adj_edge[j, l, side] = coeff[1, l, row : row + 1, :] * f
        start_if(has_south, [message(ADJ_N, j, l)])
        start_if(has_north, [message(ADJ_S, j, l)])

    def complete(j, l):
        v, out = states[j], states[j + 1]
        wait_if(has_next, [message(STATE, j, l), *(weight_messages(l)[1:] if j == 0 else [])])
        for b in range(BLOCKS):
            f = next_weight[l, rows(b), :] * (next_state[j, l, rows(b), :] - image[j, l, rows(b), :])
            follow[l, rows(b), :] = f
            spread[l, rows(b), :] = coeff[1, l, rows(b), :] * f
        for side, row in ROWS:
            follow[l, row : row + 1, :] = edge_follow[j, l, side]
            spread[l, row : row + 1, :] = adj_edge[j, l, side]
        for b in range(BLOCKS):
            f = follow[l, rows(b), :]
            back_image = (
                coeff[0, l, rows(b), :] * f
                + vertical(spread, l, b)
                + pltpu.roll(coeff[2, l, rows(b), :] * f, 1, 1)
                + pltpu.roll(coeff[3, l, rows(b), :] * f, NX - 1, 1)
            )
            here = v[l, rows(b), :]
            out[l, rows(b), :] = weight[l, rows(b), :] * here - back_image + diag[l, rows(b), :] * here
        wait_if(has_north, [message(ADJ_N, j, l)])
        wait_if(has_south, [message(ADJ_S, j, l)])
        wait_if(has_prev, [message(IMAGE_EDGE, j, l), message(IMAGE, j, l)])
        for b in range(BLOCKS):
            out[l, rows(b), :] = SCALE * (
                out[l, rows(b), :] - weight[l, rows(b), :] * before[j, l, rows(b), :]
            )
        for side, row in ROWS:
            adj = (adj_n, adj_s)[side]
            e = out[l, row : row + 1, :] - SCALE * (
                adj[j, l] + weight[l, row : row + 1, :] * before_edge[j, l, side]
            )
            out[l, row : row + 1, :] = e
            if j + 1 < STEPS:
                edge[j + 1, l, side] = e

    def gram(group, l):
        indices = range(3 * group, 3 * group + 3)
        zero = jnp.zeros((8, 128), F32)

        def step(b, acc):
            acc = list(acc)
            at = pl.ds(pl.multiple_of(b * 8, 8), 8)
            for c in range(NX // 128):
                parts = {}
                for index in indices:
                    for s in PAIRS[index]:
                        if s not in parts:
                            x = states[s][l, at, c * 128 : (c + 1) * 128]
                            parts[s] = (x, split(x))
                for n, index in enumerate(indices):
                    i, k = PAIRS[index]
                    p, e = two_prod_split(parts[i][0], parts[k][0], parts[i][1], parts[k][1])
                    s, f = two_sum(acc[2 * n], p)
                    acc[2 * n], acc[2 * n + 1] = s, acc[2 * n + 1] + (e + f)
            return tuple(acc)

        acc = lax.fori_loop(0, BLOCKS, step, (zero,) * 6)
        for n, index in enumerate(indices):
            part = quick_sum(acc[2 * n], acc[2 * n + 1])
            if l > 0:
                part = add2(part, (gram_high[index], gram_low[index]))
            gram_high[index], gram_low[index] = part

    def over_rows(index):
        total = (gram_high[index], gram_low[index])
        for shift in (4, 2, 1):
            total = add2(total, rolled(total, shift, 0))
        return total[0][0:1, :], total[1][0:1, :]

    def observed_weights():
        pos_t = jnp.swapaxes(pos[...], 0, 1)
        obsw_t = jnp.swapaxes(obsw[...], 0, 1)
        lane = lax.broadcasted_iota(jnp.int32, (128, 128), 1)
        lines = []
        for b in range(32):
            hit = pos_t[:, b : b + 1] == lane
            lines.append(jnp.sum(jnp.where(hit, obsw_t[:, b : b + 1], 0.0), axis=0, keepdims=True))
        per_block = jnp.concatenate(lines, axis=0)
        row = lax.broadcasted_iota(jnp.int32, (LEV * TY, 32), 0)
        for c in range(NX // 128):
            hot = (block[...] == row * (NX // 128) + c).astype(F32)
            out = jnp.dot(hot, per_block, precision=lax.Precision.HIGHEST, preferred_element_type=F32)
            for l in range(LEV):
                diag[l, :, c * 128 : (c + 1) * 128] = out[l * TY : (l + 1) * TY, :]

    def zeros(*refs):
        for ref in refs:
            ref[...] = jnp.zeros_like(ref)

    for l in range(LEV):
        send_and_propagate(0, l)
    for at, move in enumerate((along_y, along_z)):
        for by in (1, -1):
            signal(known_sem.at[at, 0], move(by))
    pl.when(jnp.logical_not(has_north))(lambda: zeros(halo_n, adj_n))
    pl.when(jnp.logical_not(has_south))(lambda: zeros(halo_s, adj_s))
    pl.when(jnp.logical_not(has_prev))(lambda: zeros(before, before_edge))
    pl.when(jnp.logical_not(has_next))(lambda: zeros(next_edge, next_weight_edge, next_state, next_weight))
    for load in loads[3:]:
        load.wait()
    observed_weights()
    for at, move in enumerate((along_y, along_z)):
        pl.semaphore_wait(known_sem.at[at, 0], 2)
        for by in (2, -2):
            signal(known_sem.at[at, 1], move(by))
    for l in range(LEV):
        exchange_edges(0, l)
    for j in range(STEPS):
        for l in range(LEV):
            complete(j, l)
            if j + 1 < STEPS:
                send_and_propagate(j + 1, l)
            else:
                gram(2, l)
        if j + 1 < STEPS:
            for at, move in enumerate((along_y, along_z)):
                pl.semaphore_wait(known_sem.at[at, j + 1], 2)
                for by in (1, -1) if j == 0 else ():
                    signal(known_sem.at[at, 2], move(by))
            for l in range(LEV):
                gram(j, l)
            for l in range(LEV):
                exchange_edges(j + 1, l)

    lines = [over_rows(index) for index in range(len(PAIRS))]
    blank = jnp.zeros((16 - len(PAIRS), 128), F32)
    stacked = jnp.concatenate([*(x for x, _ in lines), blank, *(x for _, x in lines), blank], axis=0)
    turned = jnp.swapaxes(jnp.concatenate([stacked, jnp.zeros((96, 128), F32)], axis=0), 0, 1)
    pieces = [turned[8 * i : 8 * i + 8, :] for i in range(16)]
    total = tree2([(x, pltpu.roll(x, 128 - 16, 1)) for x in pieces])
    for shift in (4, 2, 1):
        total = add2(total, rolled(total, shift, 0))
    lane = lax.broadcasted_iota(jnp.int32, (1, 128), 1)

    def packed(pair):
        return jnp.where(lane < 16, pair[0], jnp.where(lane < 32, pltpu.roll(pair[1], 16, 1), 0.0))

    line = packed((total[0][0:1, :], total[1][0:1, :]))

    def over_slots(parts):
        total = tree2([(x, pltpu.roll(x, 128 - 16, 1)) for x in parts])
        for shift in (4, 2, 1):
            total = add2(total, rolled(total, shift, 0))
        return total[0][0:1, :], total[1][0:1, :]

    def arrived(stage, count):
        whole = ballast.at[pl.ds(0, count)]
        pltpu.make_async_copy(whole, whole, rrecv_sem.at[stage]).wait()

    def to_plane(by, x_by):
        where = (along_y(by)[0] - core + 1, (tile + x_by) % NT)
        return remote(
            row_send.at[0], plane_recv.at[pl.ds(slot_a, 1)], send_sem.at[4], rrecv_sem.at[0], where
        )

    def to_z(by, other_core):
        return remote(
            row_send.at[1], row_recv.at[chip_z], send_sem.at[5], rrecv_sem.at[1], along_z(by, other_core)
        )

    is_second = core == 1
    row_send[0] = line
    for by in (4, 3, 5, 2, 6, 1, 7, 0):
        for other in (2, 1, 3, 0):
            copy = to_plane(by, other)
            if by == 0 and other == 0:
                pl.when(core == 0)(copy.start)
            else:
                copy.start()

    @pl.when(is_second)
    def _():
        plane_recv[pl.ds(slot_a, 1), :] = line
        arrived(0, PLANE - 1)
        mine = packed(over_slots([plane_recv[8 * i : 8 * i + 8, :] for i in range(PLANE // 8)]))
        row_send[1] = mine
        row_recv[chip_z] = mine
        for by in range(1, NZ):
            to_z(by, True).start()
            to_z(by, False).start()
        to_z(0, True).start()
        arrived(1, NZ - 1)

    @pl.when(jnp.logical_not(is_second))
    def _():
        arrived(1, NZ)

    total = tree2([(x, pltpu.roll(x, 128 - 16, 1)) for x in [row_recv[i] for i in range(NZ)]])
    line = packed(total)

    def value(i, j):
        at = PAIRS.index((min(i, j), max(i, j)))
        return tuple(jnp.broadcast_to(line[:, at + off : at + off + 1], (8, 128)) for off in (0, 16))

    a = [[value(i, n + 1) for n in range(3)] + [value(i, 0)] for i in range(3)]
    for pivot in range(2):
        for i in range(pivot + 1, 3):
            factor = div2(a[i][pivot], a[pivot][pivot])
            for n in range(pivot + 1, 4):
                a[i][n] = sub2(a[i][n], mul2(factor, a[pivot][n]))
    c2 = div2(a[2][3], a[2][2])
    c1 = div2(sub2(a[1][3], mul2(a[1][2], c2)), a[1][1])
    c0 = div2(sub2(sub2(a[0][3], mul2(a[0][1], c1)), mul2(a[0][2], c2)), a[0][0])
    combo = [jnp.concatenate([c[0]] * (NX // 128), axis=1) for c in (c0, c1, c2)]
    for l in range(LEV):
        for b in range(BLOCKS):
            at = (l, rows(b), slice(None))
            u0, u1, u2, u3 = (s[at] for s in states)
            solution_out[0, l, rows(b), :] = SCALE * (combo[0] * u0 + combo[1] * u1 + combo[2] * u2)
            residual_out[0, l, rows(b), :] = u0 - combo[0] * u1 - combo[1] * u2 - combo[2] * u3

    def sent(condition, count, semaphore):
        @pl.when(condition)
        def _():
            whole = ballast.at[pl.ds(0, count)]
            pltpu.make_async_copy(whole, whole, semaphore).wait()

    sent(has_south, SIDE_ROWS, send_sem.at[0])
    sent(has_north, SIDE_ROWS, send_sem.at[1])
    sent(has_prev, BACK_ROWS, send_sem.at[2])
    sent(has_next, AHEAD_ROWS, send_sem.at[3])
    sent(is_second, PLANE // 2 - 1, send_sem.at[4])
    sent(jnp.logical_not(is_second), PLANE // 2, send_sem.at[4])
    sent(is_second, 2 * NZ - 1, send_sem.at[5])


def on_device(right_side, error_weight, coeffs, obs_block, obs_pos, obs_weight):
    shape = (LEV, TY, NX)
    vmem, hbm = pltpu.VMEM, pltpu.HBM
    line = (STEPS, LEV, 2, 1, NX)
    half = (STEPS, LEV, 1, NX)
    scratch = [
        vmem(shape, F32),
        vmem(shape, F32),
        vmem(shape, F32),
        vmem(shape, F32),
        vmem(shape, F32),
        vmem((4, *shape), F32),
        vmem((1, 32), jnp.int32),
        vmem((32, 128), jnp.int32),
        vmem((32, 128), F32),
        vmem(shape, F32),
        vmem(line, F32),
        vmem(line[1:], F32),
        vmem(half, F32),
        vmem(half, F32),
        vmem(line, F32),
        vmem(line[1:], F32),
        vmem((STEPS, *shape), F32),
        vmem(shape, F32),
        vmem((STEPS, *shape), F32),
        vmem((STEPS, *shape), F32),
        vmem(line, F32),
        vmem(line, F32),
        vmem(line, F32),
        vmem(half, F32),
        vmem(half, F32),
        vmem(shape, F32),
        vmem(shape, F32),
        vmem((len(PAIRS), 8, 128), F32),
        vmem((len(PAIRS), 8, 128), F32),
        vmem((2, 1, 128), F32),
        vmem((NZ, 1, 128), F32),
        vmem((PLANE, 128), F32),
        pltpu.SemaphoreType.DMA((6,)),
        pltpu.SemaphoreType.DMA((6,)),
        pltpu.SemaphoreType.DMA((2, LEV, MESSAGES)),
        pltpu.SemaphoreType.DMA((LEV, 2)),
        pltpu.SemaphoreType.DMA((2,)),
        pltpu.SemaphoreType.REGULAR((2, 3)),
        vmem((BACK_ROWS, 1, 128), F32),
    ]
    solution_field, residual = pl.pallas_call(
        kernel,
        out_shape=(pltpu.VMEM((1, *shape), F32), pltpu.VMEM((1, *shape), F32)),
        in_specs=[pl.BlockSpec(memory_space=hbm)] * 6,
        out_specs=(pl.BlockSpec(memory_space=vmem),) * 2,
        scratch_shapes=scratch,
        compiler_params=pltpu.CompilerParams(collective_id=0, has_side_effects=True),
        name="krylov",
    )(
        right_side.reshape(shape),
        error_weight.reshape(shape),
        coeffs.reshape(4, *shape),
        obs_block,
        obs_pos.reshape(32, 128),
        obs_weight.reshape(32, 128),
    )
    whole = jax.ShapeDtypeStruct((1, *shape), F32)
    return pl.pallas_call(
        store,
        out_shape=(whole, whole),
        in_specs=[pl.BlockSpec(memory_space=vmem)] * 2,
        out_specs=(pl.BlockSpec(memory_space=hbm),) * 2,
        scratch_shapes=[pltpu.SemaphoreType.DMA((2,))],
        name="store",
    )(*(pltpu.with_memory_space_constraint(x, vmem) for x in (solution_field, residual)))


def store(solution_field, residual, solution_out, residual_out, sem):
    copies = [
        pltpu.make_async_copy(solution_field, solution_out, sem.at[0]),
        pltpu.make_async_copy(residual, residual_out, sem.at[1]),
    ]
    for copy in copies:
        copy.start()
    for copy in copies:
        copy.wait()


def solution(mesh):
    in_specs = (
        P("win", None, "tile", None),
        P("win", None, "tile", None),
        P(None, "win", None, "tile", None),
        P("win", "tile"),
        P("win", "tile", None),
        P("win", "tile", None),
    )
    out_specs = (P("win", None, "tile", None), P("win", None, "tile", None))
    return jax.shard_map(on_device, mesh=mesh, in_specs=in_specs, out_specs=out_specs, check_vma=False)
```

```python
import jax
import jax.numpy as jnp
from jax import lax
from jax.experimental import pallas as pl
from jax.experimental.pallas import tpu as pltpu
from jax.sharding import PartitionSpec as P

MESH = pl.DeviceIdType.MESH
F32 = jnp.float32
LEV, TY, NX = 2, 32, 1024
BLOCKS = TY // 8
STEPS = 3
SCALE = 1.0 / 16.0
NZ, NYC, NCORE, NT = 8, 8, 2, 4
NWIN = NZ * NYC * NCORE
PLANE = NYC * NCORE * NT
PAIRS = ((0, 0), (0, 1), (1, 1), (0, 2), (1, 2), (2, 2), (0, 3), (1, 3), (2, 3))
HALO, BACK, FORE, STATE, IMAGE = 0, 2, 4, 6, 10
MESSAGES = 14
WIDE = NX // 128
SIDE_ROWS = LEV * (2 * STEPS + 4) * WIDE
BACK_ROWS = (STEPS + 1) * LEV * TY * WIDE
AHEAD_ROWS = (STEPS * LEV * TY + 2 * LEV) * WIDE
BACK_SIDE_ROWS = LEV * (STEPS + 1) * WIDE
AHEAD_SIDE_ROWS = LEV * STEPS * WIDE
EARLY = 6
OUTER = ((0, 1), (TY - 1, TY - 2))


def two_sum(a, b):
    s = a + b
    t = s - a
    return s, (a - (s - t)) + (b - t)


def quick_sum(a, b):
    s = a + b
    return s, b - (s - a)


def split(a):
    c = a * 4097.0
    high = c - (c - a)
    return high, a - high


def two_prod_split(a, b, sa, sb):
    p = a * b
    return p, ((sa[0] * sb[0] - p) + sa[0] * sb[1] + sa[1] * sb[0]) + sa[1] * sb[1]


def two_prod(a, b):
    return two_prod_split(a, b, split(a), split(b))


def add2(a, b):
    s, e = two_sum(a[0], b[0])
    return quick_sum(s, e + (a[1] + b[1]))


def neg2(a):
    return -a[0], -a[1]


def sub2(a, b):
    return add2(a, neg2(b))


def mul2(a, b):
    p, e = two_prod(a[0], b[0])
    return quick_sum(p, e + (a[0] * b[1] + a[1] * b[0]))


def div2(a, b):
    zero = jnp.zeros_like(a[0])
    first = a[0] / b[0]
    rest = sub2(a, mul2((first, zero), b))
    return quick_sum(first, rest[0] / b[0])


def plus(a, b):
    s, e = two_sum(a[0], b[0])
    return s, (a[1] + b[1]) + e


def tree2(items):
    while len(items) > 1:
        items = [
            plus(items[i], items[i + 1]) if i + 1 < len(items) else items[i]
            for i in range(0, len(items), 2)
        ]
    return items[0]


def rolled(pair, shift, axis):
    return pltpu.roll(pair[0], shift, axis), pltpu.roll(pair[1], shift, axis)


def kernel(
    right_hbm,
    weight_hbm,
    coeff_hbm,
    block_hbm,
    pos_hbm,
    obsw_hbm,
    solution_out,
    residual_out,
    v0,
    v1,
    v2,
    v3,
    weight,
    coeff,
    block,
    pos,
    obsw,
    diag,
    edge,
    coeff_edge,
    centre_edge,
    weight_edge,
    halo,
    coeff_halo,
    weight_halo,
    next_halo,
    prev_halo,
    prev_centre,
    next_state,
    next_weight,
    image,
    before,
    spread_halo,
    follow,
    spread,
    gram_high,
    gram_low,
    gram_line,
    row_send,
    row_recv,
    plane_recv,
    local_sem,
    send_sem,
    recv_sem,
    once_sem,
    rrecv_sem,
    known_sem,
    ballast,
):
    win = lax.axis_index("win")
    tile = lax.axis_index("tile")
    core = win % 2
    chip_y = (win // 2) % 8
    chip_z = win // 16
    has_prev, has_next = win > 0, win < NWIN - 1
    has_north, has_south = tile > 0, tile < NT - 1
    prev_id, next_id = (win - 1, tile), (win + 1, tile)
    states = (v0, v1, v2, v3)

    loads = [
        pltpu.make_async_copy(src, dst, local_sem.at[i])
        for i, (src, dst) in enumerate(
            (
                (right_hbm, v0),
                (weight_hbm, weight),
                (coeff_hbm, coeff),
                (block_hbm, block),
                (pos_hbm, pos),
                (obsw_hbm, obsw),
            )
        )
    ]
    for load in loads:
        load.start()

    def along_y(by):
        return (win + 2 * ((chip_y + by) % NYC - chip_y), tile)

    def along_z(by, other_core=False):
        start = win + 1 - 2 * core if other_core else win
        return (start + 16 * ((chip_z + by) % NZ - chip_z), tile)

    group = core * NT + tile
    slot_a = chip_y * 8 + group
    near = [
        (win - core + ((group + i) % 8) // NT, (group + i) % NT) for i in range(1, NCORE * NT)
    ]
    near += [along_y(1), along_y(-1)]
    near += [along_z(by, other) for by in (1, -1) for other in (False, True)]

    def signal(semaphore, peer):
        pl.semaphore_signal(semaphore, inc=1, device_id=peer, device_id_type=MESH)

    barrier = pltpu.get_barrier_semaphore()

    @pl.when(has_prev)
    def _():
        signal(barrier, prev_id)

    @pl.when(has_next)
    def _():
        signal(barrier, next_id)

    for peer in near:
        signal(barrier, peer)

    for i in range(2):
        loads[i].wait()
    for side in range(2):
        for l in range(LEV):
            for n, row in enumerate(OUTER[side]):
                edge[0, l, side, n] = v0[l, row : row + 1, :]
            row = OUTER[side][0]
            weight_edge[side, l] = weight[l, row : row + 1, :]

    pl.semaphore_wait(barrier, len(near) + jnp.where(has_prev, 1, 0) + jnp.where(has_next, 1, 0))

    def remote(src, dst, send, recv, peer):
        return pltpu.make_async_remote_copy(
            src_ref=src, dst_ref=dst, send_sem=send, recv_sem=recv, device_id=peer, device_id_type=MESH
        )

    def start_if(condition, copies):
        @pl.when(condition)
        def _():
            for copy in copies:
                copy.start()

    def wait_if(condition, copies):
        @pl.when(condition)
        def _():
            for copy in copies:
                copy.wait_recv()

    beside = (has_north, has_south)

    def towards(side, by):
        return (win + by, tile + (1 if side else -1))

    def and_(*conditions):
        total = conditions[0]
        for condition in conditions[1:]:
            total = jnp.logical_and(total, condition)
        return total

    def to_side(kind, j, l, side):
        sem = recv_sem.at[j % 2, l, kind + 1 - side]
        if kind == HALO:
            return remote(edge.at[j, l, side], halo.at[j, l, 1 - side], send_sem.at[side], sem, towards(side, 0))
        dst, out, by = (next_halo, 4, -1) if kind == BACK else (prev_halo, 6, 1)
        return remote(
            edge.at[j, l, side, 0], dst.at[j, l, 1 - side], send_sem.at[out + side], sem, towards(side, by)
        )

    def send_edges(j, l, side, diagonal=True, straight=True):
        if straight:
            start_if(beside[side], [to_side(HALO, j, l, side)])
        if diagonal:
            start_if(and_(beside[side], has_prev), [to_side(BACK, j, l, side)])
            start_if(and_(beside[side], has_next), [to_side(FORE, j, l, side)])

    def edges_from(kind, j, l, side):
        extra = {HALO: (), BACK: (has_next,), FORE: (has_prev,)}[kind]
        wait_if(and_(beside[side], *extra), [to_side(kind, j, l, 1 - side)])

    def state_block(j, l, b):
        at = pl.ds(8 * b, 8)
        return remote(
            states[j].at[l, at], next_state.at[j, l, at], send_sem.at[2], recv_sem.at[j % 2, l, STATE + b], prev_id
        )

    def image_block(j, l, b):
        at = pl.ds(8 * b, 8)
        return remote(
            image.at[j, l, at], before.at[j, l, at], send_sem.at[3], recv_sem.at[j % 2, l, IMAGE + b], next_id
        )

    def first_block(l, b):
        return state_block(0, l, b)

    def weight_block(l, b):
        at = pl.ds(8 * b, 8)
        return remote(
            weight.at[l, at], next_weight.at[l, at], send_sem.at[2], once_sem.at[5 + BLOCKS * l + b], prev_id
        )

    def coeff_side(side):
        return remote(
            coeff_edge.at[side], coeff_halo.at[1 - side], send_sem.at[side], once_sem.at[1 - side], towards(side, 0)
        )

    def weight_side(side):
        return remote(
            weight_edge.at[side],
            weight_halo.at[1 - side],
            send_sem.at[4 + side],
            once_sem.at[3 - side],
            towards(side, -1),
        )

    def centre_ahead():
        return remote(centre_edge, prev_centre, send_sem.at[3], once_sem.at[4], next_id)

    row_id = lax.broadcasted_iota(jnp.int32, (8, NX), 0)
    first_row, last_row = row_id == 0, row_id == 7

    def rows(b):
        return slice(8 * b, 8 * b + 8)

    def vertical(ref, l, b, top=0.0, bottom=0.0):
        here = ref[l, rows(b), :]
        above = pltpu.roll(ref[l, rows(b - 1), :], 1, 0) if b > 0 else top
        below = pltpu.roll(ref[l, rows(b + 1), :], 7, 0) if b < BLOCKS - 1 else bottom
        north = jnp.where(first_row, above, pltpu.roll(here, 1, 0))
        south = jnp.where(last_row, below, pltpu.roll(here, 7, 0))
        return north + south

    def edge_only(side, value):
        return jnp.where((first_row, last_row)[side], value, 0.0)

    def propagate(j, l, b):
        v = states[j]
        here = v[l, rows(b), :]
        image[j, l, rows(b), :] = (
            coeff[0, l, rows(b), :] * here
            + coeff[1, l, rows(b), :] * vertical(v, l, b)
            + coeff[2, l, rows(b), :] * pltpu.roll(here, NX - 1, 1)
            + coeff[3, l, rows(b), :] * pltpu.roll(here, 1, 1)
        )
        if j > 0 or l == 0:
            start_if(has_next, [image_block(j, l, b)])

    def side_of(b):
        return {0: 0, BLOCKS - 1: 1}.get(b)

    def outside(j, l, side):
        edges_from(HALO, j, l, side)
        if j == 0 and l == 0:
            wait_if(beside[side], [coeff_side(1 - side)])
            wait_if(and_(beside[side], has_next), [weight_side(1 - side)])
        near_row, far_row = halo[j, l, side, 0], halo[j, l, side, 1]
        row = OUTER[side][0]
        here = (
            coeff_halo[side, l, 0] * near_row
            + coeff_halo[side, l, 1] * (far_row + states[j][l, row : row + 1, :])
            + coeff_halo[side, l, 2] * pltpu.roll(near_row, NX - 1, 1)
            + coeff_halo[side, l, 3] * pltpu.roll(near_row, 1, 1)
        )
        edges_from(BACK, j, l, side)
        f = weight_halo[side, l] * (next_halo[j, l, side] - here)
        spread_halo[l, side] = coeff_halo[side, l, 1] * f

    def finish(j, l, b):
        v, out = states[j], states[j + 1]
        side = side_of(b)
        f = follow[l, rows(b), :]
        top = spread_halo[l, 0] if side == 0 else 0.0
        bottom = spread_halo[l, 1] if side == 1 else 0.0
        back_image = (
            coeff[0, l, rows(b), :] * f
            + vertical(spread, l, b, top, bottom)
            + pltpu.roll(coeff[2, l, rows(b), :] * f, 1, 1)
            + pltpu.roll(coeff[3, l, rows(b), :] * f, NX - 1, 1)
        )
        here = v[l, rows(b), :]
        out[l, rows(b), :] = weight[l, rows(b), :] * here - back_image + diag[l, rows(b), :] * here
        wait_if(has_prev, [image_block(j, l, b)])
        came = before[j, l, rows(b), :]
        if side is not None:
            edges_from(FORE, j, l, side)
            if j == 0 and l == 0 and side == 0:
                wait_if(has_prev, [centre_ahead()])
            came = came + edge_only(side, prev_centre[l, side] * prev_halo[j, l, side])
        out[l, rows(b), :] = SCALE * (out[l, rows(b), :] - weight[l, rows(b), :] * came)
        if j + 1 == STEPS:
            return
        start_if(has_prev, [state_block(j + 1, l, b)])
        if side is not None:
            for n, row in enumerate(OUTER[side]):
                edge[j + 1, l, side, n] = out[l, row : row + 1, :]
            send_edges(j + 1, l, side)
        if b > 0:
            propagate(j + 1, l, b - 1)
        if b == BLOCKS - 1:
            propagate(j + 1, l, b)

    def complete(j, l):
        for b in range(BLOCKS):
            side = side_of(b)
            if side is not None:
                outside(j, l, side)
            wait_if(has_next, [state_block(j, l, b), *([weight_block(l, b)] if j == 0 else [])])
            sent_image = image[j, l, rows(b), :]
            if side is not None:
                sent_image = sent_image + edge_only(side, coeff[1, l, rows(b), :] * halo[j, l, side, 0])
            f = next_weight[l, rows(b), :] * (next_state[j, l, rows(b), :] - sent_image)
            follow[l, rows(b), :] = f
            spread[l, rows(b), :] = coeff[1, l, rows(b), :] * f
            if b > 0:
                finish(j, l, b - 1)
        finish(j, l, BLOCKS - 1)

    def gram(group, l):
        indices = range(3 * group, 3 * group + 3)
        zero = jnp.zeros((8, 128), F32)

        def step(b, acc):
            acc = list(acc)
            at = pl.ds(pl.multiple_of(b * 8, 8), 8)
            for c in range(NX // 128):
                parts = {}
                for index in indices:
                    for s in PAIRS[index]:
                        if s not in parts:
                            x = states[s][l, at, c * 128 : (c + 1) * 128]
                            parts[s] = (x, split(x))
                for n, index in enumerate(indices):
                    i, k = PAIRS[index]
                    p, e = two_prod_split(parts[i][0], parts[k][0], parts[i][1], parts[k][1])
                    s, f = two_sum(acc[2 * n], p)
                    acc[2 * n], acc[2 * n + 1] = s, acc[2 * n + 1] + (e + f)
            return tuple(acc)

        acc = lax.fori_loop(0, BLOCKS, step, (zero,) * 6)
        for n, index in enumerate(indices):
            part = (acc[2 * n], acc[2 * n + 1])
            if l == 0:
                gram_high[index], gram_low[index] = part
                continue
            part = over_rows(plus(part, (gram_high[index], gram_low[index])))
            gram_line[index : index + 1, :], gram_line[16 + index : 17 + index, :] = part

    def over_rows(total):
        for shift in (4, 2, 1):
            total = plus(total, rolled(total, shift, 0))
        return total[0][0:1, :], total[1][0:1, :]

    def observed_weights():
        pos_t = jnp.swapaxes(pos[...], 0, 1)
        obsw_t = jnp.swapaxes(obsw[...], 0, 1)
        lane = lax.broadcasted_iota(jnp.int32, (128, 128), 1)
        lines = []
        for b in range(32):
            hit = pos_t[:, b : b + 1] == lane
            lines.append(jnp.sum(jnp.where(hit, obsw_t[:, b : b + 1], 0.0), axis=0, keepdims=True))
        per_block = jnp.concatenate(lines, axis=0)
        row = lax.broadcasted_iota(jnp.int32, (LEV * TY, 32), 0)
        for c in range(NX // 128):
            hot = (block[...] == row * (NX // 128) + c).astype(F32)
            out = jnp.dot(hot, per_block, precision=lax.Precision.HIGHEST, preferred_element_type=F32)
            for l in range(LEV):
                diag[l, :, c * 128 : (c + 1) * 128] = out[l * TY : (l + 1) * TY, :]

    def zeros(*refs):
        for ref in refs:
            ref[...] = jnp.zeros(ref.shape, F32)

    gram_line[...] = jnp.zeros((128, 128), F32)
    for side in range(2):
        for by in range(LEV):
            send_edges(0, by, side, diagonal=False)
        pl.when(beside[side])(lambda side=side: signal(known_sem.at[2, 0], towards(side, 0)))
    blocks = [copy(l, b) for l in range(LEV) for b in range(BLOCKS) for copy in (first_block, weight_block)]
    start_if(has_prev, blocks[:EARLY])
    loads[2].wait()
    for l in range(LEV):
        for b in range(BLOCKS):
            propagate(0, l, b)
    for at, move in enumerate((along_y, along_z)):
        for by in (1, -1):
            signal(known_sem.at[at, 0], move(by))
    pl.semaphore_wait(known_sem.at[2, 0], jnp.where(has_north, 1, 0) + jnp.where(has_south, 1, 0))
    for side in range(2):
        start_if(and_(beside[side], has_prev), [weight_side(side)])
        for l in range(LEV):
            send_edges(0, l, side, straight=False)
    start_if(has_prev, blocks[EARLY:])
    for side in range(2):
        row = OUTER[side][0]
        for l in range(LEV):
            for n in range(4):
                coeff_edge[side, l, n] = coeff[n, l, row : row + 1, :]
            centre_edge[l, side] = coeff[1, l, row : row + 1, :]
    for side in range(2):
        start_if(beside[side], [coeff_side(side)])
    start_if(has_next, [centre_ahead()])
    start_if(has_next, [image_block(0, 1, b) for b in range(BLOCKS)])
    for side in range(2):

        @pl.when(jnp.logical_not(beside[side]))
        def _(side=side):
            zeros(coeff_halo.at[side], weight_halo.at[side])
            for j in range(STEPS):
                for l in range(LEV):
                    zeros(halo.at[j, l, side], next_halo.at[j, l, side], prev_halo.at[j, l, side])

    pl.when(jnp.logical_not(has_prev))(lambda: zeros(before, prev_halo, prev_centre))
    pl.when(jnp.logical_not(has_next))(lambda: zeros(next_state, next_weight, next_halo, weight_halo))
    for load in loads[3:]:
        load.wait()
    observed_weights()
    for at, move in enumerate((along_y, along_z)):
        pl.semaphore_wait(known_sem.at[at, 0], 2)
        for by in (2, -2):
            signal(known_sem.at[at, 1], move(by))
    for j in range(STEPS):
        for l in range(LEV):
            complete(j, l)
            if j + 1 == STEPS:
                gram(2, l)
        if j + 1 < STEPS:
            for at, move in enumerate((along_y, along_z)):
                pl.semaphore_wait(known_sem.at[at, j + 1], 2)
                for by in (1, -1) if j == 0 else ():
                    signal(known_sem.at[at, 2], move(by))
            for l in range(LEV):
                gram(j, l)

    turned = jnp.swapaxes(gram_line[...], 0, 1)
    pieces = [turned[8 * i : 8 * i + 8, :] for i in range(16)]
    total = over_rows(tree2([(x, pltpu.roll(x, 128 - 16, 1)) for x in pieces]))
    lane = lax.broadcasted_iota(jnp.int32, (1, 128), 1)

    def packed(pair):
        return jnp.where(lane < 16, pair[0], jnp.where(lane < 32, pltpu.roll(pair[1], 16, 1), 0.0))

    line = packed(total)

    def over_slots(parts):
        return over_rows(tree2([(x, pltpu.roll(x, 128 - 16, 1)) for x in parts]))

    def arrived(stage, count):
        whole = ballast.at[pl.ds(0, count)]
        pltpu.make_async_copy(whole, whole, rrecv_sem.at[stage]).wait()

    def to_plane(by, x_by):
        where = (along_y(by)[0] - core + 1, (tile + x_by) % NT)
        return remote(
            row_send.at[0], plane_recv.at[pl.ds(slot_a, 1)], send_sem.at[8], rrecv_sem.at[0], where
        )

    def to_z(by, other_core):
        return remote(
            row_send.at[1], row_recv.at[chip_z], send_sem.at[9], rrecv_sem.at[1], along_z(by, other_core)
        )

    is_second = core == 1
    row_send[0] = line
    for by in (4, 3, 5, 2, 6, 1, 7, 0):
        for other in (2, 1, 3, 0):
            copy = to_plane(by, other)
            if by == 0 and other == 0:
                pl.when(core == 0)(copy.start)
            else:
                copy.start()

    @pl.when(is_second)
    def _():
        plane_recv[pl.ds(slot_a, 1), :] = line
        arrived(0, PLANE - 1)
        mine = packed(over_slots([plane_recv[8 * i : 8 * i + 8, :] for i in range(PLANE // 8)]))
        row_send[1] = mine
        row_recv[chip_z] = mine
        for by in (4, 3, 5, 2, 6, 1, 7):
            to_z(by, True).start()
            to_z(by, False).start()
        to_z(0, True).start()
        arrived(1, NZ - 1)

    @pl.when(jnp.logical_not(is_second))
    def _():
        arrived(1, NZ)

    total = tree2([(x, pltpu.roll(x, 128 - 16, 1)) for x in [row_recv[i] for i in range(NZ)]])
    line = packed(quick_sum(*total))

    def value(i, j):
        at = PAIRS.index((min(i, j), max(i, j)))
        return tuple(jnp.broadcast_to(line[:, at + off : at + off + 1], (8, 128)) for off in (0, 16))

    a = [[value(i, n + 1) for n in range(3)] + [value(i, 0)] for i in range(3)]
    for pivot in range(2):
        for i in range(pivot + 1, 3):
            factor = div2(a[i][pivot], a[pivot][pivot])
            for n in range(pivot + 1, 4):
                a[i][n] = sub2(a[i][n], mul2(factor, a[pivot][n]))
    c2 = div2(a[2][3], a[2][2])
    c1 = div2(sub2(a[1][3], mul2(a[1][2], c2)), a[1][1])
    c0 = div2(sub2(sub2(a[0][3], mul2(a[0][1], c1)), mul2(a[0][2], c2)), a[0][0])
    combo = [jnp.concatenate([c[0]] * (NX // 128), axis=1) for c in (c0, c1, c2)]
    for l in range(LEV):
        for b in range(BLOCKS):
            at = (l, rows(b), slice(None))
            u0, u1, u2, u3 = (s[at] for s in states)
            solution_out[0, l, rows(b), :] = SCALE * (combo[0] * u0 + combo[1] * u1 + combo[2] * u2)
            residual_out[0, l, rows(b), :] = u0 - combo[0] * u1 - combo[1] * u2 - combo[2] * u3

    def sent(condition, count, semaphore):
        @pl.when(condition)
        def _():
            whole = ballast.at[pl.ds(0, count)]
            pltpu.make_async_copy(whole, whole, semaphore).wait()

    for side in range(2):
        sent(beside[side], SIDE_ROWS, send_sem.at[side])
        sent(and_(beside[side], has_prev), BACK_SIDE_ROWS, send_sem.at[4 + side])
        sent(and_(beside[side], has_next), AHEAD_SIDE_ROWS, send_sem.at[6 + side])
    sent(has_prev, BACK_ROWS, send_sem.at[2])
    sent(has_next, AHEAD_ROWS, send_sem.at[3])
    sent(is_second, PLANE // 2 - 1, send_sem.at[8])
    sent(jnp.logical_not(is_second), PLANE // 2, send_sem.at[8])
    sent(is_second, 2 * NZ - 1, send_sem.at[9])


def on_device(right_side, error_weight, coeffs, obs_block, obs_pos, obs_weight):
    shape = (LEV, TY, NX)
    vmem, hbm = pltpu.VMEM, pltpu.HBM
    line = (STEPS, LEV, 2, 1, NX)
    scratch = [
        vmem(shape, F32),
        vmem(shape, F32),
        vmem(shape, F32),
        vmem(shape, F32),
        vmem(shape, F32),
        vmem((4, *shape), F32),
        vmem((1, 32), jnp.int32),
        vmem((32, 128), jnp.int32),
        vmem((32, 128), F32),
        vmem(shape, F32),
        vmem((STEPS, LEV, 2, 2, 1, NX), F32),
        vmem((2, LEV, 4, 1, NX), F32),
        vmem((LEV, 2, 1, NX), F32),
        vmem((2, LEV, 1, NX), F32),
        vmem((STEPS, LEV, 2, 2, 1, NX), F32),
        vmem((2, LEV, 4, 1, NX), F32),
        vmem((2, LEV, 1, NX), F32),
        vmem(line, F32),
        vmem(line, F32),
        vmem((LEV, 2, 1, NX), F32),
        vmem((STEPS, *shape), F32),
        vmem(shape, F32),
        vmem((STEPS, *shape), F32),
        vmem((STEPS, *shape), F32),
        vmem((LEV, 2, 1, NX), F32),
        vmem(shape, F32),
        vmem(shape, F32),
        vmem((len(PAIRS), 8, 128), F32),
        vmem((len(PAIRS), 8, 128), F32),
        vmem((128, 128), F32),
        vmem((2, 1, 128), F32),
        vmem((NZ, 1, 128), F32),
        vmem((PLANE, 128), F32),
        pltpu.SemaphoreType.DMA((6,)),
        pltpu.SemaphoreType.DMA((10,)),
        pltpu.SemaphoreType.DMA((2, LEV, MESSAGES)),
        pltpu.SemaphoreType.DMA((5 + LEV * BLOCKS,)),
        pltpu.SemaphoreType.DMA((2,)),
        pltpu.SemaphoreType.REGULAR((3, 3)),
        vmem((BACK_ROWS, 1, 128), F32),
    ]
    solution_field, residual = pl.pallas_call(
        kernel,
        out_shape=(pltpu.VMEM((1, *shape), F32), pltpu.VMEM((1, *shape), F32)),
        in_specs=[pl.BlockSpec(memory_space=hbm)] * 6,
        out_specs=(pl.BlockSpec(memory_space=vmem),) * 2,
        scratch_shapes=scratch,
        compiler_params=pltpu.CompilerParams(collective_id=0, has_side_effects=True),
        name="krylov",
    )(
        right_side.reshape(shape),
        error_weight.reshape(shape),
        coeffs.reshape(4, *shape),
        obs_block,
        obs_pos.reshape(32, 128),
        obs_weight.reshape(32, 128),
    )
    whole = jax.ShapeDtypeStruct((1, *shape), F32)
    return pl.pallas_call(
        store,
        out_shape=(whole, whole),
        in_specs=[pl.BlockSpec(memory_space=vmem)] * 2,
        out_specs=(pl.BlockSpec(memory_space=hbm),) * 2,
        scratch_shapes=[pltpu.SemaphoreType.DMA((2,))],
        name="store",
    )(*(pltpu.with_memory_space_constraint(x, vmem) for x in (solution_field, residual)))


def store(solution_field, residual, solution_out, residual_out, sem):
    copies = [
        pltpu.make_async_copy(solution_field, solution_out, sem.at[0]),
        pltpu.make_async_copy(residual, residual_out, sem.at[1]),
    ]
    for copy in copies:
        copy.start()
    for copy in copies:
        copy.wait()


def solution(mesh):
    in_specs = (
        P("win", None, "tile", None),
        P("win", None, "tile", None),
        P(None, "win", None, "tile", None),
        P("win", "tile"),
        P("win", "tile", None),
        P("win", "tile", None),
    )
    out_specs = (P("win", None, "tile", None), P("win", None, "tile", None))
    return jax.shard_map(on_device, mesh=mesh, in_specs=in_specs, out_specs=out_specs, check_vma=False)
```

```python
import jax
import jax.numpy as jnp
from jax import lax
from jax.experimental import pallas as pl
from jax.experimental.pallas import tpu as pltpu
from jax.sharding import PartitionSpec as P

MESH = pl.DeviceIdType.MESH
F32 = jnp.float32
LEV, TY, NX = 2, 32, 1024
BLOCKS = TY // 8
STEPS = 3
SCALE = 1.0 / 16.0
NZ, NYC, NCORE, NT = 8, 8, 2, 4
NWIN = NZ * NYC * NCORE
PLANE = NYC * NCORE * NT
PAIRS = ((0, 0), (0, 1), (1, 1), (0, 2), (1, 2), (2, 2), (0, 3), (1, 3), (2, 3))
HALO, BACK, FORE, STATE, IMAGE = 0, 2, 4, 6, 10
MESSAGES = 14
WIDE = NX // 128
SIDE_ROWS = LEV * (2 * STEPS + 4) * WIDE
BACK_ROWS = (STEPS + 1) * LEV * TY * WIDE
AHEAD_ROWS = (STEPS * LEV * TY + 2 * LEV) * WIDE
BACK_SIDE_ROWS = LEV * (STEPS + 1) * WIDE
AHEAD_SIDE_ROWS = LEV * STEPS * WIDE
EARLY = 6
OUTER = ((0, 1), (TY - 1, TY - 2))


def two_sum(a, b):
    s = a + b
    t = s - a
    return s, (a - (s - t)) + (b - t)


def quick_sum(a, b):
    s = a + b
    return s, b - (s - a)


def split(a):
    c = a * 4097.0
    high = c - (c - a)
    return high, a - high


def two_prod_split(a, b, sa, sb):
    p = a * b
    return p, ((sa[0] * sb[0] - p) + sa[0] * sb[1] + sa[1] * sb[0]) + sa[1] * sb[1]


def two_prod(a, b):
    return two_prod_split(a, b, split(a), split(b))


def add2(a, b):
    s, e = two_sum(a[0], b[0])
    return quick_sum(s, e + (a[1] + b[1]))


def neg2(a):
    return -a[0], -a[1]


def sub2(a, b):
    return add2(a, neg2(b))


def mul2(a, b):
    p, e = two_prod(a[0], b[0])
    return quick_sum(p, e + (a[0] * b[1] + a[1] * b[0]))


def div2(a, b):
    zero = jnp.zeros_like(a[0])
    first = a[0] / b[0]
    rest = sub2(a, mul2((first, zero), b))
    return quick_sum(first, rest[0] / b[0])


def plus(a, b):
    s, e = two_sum(a[0], b[0])
    return s, (a[1] + b[1]) + e


def tree2(items):
    while len(items) > 1:
        items = [
            plus(items[i], items[i + 1]) if i + 1 < len(items) else items[i]
            for i in range(0, len(items), 2)
        ]
    return items[0]


def rolled(pair, shift, axis):
    return pltpu.roll(pair[0], shift, axis), pltpu.roll(pair[1], shift, axis)


def kernel(
    right_hbm,
    weight_hbm,
    coeff_hbm,
    block_hbm,
    pos_hbm,
    obsw_hbm,
    solution_out,
    residual_out,
    v0,
    v1,
    v2,
    v3,
    weight,
    coeff,
    block,
    pos,
    obsw,
    diag,
    edge,
    coeff_edge,
    centre_edge,
    weight_edge,
    halo,
    coeff_halo,
    weight_halo,
    next_halo,
    prev_halo,
    prev_centre,
    next_state,
    next_weight,
    image,
    before,
    spread_halo,
    follow,
    spread,
    gram_high,
    gram_low,
    gram_line,
    row_send,
    row_recv,
    plane_recv,
    local_sem,
    send_sem,
    recv_sem,
    once_sem,
    rrecv_sem,
    known_sem,
    ballast,
):
    win = lax.axis_index("win")
    tile = lax.axis_index("tile")
    core = win % 2
    chip_y = (win // 2) % 8
    chip_z = win // 16
    has_prev, has_next = win > 0, win < NWIN - 1
    has_north, has_south = tile > 0, tile < NT - 1
    prev_id, next_id = (win - 1, tile), (win + 1, tile)
    states = (v0, v1, v2, v3)

    loads = [
        pltpu.make_async_copy(src, dst, local_sem.at[i])
        for i, (src, dst) in enumerate(
            (
                (right_hbm, v0),
                (weight_hbm, weight),
                (coeff_hbm, coeff),
                (block_hbm, block),
                (pos_hbm, pos),
                (obsw_hbm, obsw),
            )
        )
    ]
    for load in loads:
        load.start()

    def along_y(by):
        return (win + 2 * ((chip_y + by) % NYC - chip_y), tile)

    def along_z(by, other_core=False):
        start = win + 1 - 2 * core if other_core else win
        return (start + 16 * ((chip_z + by) % NZ - chip_z), tile)

    group = core * NT + tile
    slot_a = chip_y * 8 + group
    near = [
        (win - core + ((group + i) % 8) // NT, (group + i) % NT) for i in range(1, NCORE * NT)
    ]
    near += [along_y(1), along_y(-1)]
    near += [along_z(by, other) for by in (1, -1) for other in (False, True)]

    def signal(semaphore, peer):
        pl.semaphore_signal(semaphore, inc=1, device_id=peer, device_id_type=MESH)

    barrier = pltpu.get_barrier_semaphore()

    @pl.when(has_prev)
    def _():
        signal(barrier, prev_id)

    @pl.when(has_next)
    def _():
        signal(barrier, next_id)

    for peer in near:
        signal(barrier, peer)

    for i in range(2):
        loads[i].wait()
    for side in range(2):
        for l in range(LEV):
            for n, row in enumerate(OUTER[side]):
                edge[0, l, side, n] = v0[l, row : row + 1, :]
            row = OUTER[side][0]
            weight_edge[side, l] = weight[l, row : row + 1, :]

    pl.semaphore_wait(barrier, len(near) + jnp.where(has_prev, 1, 0) + jnp.where(has_next, 1, 0))

    def remote(src, dst, send, recv, peer):
        return pltpu.make_async_remote_copy(
            src_ref=src, dst_ref=dst, send_sem=send, recv_sem=recv, device_id=peer, device_id_type=MESH
        )

    def start_if(condition, copies):
        @pl.when(condition)
        def _():
            for copy in copies:
                copy.start()

    def wait_if(condition, copies):
        @pl.when(condition)
        def _():
            for copy in copies:
                copy.wait_recv()

    beside = (has_north, has_south)

    def towards(side, by):
        return (win + by, tile + (1 if side else -1))

    def and_(*conditions):
        total = conditions[0]
        for condition in conditions[1:]:
            total = jnp.logical_and(total, condition)
        return total

    def to_side(kind, j, l, side):
        sem = recv_sem.at[j % 2, l, kind + 1 - side]
        if kind == HALO:
            return remote(edge.at[j, l, side], halo.at[j, l, 1 - side], send_sem.at[side], sem, towards(side, 0))
        dst, out, by = (next_halo, 4, -1) if kind == BACK else (prev_halo, 6, 1)
        return remote(
            edge.at[j, l, side, 0], dst.at[j, l, 1 - side], send_sem.at[out + side], sem, towards(side, by)
        )

    def send_edges(j, l, side, diagonal=True, straight=True):
        if straight:
            start_if(beside[side], [to_side(HALO, j, l, side)])
        if diagonal:
            start_if(and_(beside[side], has_prev), [to_side(BACK, j, l, side)])
            start_if(and_(beside[side], has_next), [to_side(FORE, j, l, side)])

    def edges_from(kind, j, l, side):
        extra = {HALO: (), BACK: (has_next,), FORE: (has_prev,)}[kind]
        wait_if(and_(beside[side], *extra), [to_side(kind, j, l, 1 - side)])

    def state_block(j, l, b):
        at = pl.ds(8 * b, 8)
        return remote(
            states[j].at[l, at], next_state.at[j, l, at], send_sem.at[2], recv_sem.at[j % 2, l, STATE + b], prev_id
        )

    def image_block(j, l, b):
        at = pl.ds(8 * b, 8)
        return remote(
            image.at[j, l, at], before.at[j, l, at], send_sem.at[3], recv_sem.at[j % 2, l, IMAGE + b], next_id
        )

    def first_block(l, b):
        return state_block(0, l, b)

    def weight_block(l, b):
        at = pl.ds(8 * b, 8)
        return remote(
            weight.at[l, at], next_weight.at[l, at], send_sem.at[2], once_sem.at[5 + BLOCKS * l + b], prev_id
        )

    def coeff_side(side):
        return remote(
            coeff_edge.at[side], coeff_halo.at[1 - side], send_sem.at[side], once_sem.at[1 - side], towards(side, 0)
        )

    def weight_side(side):
        return remote(
            weight_edge.at[side],
            weight_halo.at[1 - side],
            send_sem.at[4 + side],
            once_sem.at[3 - side],
            towards(side, -1),
        )

    def centre_ahead():
        return remote(centre_edge, prev_centre, send_sem.at[3], once_sem.at[4], next_id)

    row_id = lax.broadcasted_iota(jnp.int32, (8, NX), 0)
    first_row, last_row = row_id == 0, row_id == 7

    def rows(b):
        return slice(8 * b, 8 * b + 8)

    def vertical(ref, l, b, top=0.0, bottom=0.0):
        here = ref[l, rows(b), :]
        above = pltpu.roll(ref[l, rows(b - 1), :], 1, 0) if b > 0 else top
        below = pltpu.roll(ref[l, rows(b + 1), :], 7, 0) if b < BLOCKS - 1 else bottom
        north = jnp.where(first_row, above, pltpu.roll(here, 1, 0))
        south = jnp.where(last_row, below, pltpu.roll(here, 7, 0))
        return north + south

    def edge_only(side, value):
        return jnp.where((first_row, last_row)[side], value, 0.0)

    def propagate(j, l, b):
        v = states[j]
        here = v[l, rows(b), :]
        image[j, l, rows(b), :] = (
            coeff[0, l, rows(b), :] * here
            + coeff[1, l, rows(b), :] * vertical(v, l, b)
            + coeff[2, l, rows(b), :] * pltpu.roll(here, NX - 1, 1)
            + coeff[3, l, rows(b), :] * pltpu.roll(here, 1, 1)
        )
        if j > 0 or l == 0:
            start_if(has_next, [image_block(j, l, b)])

    def side_of(b):
        return {0: 0, BLOCKS - 1: 1}.get(b)

    def outside(j, l, side):
        edges_from(HALO, j, l, side)
        if j == 0 and l == 0:
            wait_if(beside[side], [coeff_side(1 - side)])
            wait_if(and_(beside[side], has_next), [weight_side(1 - side)])
        near_row, far_row = halo[j, l, side, 0], halo[j, l, side, 1]
        row = OUTER[side][0]
        here = (
            coeff_halo[side, l, 0] * near_row
            + coeff_halo[side, l, 1] * (far_row + states[j][l, row : row + 1, :])
            + coeff_halo[side, l, 2] * pltpu.roll(near_row, NX - 1, 1)
            + coeff_halo[side, l, 3] * pltpu.roll(near_row, 1, 1)
        )
        edges_from(BACK, j, l, side)
        f = weight_halo[side, l] * (next_halo[j, l, side] - here)
        spread_halo[l, side] = coeff_halo[side, l, 1] * f

    def finish(j, l, order, at):
        b = order[at]
        v, out = states[j], states[j + 1]
        side = side_of(b)
        f = follow[l, rows(b), :]
        top = spread_halo[l, 0] if side == 0 else 0.0
        bottom = spread_halo[l, 1] if side == 1 else 0.0
        back_image = (
            coeff[0, l, rows(b), :] * f
            + vertical(spread, l, b, top, bottom)
            + pltpu.roll(coeff[2, l, rows(b), :] * f, 1, 1)
            + pltpu.roll(coeff[3, l, rows(b), :] * f, NX - 1, 1)
        )
        here = v[l, rows(b), :]
        out[l, rows(b), :] = weight[l, rows(b), :] * here - back_image + diag[l, rows(b), :] * here
        wait_if(has_prev, [image_block(j, l, b)])
        came = before[j, l, rows(b), :]
        if side is not None:
            edges_from(FORE, j, l, side)
            if j == 0 and l == 0 and at == 0:
                wait_if(has_prev, [centre_ahead()])
            came = came + edge_only(side, prev_centre[l, side] * prev_halo[j, l, side])
        out[l, rows(b), :] = SCALE * (out[l, rows(b), :] - weight[l, rows(b), :] * came)
        if j + 1 == STEPS:
            keep(j, gram_block(j, l, rows(b), kept(j)))
            return
        if side is not None:
            for n, row in enumerate(OUTER[side]):
                edge[j + 1, l, side, n] = out[l, row : row + 1, :]
            send_edges(j + 1, l, side)
        start_if(has_prev, [state_block(j + 1, l, b)])
        if at > 0:
            propagate(j + 1, l, order[at - 1])
        if at == BLOCKS - 1:
            propagate(j + 1, l, b)

    def complete(j, l, order):
        for at, b in enumerate(order):
            side = side_of(b)
            if side is not None:
                outside(j, l, side)
            wait_if(has_next, [state_block(j, l, b), *([weight_block(l, b)] if j == 0 else [])])
            sent_image = image[j, l, rows(b), :]
            if side is not None:
                sent_image = sent_image + edge_only(side, coeff[1, l, rows(b), :] * halo[j, l, side, 0])
            f = next_weight[l, rows(b), :] * (next_state[j, l, rows(b), :] - sent_image)
            follow[l, rows(b), :] = f
            spread[l, rows(b), :] = coeff[1, l, rows(b), :] * f
            if at > 0:
                finish(j, l, order, at - 1)
        finish(j, l, order, BLOCKS - 1)

    def by_parity(body):
        pl.when(tile % 2 == 0)(lambda: body(tuple(range(BLOCKS))))
        pl.when(tile % 2 == 1)(lambda: body(tuple(reversed(range(BLOCKS)))))

    def gram_block(group, l, at, acc):
        acc = list(acc)
        for c in range(NX // 128):
            parts = {}
            for n in range(3):
                i, k = PAIRS[3 * group + n]
                for s in (i, k):
                    if s not in parts:
                        x = states[s][l, at, c * 128 : (c + 1) * 128]
                        parts[s] = (x, split(x))
                p, e = two_prod_split(parts[i][0], parts[k][0], parts[i][1], parts[k][1])
                s, f = two_sum(acc[2 * n], p)
                acc[2 * n], acc[2 * n + 1] = s, acc[2 * n + 1] + (e + f)
        return tuple(acc)

    def keep(group, acc):
        for n in range(3):
            gram_high[3 * group + n], gram_low[3 * group + n] = acc[2 * n], acc[2 * n + 1]

    def kept(group):
        return tuple(ref[3 * group + n] for n in range(3) for ref in (gram_high, gram_low))

    def gram_lines(group):
        acc = kept(group)
        for n in range(3):
            index = 3 * group + n
            line = over_rows((acc[2 * n], acc[2 * n + 1]))
            gram_line[index : index + 1, :], gram_line[16 + index : 17 + index, :] = line

    def gram(group):
        def step(n, acc):
            at = pl.ds(pl.multiple_of((n % BLOCKS) * 8, 8), 8)
            return gram_block(group, n // BLOCKS, at, acc)

        keep(group, lax.fori_loop(0, LEV * BLOCKS, step, (jnp.zeros((8, 128), F32),) * 6))
        gram_lines(group)

    def over_rows(total):
        for shift in (4, 2, 1):
            total = plus(total, rolled(total, shift, 0))
        return total[0][0:1, :], total[1][0:1, :]

    def observed_weights():
        pos_t = jnp.swapaxes(pos[...], 0, 1)
        obsw_t = jnp.swapaxes(obsw[...], 0, 1)
        lane = lax.broadcasted_iota(jnp.int32, (128, 128), 1)
        lines = []
        for b in range(32):
            hit = pos_t[:, b : b + 1] == lane
            lines.append(jnp.sum(jnp.where(hit, obsw_t[:, b : b + 1], 0.0), axis=0, keepdims=True))
        per_block = jnp.concatenate(lines, axis=0)
        row = lax.broadcasted_iota(jnp.int32, (LEV * TY, 32), 0)
        for c in range(NX // 128):
            hot = (block[...] == row * (NX // 128) + c).astype(F32)
            out = jnp.dot(hot, per_block, precision=lax.Precision.HIGHEST, preferred_element_type=F32)
            for l in range(LEV):
                diag[l, :, c * 128 : (c + 1) * 128] = out[l * TY : (l + 1) * TY, :]

    def zeros(*refs):
        for ref in refs:
            ref[...] = jnp.zeros(ref.shape, F32)

    gram_line[...] = jnp.zeros((128, 128), F32)
    for side in range(2):
        for by in range(LEV):
            send_edges(0, by, side, diagonal=False)
        pl.when(beside[side])(lambda side=side: signal(known_sem.at[2, 0], towards(side, 0)))
    def bulk(order):
        return [copy(l, b) for l in range(LEV) for b in order for copy in (first_block, weight_block)]

    by_parity(lambda order: start_if(has_prev, bulk(order)[:EARLY]))
    loads[2].wait()

    @by_parity
    def _(order):
        for l in range(LEV):
            for b in order:
                propagate(0, l, b)

    for at, move in enumerate((along_y, along_z)):
        for by in (1, -1):
            signal(known_sem.at[at, 0], move(by))
    pl.semaphore_wait(known_sem.at[2, 0], jnp.where(has_north, 1, 0) + jnp.where(has_south, 1, 0))
    for side in range(2):
        start_if(and_(beside[side], has_prev), [weight_side(side)])
        for l in range(LEV):
            send_edges(0, l, side, straight=False)
    by_parity(lambda order: start_if(has_prev, bulk(order)[EARLY:]))
    for side in range(2):
        row = OUTER[side][0]
        for l in range(LEV):
            for n in range(4):
                coeff_edge[side, l, n] = coeff[n, l, row : row + 1, :]
            centre_edge[l, side] = coeff[1, l, row : row + 1, :]
    for side in range(2):
        start_if(beside[side], [coeff_side(side)])
    start_if(has_next, [centre_ahead()])
    by_parity(lambda order: start_if(has_next, [image_block(0, 1, b) for b in order]))
    for side in range(2):

        @pl.when(jnp.logical_not(beside[side]))
        def _(side=side):
            zeros(coeff_halo.at[side], weight_halo.at[side])
            for j in range(STEPS):
                for l in range(LEV):
                    zeros(halo.at[j, l, side], next_halo.at[j, l, side], prev_halo.at[j, l, side])

    pl.when(jnp.logical_not(has_prev))(lambda: zeros(before, prev_halo, prev_centre))
    pl.when(jnp.logical_not(has_next))(lambda: zeros(next_state, next_weight, next_halo, weight_halo))
    for load in loads[3:]:
        load.wait()
    observed_weights()
    for at, move in enumerate((along_y, along_z)):
        pl.semaphore_wait(known_sem.at[at, 0], 2)
        for by in (2, -2):
            signal(known_sem.at[at, 1], move(by))
    for j in range(STEPS):
        if j + 1 == STEPS:
            keep(j, (jnp.zeros((8, 128), F32),) * 6)
        for l in range(LEV):
            by_parity(lambda order, j=j, l=l: complete(j, l, order))
        if j + 1 < STEPS:
            for at, move in enumerate((along_y, along_z)):
                pl.semaphore_wait(known_sem.at[at, j + 1], 2)
                for by in (1, -1) if j == 0 else ():
                    signal(known_sem.at[at, 2], move(by))
            gram(j)
    gram_lines(STEPS - 1)

    turned = jnp.swapaxes(gram_line[...], 0, 1)
    pieces = [turned[8 * i : 8 * i + 8, :] for i in range(16)]
    total = over_rows(tree2([(x, pltpu.roll(x, 128 - 16, 1)) for x in pieces]))
    lane = lax.broadcasted_iota(jnp.int32, (1, 128), 1)

    def packed(pair):
        return jnp.where(lane < 16, pair[0], jnp.where(lane < 32, pltpu.roll(pair[1], 16, 1), 0.0))

    line = packed(total)

    def over_slots(parts):
        return over_rows(tree2([(x, pltpu.roll(x, 128 - 16, 1)) for x in parts]))

    def arrived(stage, count):
        whole = ballast.at[pl.ds(0, count)]
        pltpu.make_async_copy(whole, whole, rrecv_sem.at[stage]).wait()

    def to_plane(by, x_by):
        where = (along_y(by)[0] - core + 1, (tile + x_by) % NT)
        return remote(
            row_send.at[0], plane_recv.at[pl.ds(slot_a, 1)], send_sem.at[8], rrecv_sem.at[0], where
        )

    def to_z(by, other_core):
        return remote(
            row_send.at[1], row_recv.at[chip_z], send_sem.at[9], rrecv_sem.at[1], along_z(by, other_core)
        )

    is_second = core == 1
    row_send[0] = line
    for by in (4, 3, 5, 2, 6, 1, 7, 0):
        for other in (2, 1, 3, 0):
            copy = to_plane(by, other)
            if by == 0 and other == 0:
                pl.when(core == 0)(copy.start)
            else:
                copy.start()

    @pl.when(is_second)
    def _():
        plane_recv[pl.ds(slot_a, 1), :] = line
        arrived(0, PLANE - 1)
        mine = packed(over_slots([plane_recv[8 * i : 8 * i + 8, :] for i in range(PLANE // 8)]))
        row_send[1] = mine
        row_recv[chip_z] = mine
        for by in (4, 3, 5, 2, 6, 1, 7):
            to_z(by, True).start()
            to_z(by, False).start()
        to_z(0, True).start()
        arrived(1, NZ - 1)

    @pl.when(jnp.logical_not(is_second))
    def _():
        arrived(1, NZ)

    total = tree2([(x, pltpu.roll(x, 128 - 16, 1)) for x in [row_recv[i] for i in range(NZ)]])
    line = packed(quick_sum(*total))

    def value(i, j):
        at = PAIRS.index((min(i, j), max(i, j)))
        return tuple(jnp.broadcast_to(line[:, at + off : at + off + 1], (8, 128)) for off in (0, 16))

    a = [[value(i, n + 1) for n in range(3)] + [value(i, 0)] for i in range(3)]
    for pivot in range(2):
        for i in range(pivot + 1, 3):
            factor = div2(a[i][pivot], a[pivot][pivot])
            for n in range(pivot + 1, 4):
                a[i][n] = sub2(a[i][n], mul2(factor, a[pivot][n]))
    c2 = div2(a[2][3], a[2][2])
    c1 = div2(sub2(a[1][3], mul2(a[1][2], c2)), a[1][1])
    c0 = div2(sub2(sub2(a[0][3], mul2(a[0][1], c1)), mul2(a[0][2], c2)), a[0][0])
    combo = [jnp.concatenate([c[0]] * (NX // 128), axis=1) for c in (c0, c1, c2)]
    for l in range(LEV):
        for b in range(BLOCKS):
            at = (l, rows(b), slice(None))
            u0, u1, u2, u3 = (s[at] for s in states)
            solution_out[0, l, rows(b), :] = SCALE * (combo[0] * u0 + combo[1] * u1 + combo[2] * u2)
            residual_out[0, l, rows(b), :] = u0 - combo[0] * u1 - combo[1] * u2 - combo[2] * u3

    def sent(condition, count, semaphore):
        @pl.when(condition)
        def _():
            whole = ballast.at[pl.ds(0, count)]
            pltpu.make_async_copy(whole, whole, semaphore).wait()

    for side in range(2):
        sent(beside[side], SIDE_ROWS, send_sem.at[side])
        sent(and_(beside[side], has_prev), BACK_SIDE_ROWS, send_sem.at[4 + side])
        sent(and_(beside[side], has_next), AHEAD_SIDE_ROWS, send_sem.at[6 + side])
    sent(has_prev, BACK_ROWS, send_sem.at[2])
    sent(has_next, AHEAD_ROWS, send_sem.at[3])
    sent(is_second, PLANE // 2 - 1, send_sem.at[8])
    sent(jnp.logical_not(is_second), PLANE // 2, send_sem.at[8])
    sent(is_second, 2 * NZ - 1, send_sem.at[9])


def on_device(right_side, error_weight, coeffs, obs_block, obs_pos, obs_weight):
    shape = (LEV, TY, NX)
    vmem, hbm = pltpu.VMEM, pltpu.HBM
    line = (STEPS, LEV, 2, 1, NX)
    scratch = [
        vmem(shape, F32),
        vmem(shape, F32),
        vmem(shape, F32),
        vmem(shape, F32),
        vmem(shape, F32),
        vmem((4, *shape), F32),
        vmem((1, 32), jnp.int32),
        vmem((32, 128), jnp.int32),
        vmem((32, 128), F32),
        vmem(shape, F32),
        vmem((STEPS, LEV, 2, 2, 1, NX), F32),
        vmem((2, LEV, 4, 1, NX), F32),
        vmem((LEV, 2, 1, NX), F32),
        vmem((2, LEV, 1, NX), F32),
        vmem((STEPS, LEV, 2, 2, 1, NX), F32),
        vmem((2, LEV, 4, 1, NX), F32),
        vmem((2, LEV, 1, NX), F32),
        vmem(line, F32),
        vmem(line, F32),
        vmem((LEV, 2, 1, NX), F32),
        vmem((STEPS, *shape), F32),
        vmem(shape, F32),
        vmem((STEPS, *shape), F32),
        vmem((STEPS, *shape), F32),
        vmem((LEV, 2, 1, NX), F32),
        vmem(shape, F32),
        vmem(shape, F32),
        vmem((len(PAIRS), 8, 128), F32),
        vmem((len(PAIRS), 8, 128), F32),
        vmem((128, 128), F32),
        vmem((2, 1, 128), F32),
        vmem((NZ, 1, 128), F32),
        vmem((PLANE, 128), F32),
        pltpu.SemaphoreType.DMA((6,)),
        pltpu.SemaphoreType.DMA((10,)),
        pltpu.SemaphoreType.DMA((2, LEV, MESSAGES)),
        pltpu.SemaphoreType.DMA((5 + LEV * BLOCKS,)),
        pltpu.SemaphoreType.DMA((2,)),
        pltpu.SemaphoreType.REGULAR((3, 3)),
        vmem((BACK_ROWS, 1, 128), F32),
    ]
    solution_field, residual = pl.pallas_call(
        kernel,
        out_shape=(pltpu.VMEM((1, *shape), F32), pltpu.VMEM((1, *shape), F32)),
        in_specs=[pl.BlockSpec(memory_space=hbm)] * 6,
        out_specs=(pl.BlockSpec(memory_space=vmem),) * 2,
        scratch_shapes=scratch,
        compiler_params=pltpu.CompilerParams(collective_id=0, has_side_effects=True),
        name="krylov",
    )(
        right_side.reshape(shape),
        error_weight.reshape(shape),
        coeffs.reshape(4, *shape),
        obs_block,
        obs_pos.reshape(32, 128),
        obs_weight.reshape(32, 128),
    )
    whole = jax.ShapeDtypeStruct((1, *shape), F32)
    return pl.pallas_call(
        store,
        out_shape=(whole, whole),
        in_specs=[pl.BlockSpec(memory_space=vmem)] * 2,
        out_specs=(pl.BlockSpec(memory_space=hbm),) * 2,
        scratch_shapes=[pltpu.SemaphoreType.DMA((2,))],
        name="store",
    )(*(pltpu.with_memory_space_constraint(x, vmem) for x in (solution_field, residual)))


def store(solution_field, residual, solution_out, residual_out, sem):
    copies = [
        pltpu.make_async_copy(solution_field, solution_out, sem.at[0]),
        pltpu.make_async_copy(residual, residual_out, sem.at[1]),
    ]
    for copy in copies:
        copy.start()
    for copy in copies:
        copy.wait()


def solution(mesh):
    in_specs = (
        P("win", None, "tile", None),
        P("win", None, "tile", None),
        P(None, "win", None, "tile", None),
        P("win", "tile"),
        P("win", "tile", None),
        P("win", "tile", None),
    )
    out_specs = (P("win", None, "tile", None), P("win", None, "tile", None))
    return jax.shard_map(on_device, mesh=mesh, in_specs=in_specs, out_specs=out_specs, check_vma=False)
```

```python
import jax
import jax.numpy as jnp
from jax import lax
from jax.experimental import pallas as pl
from jax.experimental.pallas import tpu as pltpu
from jax.sharding import PartitionSpec as P

MESH = pl.DeviceIdType.MESH
F32 = jnp.float32
LEV, TY, NX = 2, 32, 1024
BLOCKS = TY // 8
STEPS = 3
SCALE = 1.0 / 16.0
NZ, NYC, NCORE, NT = 8, 8, 2, 4
NWIN = NZ * NYC * NCORE
PLANE = NYC * NCORE * NT
PAIRS = ((0, 0), (0, 1), (1, 1), (0, 2), (1, 2), (2, 2), (0, 3), (1, 3), (2, 3))
HALO, BACK, FORE, STATE, IMAGE = 0, 2, 4, 6, 10
MESSAGES = 14
WIDE = NX // 128
SIDE_ROWS = LEV * (2 * STEPS + 4) * WIDE
BACK_ROWS = (STEPS + 1) * LEV * TY * WIDE
AHEAD_ROWS = (STEPS * LEV * TY + 2 * LEV) * WIDE
BACK_SIDE_ROWS = LEV * (STEPS + 1) * WIDE
AHEAD_SIDE_ROWS = LEV * STEPS * WIDE
EARLY = 6
MIDDLE = (1, 2)
OUTER = ((0, 1), (TY - 1, TY - 2))


def two_sum(a, b):
    s = a + b
    t = s - a
    return s, (a - (s - t)) + (b - t)


def quick_sum(a, b):
    s = a + b
    return s, b - (s - a)


def split(a):
    c = a * 4097.0
    high = c - (c - a)
    return high, a - high


def two_prod_split(a, b, sa, sb):
    p = a * b
    return p, ((sa[0] * sb[0] - p) + sa[0] * sb[1] + sa[1] * sb[0]) + sa[1] * sb[1]


def two_prod(a, b):
    return two_prod_split(a, b, split(a), split(b))


def add2(a, b):
    s, e = two_sum(a[0], b[0])
    return quick_sum(s, e + (a[1] + b[1]))


def neg2(a):
    return -a[0], -a[1]


def sub2(a, b):
    return add2(a, neg2(b))


def mul2(a, b):
    p, e = two_prod(a[0], b[0])
    return quick_sum(p, e + (a[0] * b[1] + a[1] * b[0]))


def div2(a, b):
    zero = jnp.zeros_like(a[0])
    first = a[0] / b[0]
    rest = sub2(a, mul2((first, zero), b))
    return quick_sum(first, rest[0] / b[0])


def plus(a, b):
    s, e = two_sum(a[0], b[0])
    return s, (a[1] + b[1]) + e


def tree2(items):
    while len(items) > 1:
        items = [
            plus(items[i], items[i + 1]) if i + 1 < len(items) else items[i]
            for i in range(0, len(items), 2)
        ]
    return items[0]


def rolled(pair, shift, axis):
    return pltpu.roll(pair[0], shift, axis), pltpu.roll(pair[1], shift, axis)


def kernel(
    right_hbm,
    weight_hbm,
    coeff_hbm,
    block_hbm,
    pos_hbm,
    obsw_hbm,
    solution_out,
    residual_out,
    v0,
    v1,
    v2,
    v3,
    weight,
    coeff,
    block,
    pos,
    obsw,
    diag,
    edge,
    coeff_edge,
    centre_edge,
    weight_edge,
    halo,
    coeff_halo,
    weight_halo,
    next_halo,
    prev_halo,
    prev_centre,
    next_state,
    next_weight,
    term,
    next_term,
    image,
    before,
    spread_halo,
    follow,
    spread,
    gram_high,
    gram_low,
    gram_line,
    row_send,
    row_recv,
    plane_recv,
    far_recv,
    final_line,
    local_sem,
    send_sem,
    recv_sem,
    once_sem,
    rrecv_sem,
    known_sem,
    ballast,
):
    win = lax.axis_index("win")
    tile = lax.axis_index("tile")
    core = win % 2
    chip_y = (win // 2) % 8
    chip_z = win // 16
    has_prev, has_next = win > 0, win < NWIN - 1
    has_north, has_south = tile > 0, tile < NT - 1
    prev_id, next_id = (win - 1, tile), (win + 1, tile)
    states = (v0, v1, v2, v3)

    loads = [
        pltpu.make_async_copy(src, dst, local_sem.at[i])
        for i, (src, dst) in enumerate(
            (
                (right_hbm, v0),
                (weight_hbm, weight),
                (coeff_hbm, coeff),
                (block_hbm, block),
                (pos_hbm, pos),
                (obsw_hbm, obsw),
            )
        )
    ]
    for load in loads:
        load.start()

    def along_y(by):
        return (win + 2 * ((chip_y + by) % NYC - chip_y), tile)

    def along_z(by, other_core=False):
        start = win + 1 - 2 * core if other_core else win
        return (start + 16 * ((chip_z + by) % NZ - chip_z), tile)

    group = core * NT + tile
    slot_a = chip_y * 8 + group
    near = [
        (win - core + ((group + i) % 8) // NT, (group + i) % NT) for i in range(1, NCORE * NT)
    ]
    near += [along_y(1), along_y(-1)]
    near += [along_z(by, other) for by in (1, -1) for other in (False, True)]

    def signal(semaphore, peer):
        pl.semaphore_signal(semaphore, inc=1, device_id=peer, device_id_type=MESH)

    barrier = pltpu.get_barrier_semaphore()

    @pl.when(has_prev)
    def _():
        signal(barrier, prev_id)

    @pl.when(has_next)
    def _():
        signal(barrier, next_id)

    for peer in near:
        signal(barrier, peer)

    for i in range(2):
        loads[i].wait()
    for side in range(2):
        for l in range(LEV):
            for n, row in enumerate(OUTER[side]):
                edge[0, l, side, n] = v0[l, row : row + 1, :]
            row = OUTER[side][0]
            weight_edge[side, l] = weight[l, row : row + 1, :]

    pl.semaphore_wait(barrier, len(near) + jnp.where(has_prev, 1, 0) + jnp.where(has_next, 1, 0))

    def remote(src, dst, send, recv, peer):
        return pltpu.make_async_remote_copy(
            src_ref=src, dst_ref=dst, send_sem=send, recv_sem=recv, device_id=peer, device_id_type=MESH
        )

    def start_if(condition, copies):
        @pl.when(condition)
        def _():
            for copy in copies:
                copy.start()

    def wait_if(condition, copies):
        @pl.when(condition)
        def _():
            for copy in copies:
                copy.wait_recv()

    beside = (has_north, has_south)

    def towards(side, by):
        return (win + by, tile + (1 if side else -1))

    def and_(*conditions):
        total = conditions[0]
        for condition in conditions[1:]:
            total = jnp.logical_and(total, condition)
        return total

    def to_side(kind, j, l, side):
        sem = recv_sem.at[j % 2, l, kind + 1 - side]
        if kind == HALO:
            return remote(edge.at[j, l, side], halo.at[j, l, 1 - side], send_sem.at[side], sem, towards(side, 0))
        dst, out, by = (next_halo, 4, -1) if kind == BACK else (prev_halo, 6, 1)
        return remote(
            edge.at[j, l, side, 0], dst.at[j, l, 1 - side], send_sem.at[out + side], sem, towards(side, by)
        )

    def send_edges(j, l, side, diagonal=True, straight=True):
        if straight:
            start_if(beside[side], [to_side(HALO, j, l, side)])
        if diagonal:
            start_if(and_(beside[side], has_prev), [to_side(BACK, j, l, side)])
            start_if(and_(beside[side], has_next), [to_side(FORE, j, l, side)])

    def edges_from(kind, j, l, side):
        extra = {HALO: (), BACK: (has_next,), FORE: (has_prev,)}[kind]
        wait_if(and_(beside[side], *extra), [to_side(kind, j, l, 1 - side)])

    def state_block(j, l, b):
        at = pl.ds(8 * b, 8)
        return remote(
            states[j].at[l, at], next_state.at[j, l, at], send_sem.at[2], recv_sem.at[j % 2, l, STATE + b], prev_id
        )

    def image_block(j, l, b):
        at = pl.ds(8 * b, 8)
        return remote(
            image.at[j, l, at], before.at[j, l, at], send_sem.at[3], recv_sem.at[j % 2, l, IMAGE + b], next_id
        )

    def first_block(l, b):
        return state_block(0, l, b)

    def weight_block(l, b):
        at = pl.ds(8 * b, 8)
        return remote(
            weight.at[l, at], next_weight.at[l, at], send_sem.at[2], once_sem.at[5 + BLOCKS * l + b], prev_id
        )

    def term_block(b):
        n = MIDDLE.index(b)
        return remote(
            term.at[n], next_term.at[n], send_sem.at[2], once_sem.at[5 + BLOCKS * LEV + n], prev_id
        )

    def from_next(j, l, b):
        return j == 0 and l == LEV - 1 and b in MIDDLE

    def coeff_side(side):
        return remote(
            coeff_edge.at[side], coeff_halo.at[1 - side], send_sem.at[side], once_sem.at[1 - side], towards(side, 0)
        )

    def weight_side(side):
        return remote(
            weight_edge.at[side],
            weight_halo.at[1 - side],
            send_sem.at[4 + side],
            once_sem.at[3 - side],
            towards(side, -1),
        )

    def centre_ahead():
        return remote(centre_edge, prev_centre, send_sem.at[3], once_sem.at[4], next_id)

    row_id = lax.broadcasted_iota(jnp.int32, (8, NX), 0)
    first_row, last_row = row_id == 0, row_id == 7

    def rows(b):
        return slice(8 * b, 8 * b + 8)

    def vertical(ref, l, b, top=0.0, bottom=0.0):
        here = ref[l, rows(b), :]
        above = pltpu.roll(ref[l, rows(b - 1), :], 1, 0) if b > 0 else top
        below = pltpu.roll(ref[l, rows(b + 1), :], 7, 0) if b < BLOCKS - 1 else bottom
        north = jnp.where(first_row, above, pltpu.roll(here, 1, 0))
        south = jnp.where(last_row, below, pltpu.roll(here, 7, 0))
        return north + south

    def edge_only(side, value):
        return jnp.where((first_row, last_row)[side], value, 0.0)

    def propagate(j, l, b):
        v = states[j]
        here = v[l, rows(b), :]
        image[j, l, rows(b), :] = (
            coeff[0, l, rows(b), :] * here
            + coeff[1, l, rows(b), :] * vertical(v, l, b)
            + coeff[2, l, rows(b), :] * pltpu.roll(here, NX - 1, 1)
            + coeff[3, l, rows(b), :] * pltpu.roll(here, 1, 1)
        )
        if j > 0 or l == 0 or from_next(j, l, b):
            start_if(has_next, [image_block(j, l, b)])

    def side_of(b):
        return {0: 0, BLOCKS - 1: 1}.get(b)

    def outside(j, l, side):
        edges_from(HALO, j, l, side)
        if j == 0 and l == 0:
            wait_if(beside[side], [coeff_side(1 - side)])
            wait_if(and_(beside[side], has_next), [weight_side(1 - side)])
        near_row, far_row = halo[j, l, side, 0], halo[j, l, side, 1]
        row = OUTER[side][0]
        here = (
            coeff_halo[side, l, 0] * near_row
            + coeff_halo[side, l, 1] * (far_row + states[j][l, row : row + 1, :])
            + coeff_halo[side, l, 2] * pltpu.roll(near_row, NX - 1, 1)
            + coeff_halo[side, l, 3] * pltpu.roll(near_row, 1, 1)
        )
        edges_from(BACK, j, l, side)
        f = weight_halo[side, l] * (next_halo[j, l, side] - here)
        spread_halo[l, side] = coeff_halo[side, l, 1] * f

    def finish(j, l, order, at):
        b = order[at]
        v, out = states[j], states[j + 1]
        side = side_of(b)
        f = follow[l, rows(b), :]
        top = spread_halo[l, 0] if side == 0 else 0.0
        bottom = spread_halo[l, 1] if side == 1 else 0.0
        back_image = (
            coeff[0, l, rows(b), :] * f
            + vertical(spread, l, b, top, bottom)
            + pltpu.roll(coeff[2, l, rows(b), :] * f, 1, 1)
            + pltpu.roll(coeff[3, l, rows(b), :] * f, NX - 1, 1)
        )
        here = v[l, rows(b), :]
        out[l, rows(b), :] = weight[l, rows(b), :] * here - back_image + diag[l, rows(b), :] * here
        if not from_next(j, l, b):
            wait_if(has_prev, [image_block(j, l, b)])
        came = before[j, l, rows(b), :]
        if side is not None:
            edges_from(FORE, j, l, side)
            if j == 0 and l == 0 and at == 0:
                wait_if(has_prev, [centre_ahead()])
            came = came + edge_only(side, prev_centre[l, side] * prev_halo[j, l, side])
        out[l, rows(b), :] = SCALE * (out[l, rows(b), :] - weight[l, rows(b), :] * came)
        if j + 1 == STEPS:
            keep(j, gram_block(j, l, rows(b), kept(j)))
            return
        if side is not None:
            for n, row in enumerate(OUTER[side]):
                edge[j + 1, l, side, n] = out[l, row : row + 1, :]
            send_edges(j + 1, l, side)
        start_if(has_prev, [state_block(j + 1, l, b)])
        if at > 0:
            propagate(j + 1, l, order[at - 1])
        if at == BLOCKS - 1:
            propagate(j + 1, l, b)

    def complete(j, l, order):
        for at, b in enumerate(order):
            side = side_of(b)
            if side is not None:
                outside(j, l, side)
            if from_next(j, l, b):
                wait_if(has_next, [term_block(b)])
                f = next_term[MIDDLE.index(b)]
            else:
                first = j == (1 if from_next(0, l, b) else 0)
                wait_if(has_next, [state_block(j, l, b), *([weight_block(l, b)] if first else [])])
                sent_image = image[j, l, rows(b), :]
                if side is not None:
                    sent_image = sent_image + edge_only(side, coeff[1, l, rows(b), :] * halo[j, l, side, 0])
                f = next_weight[l, rows(b), :] * (next_state[j, l, rows(b), :] - sent_image)
            follow[l, rows(b), :] = f
            spread[l, rows(b), :] = coeff[1, l, rows(b), :] * f
            if at > 0:
                finish(j, l, order, at - 1)
        finish(j, l, order, BLOCKS - 1)

    def by_parity(body):
        pl.when(tile % 2 == 0)(lambda: body(tuple(range(BLOCKS))))
        pl.when(tile % 2 == 1)(lambda: body(tuple(reversed(range(BLOCKS)))))

    def gram_block(group, l, at, acc):
        acc = list(acc)
        for c in range(NX // 128):
            parts = {}
            for n in range(3):
                i, k = PAIRS[3 * group + n]
                for s in (i, k):
                    if s not in parts:
                        x = states[s][l, at, c * 128 : (c + 1) * 128]
                        parts[s] = (x, split(x))
                p, e = two_prod_split(parts[i][0], parts[k][0], parts[i][1], parts[k][1])
                s, f = two_sum(acc[2 * n], p)
                acc[2 * n], acc[2 * n + 1] = s, acc[2 * n + 1] + (e + f)
        return tuple(acc)

    def keep(group, acc):
        for n in range(3):
            gram_high[3 * group + n], gram_low[3 * group + n] = acc[2 * n], acc[2 * n + 1]

    def kept(group):
        return tuple(ref[3 * group + n] for n in range(3) for ref in (gram_high, gram_low))

    def gram_lines(group):
        acc = kept(group)
        for n in range(3):
            index = 3 * group + n
            line = over_rows((acc[2 * n], acc[2 * n + 1]))
            gram_line[index : index + 1, :], gram_line[16 + index : 17 + index, :] = line

    def gram(group):
        def step(n, acc):
            at = pl.ds(pl.multiple_of((n % BLOCKS) * 8, 8), 8)
            return gram_block(group, n // BLOCKS, at, acc)

        keep(group, lax.fori_loop(0, LEV * BLOCKS, step, (jnp.zeros((8, 128), F32),) * 6))
        gram_lines(group)

    def over_rows(total):
        for shift in (4, 2, 1):
            total = plus(total, rolled(total, shift, 0))
        return total[0][0:1, :], total[1][0:1, :]

    def observed_weights():
        pos_t = jnp.swapaxes(pos[...], 0, 1)
        obsw_t = jnp.swapaxes(obsw[...], 0, 1)
        lane = lax.broadcasted_iota(jnp.int32, (128, 128), 1)
        lines = []
        for b in range(32):
            hit = pos_t[:, b : b + 1] == lane
            lines.append(jnp.sum(jnp.where(hit, obsw_t[:, b : b + 1], 0.0), axis=0, keepdims=True))
        per_block = jnp.concatenate(lines, axis=0)
        row = lax.broadcasted_iota(jnp.int32, (LEV * TY, 32), 0)
        for c in range(NX // 128):
            hot = (block[...] == row * (NX // 128) + c).astype(F32)
            out = jnp.dot(hot, per_block, precision=lax.Precision.HIGHEST, preferred_element_type=F32)
            for l in range(LEV):
                diag[l, :, c * 128 : (c + 1) * 128] = out[l * TY : (l + 1) * TY, :]

    def zeros(*refs):
        for ref in refs:
            ref[...] = jnp.zeros(ref.shape, F32)

    gram_line[...] = jnp.zeros((128, 128), F32)
    for side in range(2):
        for by in range(LEV):
            send_edges(0, by, side, diagonal=False)
        pl.when(beside[side])(lambda side=side: signal(known_sem.at[2, 0], towards(side, 0)))
    def bulk(order):
        places = [(l, b) for l in range(LEV) for b in order if not from_next(0, l, b)]
        return [copy(*place) for place in places for copy in (first_block, weight_block)]

    by_parity(lambda order: start_if(has_prev, bulk(order)[:EARLY]))
    loads[2].wait()

    @by_parity
    def _(order):
        places = [(l, b) for l in range(LEV) for b in order]
        for place in sorted(places, key=lambda place: not from_next(0, *place)):
            propagate(0, *place)

    def pass_on(number):
        if number > 0:
            pl.semaphore_wait(known_sem.at[(number - 1) // 3, (number - 1) % 3], 2)
        if number < 6:
            move, by = (along_y, along_z)[number // 3], (1, 2, 1)[number % 3]
            for peer in (move(by), move(-by)):
                signal(known_sem.at[number // 3, number % 3], peer)

    pass_on(0)
    pl.semaphore_wait(known_sem.at[2, 0], jnp.where(has_north, 1, 0) + jnp.where(has_south, 1, 0))
    for side in range(2):
        start_if(and_(beside[side], has_prev), [weight_side(side)])
        for l in range(LEV):
            send_edges(0, l, side, straight=False)
    by_parity(lambda order: start_if(has_prev, bulk(order)[EARLY:]))
    for side in range(2):
        row = OUTER[side][0]
        for l in range(LEV):
            for n in range(4):
                coeff_edge[side, l, n] = coeff[n, l, row : row + 1, :]
            centre_edge[l, side] = coeff[1, l, row : row + 1, :]
    for side in range(2):
        start_if(beside[side], [coeff_side(side)])
    start_if(has_next, [centre_ahead()])
    by_parity(lambda order: start_if(has_next, [image_block(0, 1, b) for b in order if b not in MIDDLE]))
    for side in range(2):

        @pl.when(jnp.logical_not(beside[side]))
        def _(side=side):
            zeros(coeff_halo.at[side], weight_halo.at[side])
            for j in range(STEPS):
                for l in range(LEV):
                    zeros(halo.at[j, l, side], next_halo.at[j, l, side], prev_halo.at[j, l, side])

    pl.when(jnp.logical_not(has_prev))(lambda: zeros(before, prev_halo, prev_centre))
    pl.when(jnp.logical_not(has_next))(lambda: zeros(next_state, next_weight, next_term, next_halo, weight_halo))
    for load in loads[3:]:
        load.wait()
    observed_weights()
    pass_on(1)
    @by_parity
    def _(order):
        l = LEV - 1
        inner = [b for b in order if b in MIDDLE]
        for b in inner:
            wait_if(has_prev, [image_block(0, l, b)])
            term[MIDDLE.index(b)] = weight[l, rows(b), :] * (v0[l, rows(b), :] - before[0, l, rows(b), :])
            start_if(has_prev, [term_block(b)])
        start_if(has_prev, [weight_block(l, b) for b in inner])

    for j in range(STEPS):
        if j + 1 == STEPS:
            keep(j, (jnp.zeros((8, 128), F32),) * 6)
        for l in range(LEV):
            by_parity(lambda order, j=j, l=l: complete(j, l, order))
            if j * LEV + l < 5:
                pass_on(j * LEV + l + 2)
        if j + 1 < STEPS:
            gram(j)
    gram_lines(STEPS - 1)

    turned = jnp.swapaxes(gram_line[...], 0, 1)
    pieces = [turned[8 * i : 8 * i + 8, :] for i in range(16)]
    total = over_rows(tree2([(x, pltpu.roll(x, 128 - 16, 1)) for x in pieces]))
    lane = lax.broadcasted_iota(jnp.int32, (1, 128), 1)

    def packed(pair):
        return jnp.where(lane < 16, pair[0], jnp.where(lane < 32, pltpu.roll(pair[1], 16, 1), 0.0))

    line = packed(total)

    def over_slots(parts):
        return over_rows(tree2([(x, pltpu.roll(x, 128 - 16, 1)) for x in parts]))

    def arrived(stage, count):
        whole = ballast.at[pl.ds(0, count)]
        pltpu.make_async_copy(whole, whole, rrecv_sem.at[stage]).wait()

    def to_plane(y, x):
        where = (win - core + 1 + 2 * (y - chip_y), x)
        return remote(
            row_send.at[0], plane_recv.at[pl.ds(slot_a, 1)], send_sem.at[8], rrecv_sem.at[0], where
        )

    def to_z(z, other_core):
        peer = (win + 16 * (z - chip_z) - other_core, tile)
        return remote(row_send.at[1], row_recv.at[chip_z], send_sem.at[9], rrecv_sem.at[1], peer)

    def to_first():
        return remote(
            row_send.at[0],
            far_recv.at[pl.ds(jnp.maximum(win * NT + tile - PLANE, 0), 1)],
            send_sem.at[8],
            rrecv_sem.at[2],
            (1, 0),
        )

    is_second = core == 1
    in_first_column = and_(is_second, chip_y == 0, tile == 0)
    is_first = and_(in_first_column, chip_z == 0)
    row_send[0] = line
    start_if(chip_z > 0, [to_first()])
    for y in range(NYC):
        for x in range(NT):
            start_if(jnp.logical_or(core == 0, chip_y * NT + tile != y * NT + x), [to_plane(y, x)])

    @pl.when(is_second)
    def _():
        plane_recv[pl.ds(slot_a, 1), :] = line
        arrived(0, PLANE - 1)
        plane = over_slots([plane_recv[8 * i : 8 * i + 8, :] for i in range(PLANE // 8)])
        mine = packed(plane)
        row_send[1] = mine
        row_recv[chip_z] = mine
        for z in range(NZ):
            start_if(and_(chip_z != z, jnp.logical_not(in_first_column) if z == 0 else chip_z != z), [to_z(z, 0)])
            to_z(z, 1).start()

        @pl.when(jnp.logical_not(is_first))
        def _():
            arrived(1, NZ - 1)

        @pl.when(is_first)
        def _():
            arrived(2, NWIN * NT - PLANE)
            far = over_slots([far_recv[8 * i : 8 * i + 8, :] for i in range((NWIN * NT - PLANE) // 8)])
            final_line[...] = packed(quick_sum(*plus(plane, far)))

    @pl.when(jnp.logical_not(is_second))
    def _():
        arrived(1, NZ)

    @pl.when(jnp.logical_not(is_first))
    def _():
        total = tree2([(x, pltpu.roll(x, 128 - 16, 1)) for x in [row_recv[i] for i in range(NZ)]])
        final_line[...] = packed(quick_sum(*total))

    line = final_line[...]

    def value(i, j):
        at = PAIRS.index((min(i, j), max(i, j)))
        return tuple(jnp.broadcast_to(line[:, at + off : at + off + 1], (8, 128)) for off in (0, 16))

    a = [[value(i, n + 1) for n in range(3)] + [value(i, 0)] for i in range(3)]
    for pivot in range(2):
        for i in range(pivot + 1, 3):
            factor = div2(a[i][pivot], a[pivot][pivot])
            for n in range(pivot + 1, 4):
                a[i][n] = sub2(a[i][n], mul2(factor, a[pivot][n]))
    zero = jnp.zeros((8, 128), F32)
    c2 = a[2][3][0] / a[2][2][0]
    c1 = sub2(a[1][3], mul2(a[1][2], (c2, zero)))[0] / a[1][1][0]
    left = sub2(a[0][3], mul2(a[0][1], (c1, zero)))
    c0 = sub2(left, mul2(a[0][2], (c2, zero)))[0] / a[0][0][0]
    combo = [jnp.concatenate([c] * (NX // 128), axis=1) for c in (c0, c1, c2)]
    for l in range(LEV):
        for b in range(BLOCKS):
            at = (l, rows(b), slice(None))
            u0, u1, u2, u3 = (s[at] for s in states)
            solution_out[0, l, rows(b), :] = SCALE * (combo[0] * u0 + combo[1] * u1 + combo[2] * u2)
            residual_out[0, l, rows(b), :] = u0 - combo[0] * u1 - combo[1] * u2 - combo[2] * u3

    def sent(condition, count, semaphore):
        @pl.when(condition)
        def _():
            whole = ballast.at[pl.ds(0, count)]
            pltpu.make_async_copy(whole, whole, semaphore).wait()

    for side in range(2):
        sent(beside[side], SIDE_ROWS, send_sem.at[side])
        sent(and_(beside[side], has_prev), BACK_SIDE_ROWS, send_sem.at[4 + side])
        sent(and_(beside[side], has_next), AHEAD_SIDE_ROWS, send_sem.at[6 + side])
    sent(has_prev, BACK_ROWS, send_sem.at[2])
    sent(has_next, AHEAD_ROWS, send_sem.at[3])
    more = jnp.where(chip_z > 0, 1, 0)
    sent_lines = PLANE // 2 - core + more
    for count in (PLANE // 2 - 1, PLANE // 2, PLANE // 2 + 1):
        sent(sent_lines == count, count, send_sem.at[8])
    skips_first = and_(in_first_column, chip_z > 0)
    sent(and_(is_second, jnp.logical_not(skips_first)), 2 * NZ - 1, send_sem.at[9])
    sent(skips_first, 2 * NZ - 2, send_sem.at[9])


def on_device(right_side, error_weight, coeffs, obs_block, obs_pos, obs_weight):
    shape = (LEV, TY, NX)
    vmem, hbm = pltpu.VMEM, pltpu.HBM
    line = (STEPS, LEV, 2, 1, NX)
    scratch = [
        vmem(shape, F32),
        vmem(shape, F32),
        vmem(shape, F32),
        vmem(shape, F32),
        vmem(shape, F32),
        vmem((4, *shape), F32),
        vmem((1, 32), jnp.int32),
        vmem((32, 128), jnp.int32),
        vmem((32, 128), F32),
        vmem(shape, F32),
        vmem((STEPS, LEV, 2, 2, 1, NX), F32),
        vmem((2, LEV, 4, 1, NX), F32),
        vmem((LEV, 2, 1, NX), F32),
        vmem((2, LEV, 1, NX), F32),
        vmem((STEPS, LEV, 2, 2, 1, NX), F32),
        vmem((2, LEV, 4, 1, NX), F32),
        vmem((2, LEV, 1, NX), F32),
        vmem(line, F32),
        vmem(line, F32),
        vmem((LEV, 2, 1, NX), F32),
        vmem((STEPS, *shape), F32),
        vmem(shape, F32),
        vmem((2, 8, NX), F32),
        vmem((2, 8, NX), F32),
        vmem((STEPS, *shape), F32),
        vmem((STEPS, *shape), F32),
        vmem((LEV, 2, 1, NX), F32),
        vmem(shape, F32),
        vmem(shape, F32),
        vmem((len(PAIRS), 8, 128), F32),
        vmem((len(PAIRS), 8, 128), F32),
        vmem((128, 128), F32),
        vmem((2, 1, 128), F32),
        vmem((NZ, 1, 128), F32),
        vmem((PLANE, 128), F32),
        vmem((NWIN * NT - PLANE, 128), F32),
        vmem((1, 128), F32),
        pltpu.SemaphoreType.DMA((6,)),
        pltpu.SemaphoreType.DMA((10,)),
        pltpu.SemaphoreType.DMA((2, LEV, MESSAGES)),
        pltpu.SemaphoreType.DMA((5 + LEV * BLOCKS + 2,)),
        pltpu.SemaphoreType.DMA((3,)),
        pltpu.SemaphoreType.REGULAR((3, 3)),
        vmem((BACK_ROWS, 1, 128), F32),
    ]
    solution_field, residual = pl.pallas_call(
        kernel,
        out_shape=(pltpu.VMEM((1, *shape), F32), pltpu.VMEM((1, *shape), F32)),
        in_specs=[pl.BlockSpec(memory_space=hbm)] * 6,
        out_specs=(pl.BlockSpec(memory_space=vmem),) * 2,
        scratch_shapes=scratch,
        compiler_params=pltpu.CompilerParams(collective_id=0, has_side_effects=True),
        name="krylov",
    )(
        right_side.reshape(shape),
        error_weight.reshape(shape),
        coeffs.reshape(4, *shape),
        obs_block,
        obs_pos.reshape(32, 128),
        obs_weight.reshape(32, 128),
    )
    whole = jax.ShapeDtypeStruct((1, *shape), F32)
    return pl.pallas_call(
        store,
        out_shape=(whole, whole),
        in_specs=[pl.BlockSpec(memory_space=vmem)] * 2,
        out_specs=(pl.BlockSpec(memory_space=hbm),) * 2,
        scratch_shapes=[pltpu.SemaphoreType.DMA((2,))],
        name="store",
    )(*(pltpu.with_memory_space_constraint(x, vmem) for x in (solution_field, residual)))


def store(solution_field, residual, solution_out, residual_out, sem):
    copies = [
        pltpu.make_async_copy(solution_field, solution_out, sem.at[0]),
        pltpu.make_async_copy(residual, residual_out, sem.at[1]),
    ]
    for copy in copies:
        copy.start()
    for copy in copies:
        copy.wait()


def solution(mesh):
    in_specs = (
        P("win", None, "tile", None),
        P("win", None, "tile", None),
        P(None, "win", None, "tile", None),
        P("win", "tile"),
        P("win", "tile", None),
        P("win", "tile", None),
    )
    out_specs = (P("win", None, "tile", None), P("win", None, "tile", None))
    return jax.shard_map(on_device, mesh=mesh, in_specs=in_specs, out_specs=out_specs, check_vma=False)
```

```python
import jax
import jax.numpy as jnp
from jax import lax
from jax.experimental import pallas as pl
from jax.experimental.pallas import tpu as pltpu
from jax.sharding import PartitionSpec as P

MESH = pl.DeviceIdType.MESH
F32 = jnp.float32
LEV, TY, NX = 2, 32, 1024
BLOCKS = TY // 8
STEPS = 3
SCALE = 1.0 / 16.0
NZ, NYC, NCORE, NT = 8, 8, 2, 4
NWIN = NZ * NYC * NCORE
PLANE = NYC * NCORE * NT
PAIRS = ((0, 0), (0, 1), (1, 1), (0, 2), (1, 2), (2, 2), (0, 3), (1, 3), (2, 3))
HALO, BACK, FORE, STATE, IMAGE = 0, 2, 4, 6, 10
MESSAGES = 14
WIDE = NX // 128
SIDE_ROWS = LEV * (2 * STEPS + 4) * WIDE
BACK_ROWS = (STEPS + 1) * LEV * TY * WIDE
AHEAD_ROWS = (STEPS * LEV * TY + 2 * LEV) * WIDE
BACK_SIDE_ROWS = LEV * (STEPS + 1) * WIDE
AHEAD_SIDE_ROWS = LEV * STEPS * WIDE
EARLY = 6
MIDDLE = (1, 2)
OUTER = ((0, 1), (TY - 1, TY - 2))


def two_sum(a, b):
    s = a + b
    t = s - a
    return s, (a - (s - t)) + (b - t)


def quick_sum(a, b):
    s = a + b
    return s, b - (s - a)


def split(a):
    c = a * 4097.0
    high = c - (c - a)
    return high, a - high


def two_prod_split(a, b, sa, sb):
    p = a * b
    return p, ((sa[0] * sb[0] - p) + sa[0] * sb[1] + sa[1] * sb[0]) + sa[1] * sb[1]


def two_prod(a, b):
    return two_prod_split(a, b, split(a), split(b))


def add2(a, b):
    s, e = two_sum(a[0], b[0])
    return quick_sum(s, e + (a[1] + b[1]))


def neg2(a):
    return -a[0], -a[1]


def sub2(a, b):
    return add2(a, neg2(b))


def mul2(a, b):
    p, e = two_prod(a[0], b[0])
    return quick_sum(p, e + (a[0] * b[1] + a[1] * b[0]))


def div2(a, b):
    zero = jnp.zeros_like(a[0])
    first = a[0] / b[0]
    rest = sub2(a, mul2((first, zero), b))
    return quick_sum(first, rest[0] / b[0])


def plus(a, b):
    s, e = two_sum(a[0], b[0])
    return s, (a[1] + b[1]) + e


def tree2(items):
    while len(items) > 1:
        items = [
            plus(items[i], items[i + 1]) if i + 1 < len(items) else items[i]
            for i in range(0, len(items), 2)
        ]
    return items[0]


def rolled(pair, shift, axis):
    return pltpu.roll(pair[0], shift, axis), pltpu.roll(pair[1], shift, axis)


def kernel(
    right_hbm,
    weight_hbm,
    coeff_hbm,
    block_hbm,
    pos_hbm,
    obsw_hbm,
    solution_out,
    residual_out,
    v0,
    v1,
    v2,
    v3,
    weight,
    coeff,
    block,
    pos,
    obsw,
    diag,
    edge,
    coeff_edge,
    centre_edge,
    weight_edge,
    halo,
    coeff_halo,
    weight_halo,
    next_halo,
    prev_halo,
    prev_centre,
    next_state,
    next_weight,
    term,
    next_term,
    image,
    before,
    spread_halo,
    follow,
    spread,
    gram_high,
    gram_low,
    gram_line,
    row_send,
    row_recv,
    plane_recv,
    far_recv,
    final_line,
    local_sem,
    send_sem,
    recv_sem,
    once_sem,
    rrecv_sem,
    known_sem,
    ballast,
):
    win = lax.axis_index("win")
    tile = lax.axis_index("tile")
    core = win % 2
    chip_y = (win // 2) % 8
    chip_z = win // 16
    has_prev, has_next = win > 0, win < NWIN - 1
    has_north, has_south = tile > 0, tile < NT - 1
    prev_id, next_id = (win - 1, tile), (win + 1, tile)
    states = (v0, v1, v2, v3)

    loads = [
        pltpu.make_async_copy(src, dst, local_sem.at[i])
        for i, (src, dst) in enumerate(
            (
                (right_hbm, v0),
                (weight_hbm, weight),
                (coeff_hbm, coeff),
                (block_hbm, block),
                (pos_hbm, pos),
                (obsw_hbm, obsw),
            )
        )
    ]
    for load in loads:
        load.start()

    def along_y(by):
        return (win + 2 * ((chip_y + by) % NYC - chip_y), tile)

    def along_z(by, other_core=False):
        start = win + 1 - 2 * core if other_core else win
        return (start + 16 * ((chip_z + by) % NZ - chip_z), tile)

    group = core * NT + tile
    slot_a = chip_y * 8 + group
    near = [
        (win - core + ((group + i) % 8) // NT, (group + i) % NT) for i in range(1, NCORE * NT)
    ]
    near = [along_y(1), along_y(-1)] + near
    near = [along_z(by, other) for by in (1, -1) for other in (False, True)] + near

    def signal(semaphore, peer):
        pl.semaphore_signal(semaphore, inc=1, device_id=peer, device_id_type=MESH)

    barrier = pltpu.get_barrier_semaphore()

    @pl.when(has_prev)
    def _():
        signal(barrier, prev_id)

    @pl.when(has_next)
    def _():
        signal(barrier, next_id)

    for peer in near:
        signal(barrier, peer)

    for i in range(2):
        loads[i].wait()
    for side in range(2):
        for l in range(LEV):
            for n, row in enumerate(OUTER[side]):
                edge[0, l, side, n] = v0[l, row : row + 1, :]
            row = OUTER[side][0]
            weight_edge[side, l] = weight[l, row : row + 1, :]

    pl.semaphore_wait(barrier, len(near) + jnp.where(has_prev, 1, 0) + jnp.where(has_next, 1, 0))

    def whole_if(condition, count, semaphore):
        @pl.when(condition)
        def _():
            whole = ballast.at[pl.ds(0, count)]
            pltpu.make_async_copy(whole, whole, semaphore).wait()

    def remote(src, dst, send, recv, peer):
        return pltpu.make_async_remote_copy(
            src_ref=src, dst_ref=dst, send_sem=send, recv_sem=recv, device_id=peer, device_id_type=MESH
        )

    def start_if(condition, copies):
        @pl.when(condition)
        def _():
            for copy in copies:
                copy.start()

    def wait_if(condition, copies):
        @pl.when(condition)
        def _():
            for copy in copies:
                copy.wait_recv()

    beside = (has_north, has_south)

    def towards(side, by):
        return (win + by, tile + (1 if side else -1))

    def and_(*conditions):
        total = conditions[0]
        for condition in conditions[1:]:
            total = jnp.logical_and(total, condition)
        return total

    def to_side(kind, j, l, side):
        sem = recv_sem.at[j % 2, l, kind + 1 - side]
        if kind == HALO:
            return remote(edge.at[j, l, side], halo.at[j, l, 1 - side], send_sem.at[side], sem, towards(side, 0))
        dst, out, by = (next_halo, 4, -1) if kind == BACK else (prev_halo, 6, 1)
        return remote(
            edge.at[j, l, side, 0], dst.at[j, l, 1 - side], send_sem.at[out + side], sem, towards(side, by)
        )

    def send_edges(j, l, side, diagonal=True, straight=True):
        if straight:
            start_if(beside[side], [to_side(HALO, j, l, side)])
        if diagonal:
            start_if(and_(beside[side], has_prev), [to_side(BACK, j, l, side)])
            start_if(and_(beside[side], has_next), [to_side(FORE, j, l, side)])

    def edges_from(kind, j, l, side):
        extra = {HALO: (), BACK: (has_next,), FORE: (has_prev,)}[kind]
        wait_if(and_(beside[side], *extra), [to_side(kind, j, l, 1 - side)])

    def state_block(j, l, b):
        at = pl.ds(8 * b, 8)
        return remote(
            states[j].at[l, at], next_state.at[j, l, at], send_sem.at[2], recv_sem.at[j % 2, l, STATE + b], prev_id
        )

    def image_block(j, l, b):
        at = pl.ds(8 * b, 8)
        return remote(
            image.at[j, l, at], before.at[j, l, at], send_sem.at[3], recv_sem.at[j % 2, l, IMAGE + b], next_id
        )

    def first_block(l, b):
        return state_block(0, l, b)

    def weight_block(l, b):
        at = pl.ds(8 * b, 8)
        late = int(from_next(0, l, b))
        return remote(
            weight.at[l, at], next_weight.at[l, at], send_sem.at[2], recv_sem.at[late, l, STATE + b], prev_id
        )

    def term_block(b):
        n = MIDDLE.index(b)
        return remote(
            term.at[n], next_term.at[n], send_sem.at[2], recv_sem.at[0, LEV - 1, STATE + b], prev_id
        )

    def from_next(j, l, b):
        return j == 0 and l == LEV - 1 and b in MIDDLE

    def coeff_side(side):
        return remote(
            coeff_edge.at[side], coeff_halo.at[1 - side], send_sem.at[side], recv_sem.at[0, 0, HALO + 1 - side], towards(side, 0)
        )

    def weight_side(side):
        return remote(
            weight_edge.at[side],
            weight_halo.at[1 - side],
            send_sem.at[4 + side],
            recv_sem.at[0, 0, BACK + 1 - side],
            towards(side, -1),
        )

    def centre_ahead():
        return remote(centre_edge, prev_centre, send_sem.at[3], once_sem.at[0], next_id)

    row_id = lax.broadcasted_iota(jnp.int32, (8, NX), 0)
    first_row, last_row = row_id == 0, row_id == 7

    def rows(b):
        return slice(8 * b, 8 * b + 8)

    def vertical(ref, l, b, top=0.0, bottom=0.0):
        here = ref[l, rows(b), :]
        above = pltpu.roll(ref[l, rows(b - 1), :], 1, 0) if b > 0 else top
        below = pltpu.roll(ref[l, rows(b + 1), :], 7, 0) if b < BLOCKS - 1 else bottom
        north = jnp.where(first_row, above, pltpu.roll(here, 1, 0))
        south = jnp.where(last_row, below, pltpu.roll(here, 7, 0))
        return north + south

    def edge_only(side, value):
        return jnp.where((first_row, last_row)[side], value, 0.0)

    def propagate(j, l, b):
        v = states[j]
        here = v[l, rows(b), :]
        image[j, l, rows(b), :] = (
            coeff[0, l, rows(b), :] * here
            + coeff[1, l, rows(b), :] * vertical(v, l, b)
            + coeff[2, l, rows(b), :] * pltpu.roll(here, NX - 1, 1)
            + coeff[3, l, rows(b), :] * pltpu.roll(here, 1, 1)
        )
        if j > 0 or l == 0 or from_next(j, l, b):
            start_if(has_next, [image_block(j, l, b)])

    def side_of(b):
        return {0: 0, BLOCKS - 1: 1}.get(b)

    def outside(j, l, side):
        first = j == 0 and l == 0
        if first:
            whole_if(beside[side], (2 + LEV * 4) * WIDE, recv_sem.at[0, 0, HALO + side])
        else:
            edges_from(HALO, j, l, side)
        near_row, far_row = halo[j, l, side, 0], halo[j, l, side, 1]
        row = OUTER[side][0]
        here = (
            coeff_halo[side, l, 0] * near_row
            + coeff_halo[side, l, 1] * (far_row + states[j][l, row : row + 1, :])
            + coeff_halo[side, l, 2] * pltpu.roll(near_row, NX - 1, 1)
            + coeff_halo[side, l, 3] * pltpu.roll(near_row, 1, 1)
        )
        if first:
            whole_if(and_(beside[side], has_next), (1 + LEV) * WIDE, recv_sem.at[0, 0, BACK + side])
        else:
            edges_from(BACK, j, l, side)
        f = weight_halo[side, l] * (next_halo[j, l, side] - here)
        spread_halo[l, side] = coeff_halo[side, l, 1] * f

    def finish(j, l, order, at):
        b = order[at]
        v, out = states[j], states[j + 1]
        side = side_of(b)
        f = follow[l, rows(b), :]
        top = spread_halo[l, 0] if side == 0 else 0.0
        bottom = spread_halo[l, 1] if side == 1 else 0.0
        back_image = (
            coeff[0, l, rows(b), :] * f
            + vertical(spread, l, b, top, bottom)
            + pltpu.roll(coeff[2, l, rows(b), :] * f, 1, 1)
            + pltpu.roll(coeff[3, l, rows(b), :] * f, NX - 1, 1)
        )
        here = v[l, rows(b), :]
        out[l, rows(b), :] = weight[l, rows(b), :] * here - back_image + diag[l, rows(b), :] * here
        if not from_next(j, l, b):
            wait_if(has_prev, [image_block(j, l, b)])
        came = before[j, l, rows(b), :]
        if side is not None:
            edges_from(FORE, j, l, side)
            if j == 0 and l == 0 and at == 0:
                wait_if(has_prev, [centre_ahead()])
            came = came + edge_only(side, prev_centre[l, side] * prev_halo[j, l, side])
        out[l, rows(b), :] = SCALE * (out[l, rows(b), :] - weight[l, rows(b), :] * came)
        if j + 1 == STEPS:
            keep(j, gram_block(j, l, rows(b), kept(j)))
            return
        if side is not None:
            for n, row in enumerate(OUTER[side]):
                edge[j + 1, l, side, n] = out[l, row : row + 1, :]
            send_edges(j + 1, l, side)
        start_if(has_prev, [state_block(j + 1, l, b)])
        if at > 0:
            propagate(j + 1, l, order[at - 1])
        if at == BLOCKS - 1:
            propagate(j + 1, l, b)

    def complete(j, l, order):
        for at, b in enumerate(order):
            side = side_of(b)
            if side is not None:
                outside(j, l, side)
            if from_next(j, l, b):
                wait_if(has_next, [term_block(b)])
                f = next_term[MIDDLE.index(b)]
            else:
                first = j == (1 if from_next(0, l, b) else 0)
                if first:
                    whole_if(has_next, 2 * 8 * WIDE, recv_sem.at[j, l, STATE + b])
                else:
                    wait_if(has_next, [state_block(j, l, b)])
                sent_image = image[j, l, rows(b), :]
                if side is not None:
                    sent_image = sent_image + edge_only(side, coeff[1, l, rows(b), :] * halo[j, l, side, 0])
                f = next_weight[l, rows(b), :] * (next_state[j, l, rows(b), :] - sent_image)
            follow[l, rows(b), :] = f
            spread[l, rows(b), :] = coeff[1, l, rows(b), :] * f
            if at > 0:
                finish(j, l, order, at - 1)
        finish(j, l, order, BLOCKS - 1)

    def by_parity(body):
        pl.when(tile % 2 == 0)(lambda: body(tuple(range(BLOCKS))))
        pl.when(tile % 2 == 1)(lambda: body(tuple(reversed(range(BLOCKS)))))

    def gram_block(group, l, at, acc):
        acc = list(acc)
        for c in range(NX // 128):
            parts = {}
            for n in range(3):
                i, k = PAIRS[3 * group + n]
                for s in (i, k):
                    if s not in parts:
                        x = states[s][l, at, c * 128 : (c + 1) * 128]
                        parts[s] = (x, split(x))
                p, e = two_prod_split(parts[i][0], parts[k][0], parts[i][1], parts[k][1])
                s, f = two_sum(acc[2 * n], p)
                acc[2 * n], acc[2 * n + 1] = s, acc[2 * n + 1] + (e + f)
        return tuple(acc)

    def keep(group, acc):
        for n in range(3):
            gram_high[3 * group + n], gram_low[3 * group + n] = acc[2 * n], acc[2 * n + 1]

    def kept(group):
        return tuple(ref[3 * group + n] for n in range(3) for ref in (gram_high, gram_low))

    def gram_lines(group):
        acc = kept(group)
        for n in range(3):
            index = 3 * group + n
            line = over_rows((acc[2 * n], acc[2 * n + 1]))
            gram_line[index : index + 1, :], gram_line[16 + index : 17 + index, :] = line

    def gram(group):
        def step(n, acc):
            at = pl.ds(pl.multiple_of((n % BLOCKS) * 8, 8), 8)
            return gram_block(group, n // BLOCKS, at, acc)

        keep(group, lax.fori_loop(0, LEV * BLOCKS, step, (jnp.zeros((8, 128), F32),) * 6))
        gram_lines(group)

    def over_rows(total):
        for shift in (4, 2, 1):
            total = plus(total, rolled(total, shift, 0))
        return total[0][0:1, :], total[1][0:1, :]

    def observed_weights():
        pos_t = jnp.swapaxes(pos[...], 0, 1)
        obsw_t = jnp.swapaxes(obsw[...], 0, 1)
        lane = lax.broadcasted_iota(jnp.int32, (128, 128), 1)
        lines = []
        for b in range(32):
            hit = pos_t[:, b : b + 1] == lane
            lines.append(jnp.sum(jnp.where(hit, obsw_t[:, b : b + 1], 0.0), axis=0, keepdims=True))
        per_block = jnp.concatenate(lines, axis=0)
        row = lax.broadcasted_iota(jnp.int32, (LEV * TY, 32), 0)
        for c in range(NX // 128):
            hot = (block[...] == row * (NX // 128) + c).astype(F32)
            out = jnp.dot(hot, per_block, precision=lax.Precision.HIGHEST, preferred_element_type=F32)
            for l in range(LEV):
                diag[l, :, c * 128 : (c + 1) * 128] = out[l * TY : (l + 1) * TY, :]

    def zeros(*refs):
        for ref in refs:
            ref[...] = jnp.zeros(ref.shape, F32)

    gram_line[...] = jnp.zeros((128, 128), F32)
    for side in range(2):
        for by in range(LEV):
            send_edges(0, by, side, diagonal=False)
        pl.when(beside[side])(lambda side=side: signal(known_sem.at[6], towards(side, 0)))
    def bulk(order):
        places = [(l, b) for l in range(LEV) for b in order if not from_next(0, l, b)]
        return [copy(*place) for place in places for copy in (first_block, weight_block)]

    by_parity(lambda order: start_if(has_prev, bulk(order)[:EARLY]))
    loads[2].wait()

    @by_parity
    def _(order):
        places = [(l, b) for l in range(LEV) for b in order]
        for place in sorted(places, key=lambda place: not from_next(0, *place)):
            propagate(0, *place)

    def pass_on(number):
        if number > 0:
            pl.semaphore_wait(known_sem.at[number - 1], 2)
        if number < 6:
            move, by = (along_y, along_z)[number // 3], (1, 2, 1)[number % 3]
            for peer in (move(by), move(-by)):
                signal(known_sem.at[number], peer)

    pass_on(0)
    pl.semaphore_wait(known_sem.at[6], jnp.where(has_north, 1, 0) + jnp.where(has_south, 1, 0))
    for side in range(2):
        start_if(and_(beside[side], has_prev), [weight_side(side)])
        for l in range(LEV):
            send_edges(0, l, side, straight=False)
    by_parity(lambda order: start_if(has_prev, bulk(order)[EARLY:]))
    for side in range(2):
        row = OUTER[side][0]
        for l in range(LEV):
            for n in range(4):
                coeff_edge[side, l, n] = coeff[n, l, row : row + 1, :]
            centre_edge[l, side] = coeff[1, l, row : row + 1, :]
    for side in range(2):
        start_if(beside[side], [coeff_side(side)])
    start_if(has_next, [centre_ahead()])
    by_parity(lambda order: start_if(has_next, [image_block(0, 1, b) for b in order if b not in MIDDLE]))
    for side in range(2):

        @pl.when(jnp.logical_not(beside[side]))
        def _(side=side):
            zeros(coeff_halo.at[side], weight_halo.at[side])
            for j in range(STEPS):
                for l in range(LEV):
                    zeros(halo.at[j, l, side], next_halo.at[j, l, side], prev_halo.at[j, l, side])

    pl.when(jnp.logical_not(has_prev))(lambda: zeros(before, prev_halo, prev_centre))
    pl.when(jnp.logical_not(has_next))(lambda: zeros(next_state, next_weight, next_term, next_halo, weight_halo))
    for load in loads[3:]:
        load.wait()
    observed_weights()
    pass_on(1)
    @by_parity
    def _(order):
        l = LEV - 1
        inner = [b for b in order if b in MIDDLE]
        for b in inner:
            wait_if(has_prev, [image_block(0, l, b)])
            term[MIDDLE.index(b)] = weight[l, rows(b), :] * (v0[l, rows(b), :] - before[0, l, rows(b), :])
            start_if(has_prev, [term_block(b)])
        start_if(has_prev, [weight_block(l, b) for b in inner])

    for j in range(STEPS):
        if j + 1 == STEPS:
            keep(j, (jnp.zeros((8, 128), F32),) * 6)
        for l in range(LEV):
            by_parity(lambda order, j=j, l=l: complete(j, l, order))
            if j * LEV + l < 5:
                pass_on(j * LEV + l + 2)
        if j + 1 < STEPS:
            gram(j)
    gram_lines(STEPS - 1)

    turned = jnp.swapaxes(gram_line[...], 0, 1)
    pieces = [turned[8 * i : 8 * i + 8, :] for i in range(16)]
    total = over_rows(tree2([(x, pltpu.roll(x, 128 - 16, 1)) for x in pieces]))
    lane = lax.broadcasted_iota(jnp.int32, (1, 128), 1)

    def packed(pair):
        return jnp.where(lane < 16, pair[0], jnp.where(lane < 32, pltpu.roll(pair[1], 16, 1), 0.0))

    line = packed(total)

    def over_slots(parts):
        return over_rows(tree2([(x, pltpu.roll(x, 128 - 16, 1)) for x in parts]))

    def arrived(stage, count):
        whole = ballast.at[pl.ds(0, count)]
        pltpu.make_async_copy(whole, whole, rrecv_sem.at[stage]).wait()

    def to_plane(y, x):
        where = (win - core + 1 + 2 * (y - chip_y), x)
        return remote(
            row_send.at[0], plane_recv.at[pl.ds(slot_a, 1)], send_sem.at[8], rrecv_sem.at[0], where
        )

    def to_z(z, other_core):
        peer = (win + 16 * (z - chip_z) - other_core, tile)
        return remote(row_send.at[1], row_recv.at[chip_z], send_sem.at[9], rrecv_sem.at[1], peer)

    def to_first():
        return remote(
            row_send.at[0],
            far_recv.at[pl.ds(jnp.maximum(win * NT + tile - PLANE, 0), 1)],
            send_sem.at[8],
            rrecv_sem.at[2],
            (1, 0),
        )

    is_second = core == 1
    in_first_column = and_(is_second, chip_y == 0, tile == 0)
    is_first = and_(in_first_column, chip_z == 0)
    row_send[0] = line
    start_if(chip_z > 0, [to_first()])
    for y in range(NYC):
        for x in range(NT):
            start_if(jnp.logical_or(core == 0, chip_y * NT + tile != y * NT + x), [to_plane(y, x)])

    @pl.when(is_second)
    def _():
        plane_recv[pl.ds(slot_a, 1), :] = line
        arrived(0, PLANE - 1)
        plane = over_slots([plane_recv[8 * i : 8 * i + 8, :] for i in range(PLANE // 8)])
        mine = packed(plane)
        row_send[1] = mine
        row_recv[chip_z] = mine
        for z in range(NZ):
            start_if(and_(chip_z != z, jnp.logical_not(in_first_column) if z == 0 else chip_z != z), [to_z(z, 0)])
            to_z(z, 1).start()

        @pl.when(jnp.logical_not(is_first))
        def _():
            arrived(1, NZ - 1)

        @pl.when(is_first)
        def _():
            arrived(2, NWIN * NT - PLANE)
            far = over_slots([far_recv[8 * i : 8 * i + 8, :] for i in range((NWIN * NT - PLANE) // 8)])
            final_line[...] = packed(quick_sum(*plus(plane, far)))

    @pl.when(jnp.logical_not(is_second))
    def _():
        arrived(1, NZ)

    @pl.when(jnp.logical_not(is_first))
    def _():
        total = tree2([(x, pltpu.roll(x, 128 - 16, 1)) for x in [row_recv[i] for i in range(NZ)]])
        final_line[...] = packed(quick_sum(*total))

    line = final_line[...]

    def value(i, j):
        at = PAIRS.index((min(i, j), max(i, j)))
        return tuple(jnp.broadcast_to(line[:, at + off : at + off + 1], (8, 128)) for off in (0, 16))

    a = [[value(i, n + 1) for n in range(3)] + [value(i, 0)] for i in range(3)]
    for pivot in range(2):
        for i in range(pivot + 1, 3):
            factor = div2(a[i][pivot], a[pivot][pivot])
            for n in range(pivot + 1, 4):
                a[i][n] = sub2(a[i][n], mul2(factor, a[pivot][n]))
    zero = jnp.zeros((8, 128), F32)
    c2 = a[2][3][0] / a[2][2][0]
    c1 = sub2(a[1][3], mul2(a[1][2], (c2, zero)))[0] / a[1][1][0]
    left = sub2(a[0][3], mul2(a[0][1], (c1, zero)))
    c0 = sub2(left, mul2(a[0][2], (c2, zero)))[0] / a[0][0][0]
    combo = [jnp.concatenate([c] * (NX // 128), axis=1) for c in (c0, c1, c2)]
    for l in range(LEV):
        for b in range(BLOCKS):
            at = (l, rows(b), slice(None))
            u0, u1, u2, u3 = (s[at] for s in states)
            solution_out[0, l, rows(b), :] = SCALE * (combo[0] * u0 + combo[1] * u1 + combo[2] * u2)
            residual_out[0, l, rows(b), :] = u0 - combo[0] * u1 - combo[1] * u2 - combo[2] * u3

    for side in range(2):
        whole_if(beside[side], SIDE_ROWS, send_sem.at[side])
        whole_if(and_(beside[side], has_prev), BACK_SIDE_ROWS, send_sem.at[4 + side])
        whole_if(and_(beside[side], has_next), AHEAD_SIDE_ROWS, send_sem.at[6 + side])
    whole_if(has_prev, BACK_ROWS, send_sem.at[2])
    whole_if(has_next, AHEAD_ROWS, send_sem.at[3])
    more = jnp.where(chip_z > 0, 1, 0)
    sent_lines = PLANE // 2 - core + more
    for count in (PLANE // 2 - 1, PLANE // 2, PLANE // 2 + 1):
        whole_if(sent_lines == count, count, send_sem.at[8])
    skips_first = and_(in_first_column, chip_z > 0)
    whole_if(and_(is_second, jnp.logical_not(skips_first)), 2 * NZ - 1, send_sem.at[9])
    whole_if(skips_first, 2 * NZ - 2, send_sem.at[9])


def on_device(right_side, error_weight, coeffs, obs_block, obs_pos, obs_weight):
    shape = (LEV, TY, NX)
    vmem, hbm = pltpu.VMEM, pltpu.HBM
    line = (STEPS, LEV, 2, 1, NX)
    scratch = [
        vmem(shape, F32),
        vmem(shape, F32),
        vmem(shape, F32),
        vmem(shape, F32),
        vmem(shape, F32),
        vmem((4, *shape), F32),
        vmem((1, 32), jnp.int32),
        vmem((32, 128), jnp.int32),
        vmem((32, 128), F32),
        vmem(shape, F32),
        vmem((STEPS, LEV, 2, 2, 1, NX), F32),
        vmem((2, LEV, 4, 1, NX), F32),
        vmem((LEV, 2, 1, NX), F32),
        vmem((2, LEV, 1, NX), F32),
        vmem((STEPS, LEV, 2, 2, 1, NX), F32),
        vmem((2, LEV, 4, 1, NX), F32),
        vmem((2, LEV, 1, NX), F32),
        vmem(line, F32),
        vmem(line, F32),
        vmem((LEV, 2, 1, NX), F32),
        vmem((STEPS, *shape), F32),
        vmem(shape, F32),
        vmem((2, 8, NX), F32),
        vmem((2, 8, NX), F32),
        vmem((STEPS, *shape), F32),
        vmem((STEPS, *shape), F32),
        vmem((LEV, 2, 1, NX), F32),
        vmem(shape, F32),
        vmem(shape, F32),
        vmem((len(PAIRS), 8, 128), F32),
        vmem((len(PAIRS), 8, 128), F32),
        vmem((128, 128), F32),
        vmem((2, 1, 128), F32),
        vmem((NZ, 1, 128), F32),
        vmem((PLANE, 128), F32),
        vmem((NWIN * NT - PLANE, 128), F32),
        vmem((1, 128), F32),
        pltpu.SemaphoreType.DMA((6,)),
        pltpu.SemaphoreType.DMA((10,)),
        pltpu.SemaphoreType.DMA((2, LEV, MESSAGES)),
        pltpu.SemaphoreType.DMA((1,)),
        pltpu.SemaphoreType.DMA((3,)),
        pltpu.SemaphoreType.REGULAR((7,)),
        vmem((BACK_ROWS, 1, 128), F32),
    ]
    solution_field, residual = pl.pallas_call(
        kernel,
        out_shape=(pltpu.VMEM((1, *shape), F32), pltpu.VMEM((1, *shape), F32)),
        in_specs=[pl.BlockSpec(memory_space=hbm)] * 6,
        out_specs=(pl.BlockSpec(memory_space=vmem),) * 2,
        scratch_shapes=scratch,
        compiler_params=pltpu.CompilerParams(collective_id=0, has_side_effects=True),
        name="krylov",
    )(
        right_side.reshape(shape),
        error_weight.reshape(shape),
        coeffs.reshape(4, *shape),
        obs_block,
        obs_pos.reshape(32, 128),
        obs_weight.reshape(32, 128),
    )
    whole = jax.ShapeDtypeStruct((1, *shape), F32)
    return pl.pallas_call(
        store,
        out_shape=(whole, whole),
        in_specs=[pl.BlockSpec(memory_space=vmem)] * 2,
        out_specs=(pl.BlockSpec(memory_space=hbm),) * 2,
        scratch_shapes=[pltpu.SemaphoreType.DMA((2 * LEV,))],
        name="store",
    )(*(pltpu.with_memory_space_constraint(x, vmem) for x in (solution_field, residual)))


def store(solution_field, residual, solution_out, residual_out, sem):
    copies = [
        pltpu.make_async_copy(src.at[0, l], dst.at[0, l], sem.at[LEV * n + l])
        for n, (src, dst) in enumerate(((solution_field, solution_out), (residual, residual_out)))
        for l in range(LEV)
    ]
    for copy in copies:
        copy.start()
    for copy in copies:
        copy.wait()


def solution(mesh):
    in_specs = (
        P("win", None, "tile", None),
        P("win", None, "tile", None),
        P(None, "win", None, "tile", None),
        P("win", "tile"),
        P("win", "tile", None),
        P("win", "tile", None),
    )
    out_specs = (P("win", None, "tile", None), P("win", None, "tile", None))
    return jax.shard_map(on_device, mesh=mesh, in_specs=in_specs, out_specs=out_specs, check_vma=False)
```

```python
import jax
import jax.numpy as jnp
from jax import lax
from jax.experimental import pallas as pl
from jax.experimental.pallas import tpu as pltpu
from jax.sharding import PartitionSpec as P

MESH = pl.DeviceIdType.MESH
F32 = jnp.float32
LEV, TY, NX = 2, 32, 1024
BLOCKS = TY // 8
STEPS = 3
SCALE = 1.0 / 16.0
NZ, NYC, NCORE, NT = 8, 8, 2, 4
NWIN = NZ * NYC * NCORE
PLANE = NYC * NCORE * NT
PAIRS = ((0, 0), (0, 1), (1, 1), (0, 2), (1, 2), (2, 2), (0, 3), (1, 3), (2, 3))
HALO, BACK, FORE, STATE, IMAGE = 0, 2, 4, 6, 10
MESSAGES = 14
WIDE = NX // 128
SIDE_ROWS = LEV * (2 * STEPS + 4) * WIDE
BACK_ROWS = (STEPS + 1) * LEV * TY * WIDE
AHEAD_ROWS = (STEPS * LEV * TY + 2 * LEV) * WIDE
BACK_SIDE_ROWS = LEV * (STEPS + 1) * WIDE
AHEAD_SIDE_ROWS = LEV * STEPS * WIDE
EARLY = 6
MIDDLE = (1, 2)
OUTER = ((0, 1), (TY - 1, TY - 2))


def two_sum(a, b):
    s = a + b
    t = s - a
    return s, (a - (s - t)) + (b - t)


def quick_sum(a, b):
    s = a + b
    return s, b - (s - a)


def split(a):
    c = a * 4097.0
    high = c - (c - a)
    return high, a - high


def two_prod_split(a, b, sa, sb):
    p = a * b
    return p, ((sa[0] * sb[0] - p) + sa[0] * sb[1] + sa[1] * sb[0]) + sa[1] * sb[1]


def two_prod(a, b):
    return two_prod_split(a, b, split(a), split(b))


def add2(a, b):
    s, e = two_sum(a[0], b[0])
    return quick_sum(s, e + (a[1] + b[1]))


def neg2(a):
    return -a[0], -a[1]


def sub2(a, b):
    return add2(a, neg2(b))


def mul2(a, b):
    p, e = two_prod(a[0], b[0])
    return quick_sum(p, e + (a[0] * b[1] + a[1] * b[0]))


def div2(a, b):
    zero = jnp.zeros_like(a[0])
    first = a[0] / b[0]
    rest = sub2(a, mul2((first, zero), b))
    return quick_sum(first, rest[0] / b[0])


def plus(a, b):
    s, e = two_sum(a[0], b[0])
    return s, (a[1] + b[1]) + e


def tree2(items):
    while len(items) > 1:
        items = [
            plus(items[i], items[i + 1]) if i + 1 < len(items) else items[i]
            for i in range(0, len(items), 2)
        ]
    return items[0]


def rolled(pair, shift, axis):
    return pltpu.roll(pair[0], shift, axis), pltpu.roll(pair[1], shift, axis)


def kernel(
    right_hbm,
    weight_hbm,
    coeff_hbm,
    block_hbm,
    pos_hbm,
    obsw_hbm,
    solution_out,
    residual_out,
    v0,
    v1,
    v2,
    v3,
    weight,
    coeff,
    block,
    pos,
    obsw,
    diag,
    edge,
    coeff_edge,
    centre_edge,
    weight_edge,
    halo,
    coeff_halo,
    weight_halo,
    next_halo,
    prev_halo,
    prev_centre,
    next_state,
    next_weight,
    term,
    next_term,
    image,
    before,
    spread_halo,
    follow,
    spread,
    gram_high,
    gram_low,
    gram_line,
    row_send,
    row_recv,
    plane_recv,
    far_recv,
    final_line,
    local_sem,
    send_sem,
    recv_sem,
    once_sem,
    rrecv_sem,
    known_sem,
    ballast,
):
    win = lax.axis_index("win")
    tile = lax.axis_index("tile")
    core = win % 2
    chip_y = (win // 2) % 8
    chip_z = win // 16
    has_prev, has_next = win > 0, win < NWIN - 1
    has_north, has_south = tile > 0, tile < NT - 1
    prev_id, next_id = (win - 1, tile), (win + 1, tile)
    states = (v0, v1, v2, v3)

    loads = [
        pltpu.make_async_copy(src, dst, local_sem.at[i])
        for i, (src, dst) in enumerate(
            (
                (right_hbm, v0),
                (weight_hbm, weight),
                (coeff_hbm, coeff),
                (block_hbm, block),
                (pos_hbm, pos),
                (obsw_hbm, obsw),
            )
        )
    ]
    for load in loads:
        load.start()

    def along_y(by):
        return (win + 2 * ((chip_y + by) % NYC - chip_y), tile)

    def along_z(by, other_core=False):
        start = win + 1 - 2 * core if other_core else win
        return (start + 16 * ((chip_z + by) % NZ - chip_z), tile)

    group = core * NT + tile
    slot_a = chip_y * 8 + group
    near = [
        (win - core + ((group + i) % 8) // NT, (group + i) % NT) for i in range(1, NCORE * NT)
    ]
    near = [along_y(1), along_y(-1)] + near
    near = [along_z(by, other) for by in (1, -1) for other in (False, True)] + near

    def signal(semaphore, peer):
        pl.semaphore_signal(semaphore, inc=1, device_id=peer, device_id_type=MESH)

    barrier = pltpu.get_barrier_semaphore()

    @pl.when(has_prev)
    def _():
        signal(barrier, prev_id)

    @pl.when(has_next)
    def _():
        signal(barrier, next_id)

    for peer in near:
        signal(barrier, peer)

    for i in range(2):
        loads[i].wait()
    for side in range(2):
        for l in range(LEV):
            for n, row in enumerate(OUTER[side]):
                edge[0, l, side, n] = v0[l, row : row + 1, :]
            row = OUTER[side][0]
            weight_edge[side, l] = weight[l, row : row + 1, :]

    pl.semaphore_wait(barrier, len(near) + jnp.where(has_prev, 1, 0) + jnp.where(has_next, 1, 0))

    def whole_if(condition, count, semaphore):
        @pl.when(condition)
        def _():
            whole = ballast.at[pl.ds(0, count)]
            pltpu.make_async_copy(whole, whole, semaphore).wait()

    def remote(src, dst, send, recv, peer):
        return pltpu.make_async_remote_copy(
            src_ref=src, dst_ref=dst, send_sem=send, recv_sem=recv, device_id=peer, device_id_type=MESH
        )

    def start_if(condition, copies):
        @pl.when(condition)
        def _():
            for copy in copies:
                copy.start()

    def wait_if(condition, copies):
        @pl.when(condition)
        def _():
            for copy in copies:
                copy.wait_recv()

    beside = (has_north, has_south)

    def towards(side, by):
        return (win + by, tile + (1 if side else -1))

    def and_(*conditions):
        total = conditions[0]
        for condition in conditions[1:]:
            total = jnp.logical_and(total, condition)
        return total

    def to_side(kind, j, l, side):
        sem = recv_sem.at[j % 2, l, kind + 1 - side]
        if kind == HALO:
            return remote(edge.at[j, l, side], halo.at[j, l, 1 - side], send_sem.at[side], sem, towards(side, 0))
        dst, out, by = (next_halo, 4, -1) if kind == BACK else (prev_halo, 6, 1)
        return remote(
            edge.at[j, l, side, 0], dst.at[j, l, 1 - side], send_sem.at[out + side], sem, towards(side, by)
        )

    def send_edges(j, l, side, diagonal=True, straight=True):
        if diagonal:
            start_if(and_(beside[side], has_prev), [to_side(BACK, j, l, side)])
            start_if(and_(beside[side], has_next), [to_side(FORE, j, l, side)])
        if straight:
            start_if(beside[side], [to_side(HALO, j, l, side)])

    def edges_from(kind, j, l, side):
        extra = {HALO: (), BACK: (has_next,), FORE: (has_prev,)}[kind]
        wait_if(and_(beside[side], *extra), [to_side(kind, j, l, 1 - side)])

    def state_block(j, l, b):
        at = pl.ds(8 * b, 8)
        return remote(
            states[j].at[l, at], next_state.at[j, l, at], send_sem.at[2], recv_sem.at[j % 2, l, STATE + b], prev_id
        )

    def image_block(j, l, b):
        at = pl.ds(8 * b, 8)
        return remote(
            image.at[j, l, at], before.at[j, l, at], send_sem.at[3], recv_sem.at[j % 2, l, IMAGE + b], next_id
        )

    def first_block(l, b):
        return state_block(0, l, b)

    def weight_block(l, b):
        at = pl.ds(8 * b, 8)
        late = int(from_next(0, l, b))
        return remote(
            weight.at[l, at], next_weight.at[l, at], send_sem.at[2], recv_sem.at[late, l, STATE + b], prev_id
        )

    def term_block(b):
        n = MIDDLE.index(b)
        return remote(
            term.at[n], next_term.at[n], send_sem.at[2], recv_sem.at[0, LEV - 1, STATE + b], prev_id
        )

    def from_next(j, l, b):
        return j == 0 and l == LEV - 1 and b in MIDDLE

    def coeff_side(side):
        return remote(
            coeff_edge.at[side], coeff_halo.at[1 - side], send_sem.at[side], recv_sem.at[0, 0, HALO + 1 - side], towards(side, 0)
        )

    def weight_side(side):
        return remote(
            weight_edge.at[side],
            weight_halo.at[1 - side],
            send_sem.at[4 + side],
            recv_sem.at[0, 0, BACK + 1 - side],
            towards(side, -1),
        )

    def centre_ahead():
        return remote(centre_edge, prev_centre, send_sem.at[3], once_sem.at[0], next_id)

    row_id = lax.broadcasted_iota(jnp.int32, (8, NX), 0)
    first_row, last_row = row_id == 0, row_id == 7

    def rows(b):
        return slice(8 * b, 8 * b + 8)

    def vertical(ref, l, b, top=0.0, bottom=0.0):
        here = ref[l, rows(b), :]
        above = pltpu.roll(ref[l, rows(b - 1), :], 1, 0) if b > 0 else top
        below = pltpu.roll(ref[l, rows(b + 1), :], 7, 0) if b < BLOCKS - 1 else bottom
        north = jnp.where(first_row, above, pltpu.roll(here, 1, 0))
        south = jnp.where(last_row, below, pltpu.roll(here, 7, 0))
        return north + south

    def edge_only(side, value):
        return jnp.where((first_row, last_row)[side], value, 0.0)

    def propagate(j, l, b):
        v = states[j]
        here = v[l, rows(b), :]
        image[j, l, rows(b), :] = (
            coeff[0, l, rows(b), :] * here
            + coeff[1, l, rows(b), :] * vertical(v, l, b)
            + coeff[2, l, rows(b), :] * pltpu.roll(here, NX - 1, 1)
            + coeff[3, l, rows(b), :] * pltpu.roll(here, 1, 1)
        )
        if j > 0 or l == 0 or from_next(j, l, b):
            start_if(has_next, [image_block(j, l, b)])

    def side_of(b):
        return {0: 0, BLOCKS - 1: 1}.get(b)

    def outside(j, l, side):
        first = j == 0 and l == 0
        if first:
            whole_if(beside[side], (2 + LEV * 4) * WIDE, recv_sem.at[0, 0, HALO + side])
        else:
            edges_from(HALO, j, l, side)
        near_row, far_row = halo[j, l, side, 0], halo[j, l, side, 1]
        row = OUTER[side][0]
        here = (
            coeff_halo[side, l, 0] * near_row
            + coeff_halo[side, l, 1] * (far_row + states[j][l, row : row + 1, :])
            + coeff_halo[side, l, 2] * pltpu.roll(near_row, NX - 1, 1)
            + coeff_halo[side, l, 3] * pltpu.roll(near_row, 1, 1)
        )
        if first:
            whole_if(and_(beside[side], has_next), (1 + LEV) * WIDE, recv_sem.at[0, 0, BACK + side])
        else:
            edges_from(BACK, j, l, side)
        f = weight_halo[side, l] * (next_halo[j, l, side] - here)
        spread_halo[l, side] = coeff_halo[side, l, 1] * f

    def finish(j, l, order, at):
        b = order[at]
        v, out = states[j], states[j + 1]
        side = side_of(b)
        f = follow[l, rows(b), :]
        top = spread_halo[l, 0] if side == 0 else 0.0
        bottom = spread_halo[l, 1] if side == 1 else 0.0
        back_image = (
            coeff[0, l, rows(b), :] * f
            + vertical(spread, l, b, top, bottom)
            + pltpu.roll(coeff[2, l, rows(b), :] * f, 1, 1)
            + pltpu.roll(coeff[3, l, rows(b), :] * f, NX - 1, 1)
        )
        here = v[l, rows(b), :]
        out[l, rows(b), :] = weight[l, rows(b), :] * here - back_image + diag[l, rows(b), :] * here
        if not from_next(j, l, b):
            wait_if(has_prev, [image_block(j, l, b)])
        came = before[j, l, rows(b), :]
        if side is not None:
            edges_from(FORE, j, l, side)
            if j == 0 and l == 0 and at == 0:
                wait_if(has_prev, [centre_ahead()])
            came = came + edge_only(side, prev_centre[l, side] * prev_halo[j, l, side])
        out[l, rows(b), :] = SCALE * (out[l, rows(b), :] - weight[l, rows(b), :] * came)
        if j + 1 == STEPS:
            keep(j, gram_block(j, l, rows(b), kept(j)))
            return
        if side is not None:
            for n, row in enumerate(OUTER[side]):
                edge[j + 1, l, side, n] = out[l, row : row + 1, :]
            send_edges(j + 1, l, side)
        start_if(has_prev, [state_block(j + 1, l, b)])
        if at > 0:
            propagate(j + 1, l, order[at - 1])
        if at == BLOCKS - 1:
            propagate(j + 1, l, b)

    def complete(j, l, order):
        for at, b in enumerate(order):
            side = side_of(b)
            if side is not None:
                outside(j, l, side)
            if from_next(j, l, b):
                wait_if(has_next, [term_block(b)])
                f = next_term[MIDDLE.index(b)]
            else:
                first = j == (1 if from_next(0, l, b) else 0)
                if first:
                    whole_if(has_next, 2 * 8 * WIDE, recv_sem.at[j, l, STATE + b])
                else:
                    wait_if(has_next, [state_block(j, l, b)])
                sent_image = image[j, l, rows(b), :]
                if side is not None:
                    sent_image = sent_image + edge_only(side, coeff[1, l, rows(b), :] * halo[j, l, side, 0])
                f = next_weight[l, rows(b), :] * (next_state[j, l, rows(b), :] - sent_image)
            follow[l, rows(b), :] = f
            spread[l, rows(b), :] = coeff[1, l, rows(b), :] * f
            if at > 0:
                finish(j, l, order, at - 1)
        finish(j, l, order, BLOCKS - 1)

    def by_parity(body):
        pl.when(tile % 2 == 0)(lambda: body(tuple(range(BLOCKS))))
        pl.when(tile % 2 == 1)(lambda: body(tuple(reversed(range(BLOCKS)))))

    def gram_block(group, l, at, acc):
        acc = list(acc)
        for c in range(NX // 128):
            parts = {}
            for n in range(3):
                i, k = PAIRS[3 * group + n]
                for s in (i, k):
                    if s not in parts:
                        x = states[s][l, at, c * 128 : (c + 1) * 128]
                        parts[s] = (x, split(x))
                p, e = two_prod_split(parts[i][0], parts[k][0], parts[i][1], parts[k][1])
                s, f = two_sum(acc[2 * n], p)
                acc[2 * n], acc[2 * n + 1] = s, acc[2 * n + 1] + (e + f)
        return tuple(acc)

    def keep(group, acc):
        for n in range(3):
            gram_high[3 * group + n], gram_low[3 * group + n] = acc[2 * n], acc[2 * n + 1]

    def kept(group):
        return tuple(ref[3 * group + n] for n in range(3) for ref in (gram_high, gram_low))

    def gram_lines(group):
        acc = kept(group)
        for n in range(3):
            index = 3 * group + n
            line = over_rows((acc[2 * n], acc[2 * n + 1]))
            gram_line[index : index + 1, :], gram_line[16 + index : 17 + index, :] = line

    def gram(group):
        def step(n, acc):
            at = pl.ds(pl.multiple_of((n % BLOCKS) * 8, 8), 8)
            return gram_block(group, n // BLOCKS, at, acc)

        keep(group, lax.fori_loop(0, LEV * BLOCKS, step, (jnp.zeros((8, 128), F32),) * 6))
        gram_lines(group)

    def over_rows(total):
        for shift in (4, 2, 1):
            total = plus(total, rolled(total, shift, 0))
        return total[0][0:1, :], total[1][0:1, :]

    def observed_weights():
        pos_t = jnp.swapaxes(pos[...], 0, 1)
        obsw_t = jnp.swapaxes(obsw[...], 0, 1)
        lane = lax.broadcasted_iota(jnp.int32, (128, 128), 1)
        lines = []
        for b in range(32):
            hit = pos_t[:, b : b + 1] == lane
            lines.append(jnp.sum(jnp.where(hit, obsw_t[:, b : b + 1], 0.0), axis=0, keepdims=True))
        per_block = jnp.concatenate(lines, axis=0)
        row = lax.broadcasted_iota(jnp.int32, (LEV * TY, 32), 0)
        for c in range(NX // 128):
            hot = (block[...] == row * (NX // 128) + c).astype(F32)
            out = jnp.dot(hot, per_block, precision=lax.Precision.HIGHEST, preferred_element_type=F32)
            for l in range(LEV):
                diag[l, :, c * 128 : (c + 1) * 128] = out[l * TY : (l + 1) * TY, :]

    def zeros(*refs):
        for ref in refs:
            ref[...] = jnp.zeros(ref.shape, F32)

    gram_line[...] = jnp.zeros((128, 128), F32)
    for side in range(2):
        for by in range(LEV):
            send_edges(0, by, side, diagonal=False)
        pl.when(beside[side])(lambda side=side: signal(known_sem.at[6], towards(side, 0)))
    def bulk(order):
        places = [(l, b) for l in range(LEV) for b in order if not from_next(0, l, b)]
        return [copy(*place) for place in places for copy in (first_block, weight_block)]

    by_parity(lambda order: start_if(has_prev, bulk(order)[:EARLY]))
    loads[2].wait()

    @by_parity
    def _(order):
        places = [(l, b) for l in range(LEV) for b in order]
        for place in sorted(places, key=lambda place: not from_next(0, *place)):
            propagate(0, *place)

    def pass_on(number):
        if number > 0:
            pl.semaphore_wait(known_sem.at[number - 1], 2)
        if number < 6:
            move, by = (along_y, along_z)[number // 3], (1, 2, 1)[number % 3]
            for peer in (move(by), move(-by)):
                signal(known_sem.at[number], peer)

    pass_on(0)
    pl.semaphore_wait(known_sem.at[6], jnp.where(has_north, 1, 0) + jnp.where(has_south, 1, 0))
    for side in range(2):
        start_if(and_(beside[side], has_prev), [weight_side(side)])
        for l in range(LEV):
            send_edges(0, l, side, straight=False)
    by_parity(lambda order: start_if(has_prev, bulk(order)[EARLY:]))
    for side in range(2):
        row = OUTER[side][0]
        for l in range(LEV):
            for n in range(4):
                coeff_edge[side, l, n] = coeff[n, l, row : row + 1, :]
            centre_edge[l, side] = coeff[1, l, row : row + 1, :]
    for side in range(2):
        start_if(beside[side], [coeff_side(side)])
    start_if(has_next, [centre_ahead()])
    by_parity(lambda order: start_if(has_next, [image_block(0, 1, b) for b in order if b not in MIDDLE]))
    for side in range(2):

        @pl.when(jnp.logical_not(beside[side]))
        def _(side=side):
            zeros(coeff_halo.at[side], weight_halo.at[side])
            for j in range(STEPS):
                for l in range(LEV):
                    zeros(halo.at[j, l, side], next_halo.at[j, l, side], prev_halo.at[j, l, side])

    pl.when(jnp.logical_not(has_prev))(lambda: zeros(before, prev_halo, prev_centre))
    pl.when(jnp.logical_not(has_next))(lambda: zeros(next_state, next_weight, next_term, next_halo, weight_halo))
    for load in loads[3:]:
        load.wait()
    observed_weights()
    pass_on(1)
    @by_parity
    def _(order):
        l = LEV - 1
        inner = [b for b in order if b in MIDDLE]
        for b in inner:
            wait_if(has_prev, [image_block(0, l, b)])
            term[MIDDLE.index(b)] = weight[l, rows(b), :] * (v0[l, rows(b), :] - before[0, l, rows(b), :])
            start_if(has_prev, [term_block(b)])
        start_if(has_prev, [weight_block(l, b) for b in inner])

    for j in range(STEPS):
        if j + 1 == STEPS:
            keep(j, (jnp.zeros((8, 128), F32),) * 6)
        for l in range(LEV):
            by_parity(lambda order, j=j, l=l: complete(j, l, order))
            if j * LEV + l < 5:
                pass_on(j * LEV + l + 2)
        if j + 1 < STEPS:
            gram(j)
    gram_lines(STEPS - 1)

    turned = jnp.swapaxes(gram_line[...], 0, 1)
    pieces = [turned[8 * i : 8 * i + 8, :] for i in range(16)]
    total = over_rows(tree2([(x, pltpu.roll(x, 128 - 16, 1)) for x in pieces]))
    lane = lax.broadcasted_iota(jnp.int32, (1, 128), 1)

    def packed(pair):
        return jnp.where(lane < 16, pair[0], jnp.where(lane < 32, pltpu.roll(pair[1], 16, 1), 0.0))

    line = packed(total)

    def over_slots(parts):
        return over_rows(tree2([(x, pltpu.roll(x, 128 - 16, 1)) for x in parts]))

    def arrived(stage, count):
        whole = ballast.at[pl.ds(0, count)]
        pltpu.make_async_copy(whole, whole, rrecv_sem.at[stage]).wait()

    def to_plane(y, x):
        where = (win - core + 1 + 2 * (y - chip_y), x)
        return remote(
            row_send.at[0], plane_recv.at[pl.ds(slot_a, 1)], send_sem.at[8], rrecv_sem.at[0], where
        )

    def to_z(z, other_core):
        peer = (win + 16 * (z - chip_z) - other_core, tile)
        return remote(row_send.at[1], row_recv.at[chip_z], send_sem.at[9], rrecv_sem.at[1], peer)

    def to_first():
        return remote(
            row_send.at[0],
            far_recv.at[pl.ds(jnp.maximum(win * NT + tile - PLANE, 0), 1)],
            send_sem.at[8],
            rrecv_sem.at[2],
            (1, 0),
        )

    is_second = core == 1
    in_first_column = and_(is_second, chip_y == 0, tile == 0)
    is_first = and_(in_first_column, chip_z == 0)
    row_send[0] = line
    start_if(chip_z > 0, [to_first()])
    for y in range(NYC):
        for x in range(NT):
            start_if(jnp.logical_or(core == 0, chip_y * NT + tile != y * NT + x), [to_plane(y, x)])

    @pl.when(is_second)
    def _():
        plane_recv[pl.ds(slot_a, 1), :] = line
        arrived(0, PLANE - 1)
        plane = over_slots([plane_recv[8 * i : 8 * i + 8, :] for i in range(PLANE // 8)])
        mine = packed(plane)
        row_send[1] = mine
        row_recv[chip_z] = mine
        for z in range(NZ):
            start_if(and_(chip_z != z, jnp.logical_not(in_first_column) if z == 0 else chip_z != z), [to_z(z, 0)])
            to_z(z, 1).start()

        @pl.when(jnp.logical_not(is_first))
        def _():
            arrived(1, NZ - 1)

        @pl.when(is_first)
        def _():
            arrived(2, NWIN * NT - PLANE)
            far = over_slots([far_recv[8 * i : 8 * i + 8, :] for i in range((NWIN * NT - PLANE) // 8)])
            final_line[...] = packed(quick_sum(*plus(plane, far)))

    @pl.when(jnp.logical_not(is_second))
    def _():
        arrived(1, NZ)

    @pl.when(jnp.logical_not(is_first))
    def _():
        total = tree2([(x, pltpu.roll(x, 128 - 16, 1)) for x in [row_recv[i] for i in range(NZ)]])
        final_line[...] = packed(quick_sum(*total))

    line = final_line[...]

    def value(i, j):
        at = PAIRS.index((min(i, j), max(i, j)))
        return tuple(jnp.broadcast_to(line[:, at + off : at + off + 1], (8, 128)) for off in (0, 16))

    a = [[value(i, n + 1) for n in range(3)] + [value(i, 0)] for i in range(3)]
    for pivot in range(2):
        for i in range(pivot + 1, 3):
            factor = div2(a[i][pivot], a[pivot][pivot])
            for n in range(pivot + 1, 4):
                a[i][n] = sub2(a[i][n], mul2(factor, a[pivot][n]))
    zero = jnp.zeros((8, 128), F32)
    c2 = a[2][3][0] / a[2][2][0]
    c1 = sub2(a[1][3], mul2(a[1][2], (c2, zero)))[0] / a[1][1][0]
    left = sub2(a[0][3], mul2(a[0][1], (c1, zero)))
    c0 = sub2(left, mul2(a[0][2], (c2, zero)))[0] / a[0][0][0]
    combo = [jnp.concatenate([c] * (NX // 128), axis=1) for c in (c0, c1, c2)]
    for l in range(LEV):
        for b in range(BLOCKS):
            at = (l, rows(b), slice(None))
            u0, u1, u2, u3 = (s[at] for s in states)
            solution_out[0, l, rows(b), :] = SCALE * (combo[0] * u0 + combo[1] * u1 + combo[2] * u2)
            residual_out[0, l, rows(b), :] = u0 - combo[0] * u1 - combo[1] * u2 - combo[2] * u3

    for side in range(2):
        whole_if(beside[side], SIDE_ROWS, send_sem.at[side])
        whole_if(and_(beside[side], has_prev), BACK_SIDE_ROWS, send_sem.at[4 + side])
        whole_if(and_(beside[side], has_next), AHEAD_SIDE_ROWS, send_sem.at[6 + side])
    whole_if(has_prev, BACK_ROWS, send_sem.at[2])
    whole_if(has_next, AHEAD_ROWS, send_sem.at[3])
    more = jnp.where(chip_z > 0, 1, 0)
    sent_lines = PLANE // 2 - core + more
    for count in (PLANE // 2 - 1, PLANE // 2, PLANE // 2 + 1):
        whole_if(sent_lines == count, count, send_sem.at[8])
    skips_first = and_(in_first_column, chip_z > 0)
    whole_if(and_(is_second, jnp.logical_not(skips_first)), 2 * NZ - 1, send_sem.at[9])
    whole_if(skips_first, 2 * NZ - 2, send_sem.at[9])


def on_device(right_side, error_weight, coeffs, obs_block, obs_pos, obs_weight):
    shape = (LEV, TY, NX)
    vmem, hbm = pltpu.VMEM, pltpu.HBM
    line = (STEPS, LEV, 2, 1, NX)
    scratch = [
        vmem(shape, F32),
        vmem(shape, F32),
        vmem(shape, F32),
        vmem(shape, F32),
        vmem(shape, F32),
        vmem((4, *shape), F32),
        vmem((1, 32), jnp.int32),
        vmem((32, 128), jnp.int32),
        vmem((32, 128), F32),
        vmem(shape, F32),
        vmem((STEPS, LEV, 2, 2, 1, NX), F32),
        vmem((2, LEV, 4, 1, NX), F32),
        vmem((LEV, 2, 1, NX), F32),
        vmem((2, LEV, 1, NX), F32),
        vmem((STEPS, LEV, 2, 2, 1, NX), F32),
        vmem((2, LEV, 4, 1, NX), F32),
        vmem((2, LEV, 1, NX), F32),
        vmem(line, F32),
        vmem(line, F32),
        vmem((LEV, 2, 1, NX), F32),
        vmem((STEPS, *shape), F32),
        vmem(shape, F32),
        vmem((2, 8, NX), F32),
        vmem((2, 8, NX), F32),
        vmem((STEPS, *shape), F32),
        vmem((STEPS, *shape), F32),
        vmem((LEV, 2, 1, NX), F32),
        vmem(shape, F32),
        vmem(shape, F32),
        vmem((len(PAIRS), 8, 128), F32),
        vmem((len(PAIRS), 8, 128), F32),
        vmem((128, 128), F32),
        vmem((2, 1, 128), F32),
        vmem((NZ, 1, 128), F32),
        vmem((PLANE, 128), F32),
        vmem((NWIN * NT - PLANE, 128), F32),
        vmem((1, 128), F32),
        pltpu.SemaphoreType.DMA((6,)),
        pltpu.SemaphoreType.DMA((10,)),
        pltpu.SemaphoreType.DMA((2, LEV, MESSAGES)),
        pltpu.SemaphoreType.DMA((1,)),
        pltpu.SemaphoreType.DMA((3,)),
        pltpu.SemaphoreType.REGULAR((7,)),
        vmem((BACK_ROWS, 1, 128), F32),
    ]
    solution_field, residual = pl.pallas_call(
        kernel,
        out_shape=(pltpu.VMEM((1, *shape), F32), pltpu.VMEM((1, *shape), F32)),
        in_specs=[pl.BlockSpec(memory_space=hbm)] * 6,
        out_specs=(pl.BlockSpec(memory_space=vmem),) * 2,
        scratch_shapes=scratch,
        compiler_params=pltpu.CompilerParams(collective_id=0, has_side_effects=True),
        name="krylov",
    )(
        right_side.reshape(shape),
        error_weight.reshape(shape),
        coeffs.reshape(4, *shape),
        obs_block,
        obs_pos.reshape(32, 128),
        obs_weight.reshape(32, 128),
    )
    whole = jax.ShapeDtypeStruct((1, *shape), F32)
    return pl.pallas_call(
        store,
        out_shape=(whole, whole),
        in_specs=[pl.BlockSpec(memory_space=vmem)] * 2,
        out_specs=(pl.BlockSpec(memory_space=hbm),) * 2,
        scratch_shapes=[pltpu.SemaphoreType.DMA((2 * LEV,))],
        name="store",
    )(*(pltpu.with_memory_space_constraint(x, vmem) for x in (solution_field, residual)))


def store(solution_field, residual, solution_out, residual_out, sem):
    copies = [
        pltpu.make_async_copy(src.at[0, l], dst.at[0, l], sem.at[LEV * n + l])
        for n, (src, dst) in enumerate(((solution_field, solution_out), (residual, residual_out)))
        for l in range(LEV)
    ]
    for copy in copies:
        copy.start()
    for copy in copies:
        copy.wait()


def solution(mesh):
    in_specs = (
        P("win", None, "tile", None),
        P("win", None, "tile", None),
        P(None, "win", None, "tile", None),
        P("win", "tile"),
        P("win", "tile", None),
        P("win", "tile", None),
    )
    out_specs = (P("win", None, "tile", None), P("win", None, "tile", None))
    return jax.shard_map(on_device, mesh=mesh, in_specs=in_specs, out_specs=out_specs, check_vma=False)
```
